32 devices in a mesh: shard: 4 (over y, x), ctx: 2 (over core), tp: 4 (over z).
Axes of the slice: x: 2, y: 2, z: 4, core: 2. Of those that a mesh axis runs over, the one named last changes fastest.
Arguments:
- hidden_in: bfloat16 [4, 4, 512, 2048], P('shard', 'ctx'), may hold values from -6 to 6
- grad_out: bfloat16 [4, 4, 512, 2048], P('shard', 'ctx'), may hold values from -6 to 6
- segment_ids: int32 [4, 2048], P('shard'), may hold values from 0 to 5, never falling along the last dimension, each value on 1 to 1024 neighbouring positions
- group_order: int32 [4], replicated, may hold values from 0 to 3, each once
- ln1_gain: bfloat16 [2048], P('shard'), may hold values from 0.5 to 1.5
- ln1_bias: bfloat16 [2048], P('shard'), may hold values from -3 to 3
- qkv_weight: bfloat16 [2048, 6144], P('shard', 'tp'), may hold values from -3 to 3
- qkv_bias: bfloat16 [4, 1536], P('tp', 'shard'), may hold values from -3 to 3
- dense_weight: bfloat16 [2048, 2048], P('shard', 'tp'), may hold values from -0.375 to 0.375
- dense_bias: bfloat16 [2048], P('shard'), may hold values from -3 to 3
- ln2_gain: bfloat16 [2048], P('shard'), may hold values from 0.5 to 1.5
- ln2_bias: bfloat16 [2048], P('shard'), may hold values from -3 to 3
- up_weight: bfloat16 [2048, 8192], P('shard', 'tp'), may hold values from -0.125 to 0.125
- up_bias: bfloat16 [4, 2048], P('tp', 'shard'), may hold values from -3 to 3
- down_weight: bfloat16 [2048, 8192], P('shard', 'tp'), may hold values from -0.0625 to 0.0625
- down_bias: bfloat16 [2048], P('shard'), may hold values from -3 to 3
Outputs:
- output: float32 [4, 4, 512, 2048], P('shard', 'ctx', None, 'tp')
- input_grad: float32 [4, 4, 512, 2048], P('shard', 'ctx', None, 'tp')
- ln1_gain_grad: float32 [2048], P('shard')
- ln1_bias_grad: float32 [2048], P('shard')
- qkv_weight_grad: float32 [2048, 6144], P('shard', 'tp')
- qkv_bias_grad: float32 [4, 1536], P('tp', 'shard')
- dense_weight_grad: float32 [2048, 2048], P('shard', 'tp')
- out_bias_grad: float32 [2048], P('shard')
- ln2_gain_grad: float32 [2048], P('shard')
- ln2_bias_grad: float32 [2048], P('shard')
- up_weight_grad: float32 [2048, 8192], P('shard', 'tp')
- up_bias_grad: float32 [4, 2048], P('tp', 'shard')
- down_weight_grad: float32 [2048, 8192], P('shard', 'tp')
The draws below stay inside these ranges and needn't reach their ends.
Inputs may be any that keep to these rules, and one draw needn't show every extreme that they name: A permutation: stored block k of every row holds the row's places group_order[k] * 512 to group_order[k] * 512 + 511. `segment_ids`: never falling along a row; each segment has 1 to 1024 tokens, one exactly 1024.
All inputs are finite; a program needn't handle non-finite values.
Results may differ from the reference program's by a relative error of at most 0.012.
Values may be sent and summed in bfloat16 or wider, within the bound.
A program may use at most 320 MiB of HBM per device.

```python
import math
import jax
import jax.numpy as jnp
import numpy as np
from jax import lax

D = 2048
FF = 8192
HEADS = 8
HD = 256
ROT = 64
CL = 512
GROUPS = 4
LEN = 2048
ROWS = 4
N_TP = 4


def draw_qkv_weight(key, part):
    base_draw = jnp.clip(jax.random.normal(key, (D, HEADS, 3, HD), jnp.float32), -6.0, 6.0) / math.sqrt(D)
    weight = base_draw
    return weight.reshape(D, 3 * D).astype(jnp.bfloat16)


def level_of(stream_key, dims, shards, low, largest):
    def one(position, shards_of):
        heights = jax.random.uniform(jax.random.fold_in(jax.random.fold_in(stream_key, 6), position), (shards_of,), jnp.float32, low / len(shards), largest / len(shards))
        return jnp.repeat(jnp.exp(heights), dims[position] // shards_of).reshape((-1,) + (1,) * (len(dims) - position - 1))

    gain = one(*shards[0])
    for cut in shards[1:]:
        gain = gain * one(*cut)
    return gain


def length_profile(count, total, reach, slope):
    portions = [(1 << 20) // math.isqrt(rank ** slope) + 1 for rank in range(2, count + 1)]
    surplus, holding = total - reach - (count - 1), [1] * (count - 1)
    while surplus > 0:
        free = [i for i in range(count - 1) if holding[i] < reach]
        mass, left = sum([portions[i] for i in free]), surplus
        for i in free:
            extra = min(reach - holding[i], max(1, left * portions[i] // mass), surplus)
            holding[i] = holding[i] + extra
            surplus = surplus - extra
    return np.array([reach] + holding)


def uneven_parts(rng, amount, total, limit, slope):
    if amount == 2:
        one = jax.random.randint(rng, (), max(1, total - limit), min(limit, total - 1) + 1)
        return jnp.stack([one, total - one])
    sizes = jnp.asarray(length_profile(amount, total, limit, slope), jnp.int32)
    pairs = (amount - 1) // 2
    donor, receiver = sizes[1:1 + 2 * pairs:2], sizes[2:2 + 2 * pairs:2]
    room = jnp.minimum(donor - 1, limit - receiver)
    moved = jax.random.randint(jax.random.fold_in(rng, 1), (pairs,), 0, 1 << 20) % (room + 1)
    sizes = sizes.at[1:1 + 2 * pairs:2].set(donor - moved).at[2:2 + 2 * pairs:2].set(receiver + moved)
    return sizes[jax.random.permutation(jax.random.fold_in(rng, 2), amount)]


def noise(rng, shape, scale, most, split=(), kind=jnp.bfloat16):
    array = jax.random.normal(rng, shape, jnp.float32) * scale
    if len(split) > 0:
        array = level_of(rng, shape, split, -0.22, 0.18) * array
    return jnp.clip(array, min=-most, max=most).astype(kind)


def setup_inputs(seed: int = 0) -> dict:
    streams_of = jax.random.split(jax.random.key(seed), 17)
    hidden_in = noise(streams_of[0], (ROWS, GROUPS, CL, D), 1.0, 6.0, ((0, 4), (1, 2)))
    grad_out = noise(streams_of[1], (ROWS, GROUPS, CL, D), 1.0, 6.0, ((0, 4), (1, 2)))
    segment_ids = jax.vmap(lambda own: jnp.searchsorted(jnp.cumsum(uneven_parts(own, 6, LEN, LEN // 2, 2)), jnp.arange(LEN), side="right"))(jax.random.split(streams_of[2], ROWS)).reshape((ROWS, LEN)).astype(jnp.int32)
    group_order = jax.random.permutation(streams_of[3], GROUPS).astype(jnp.int32)
    ln1_gain = jnp.clip(1.0 + 0.1 * jax.random.normal(streams_of[4], (D,), jnp.float32), 0.5, 1.5).astype(jnp.bfloat16)
    ln1_bias = noise(streams_of[5], (D,), 0.5, 3.0, ((0, 4),))
    qkv_weight = draw_qkv_weight(jax.random.fold_in(streams_of[16], 71), 0)
    qkv_bias = noise(streams_of[7], (N_TP, 3 * D // N_TP), 0.5, 3.0, ((0, 4), (1, 4)))
    dense_weight = noise(streams_of[8], (D, D), (D // 8) ** -0.5, 0.375, ((0, 4), (1, 4)))
    dense_bias = noise(streams_of[9], (D,), 0.5, 3.0, ((0, 4),))
    ln2_gain = jnp.clip(1.0 + 0.1 * jax.random.normal(streams_of[10], (D,), jnp.float32), 0.5, 1.5).astype(jnp.bfloat16)
    ln2_bias = noise(streams_of[11], (D,), 0.5, 3.0, ((0, 4),))
    up_weight = noise(streams_of[12], (D, FF), D ** -0.5, 0.125, ((0, 4), (1, 4)))
    up_bias = noise(streams_of[13], (N_TP, FF // N_TP), 0.5, 3.0, ((0, 4), (1, 4)))
    down_weight = noise(streams_of[14], (D, FF), FF ** -0.5, 0.0625, ((0, 4), (1, 4)))
    down_bias = noise(streams_of[15], (D,), 0.5, 3.0, ((0, 4),))
    return dict(hidden_in=hidden_in, grad_out=grad_out, segment_ids=segment_ids, group_order=group_order, ln1_gain=ln1_gain, ln1_bias=ln1_bias, qkv_weight=qkv_weight, qkv_bias=qkv_bias, dense_weight=dense_weight, dense_bias=dense_bias, ln2_gain=ln2_gain, ln2_bias=ln2_bias, up_weight=up_weight, up_bias=up_bias, down_weight=down_weight, down_bias=down_bias)


EPSILON = 1e-05
ROTARY_BASE = 10000.0

def layer_norm(values, gain_vec, shift_vec):
    mean_row = lax.optimization_barrier(jnp.mean(values, axis=-1, keepdims=True))
    centered = values - mean_row
    inverse = lax.rsqrt(lax.optimization_barrier(jnp.mean(centered * centered, axis=-1, keepdims=True)) + EPSILON)
    normed = centered * inverse
    return (normed * gain_vec + shift_vec, normed, inverse)

def norm_backward(grad_norm, normed, inverse, gain_vec):
    scaled = grad_norm * gain_vec
    inner_term = scaled - lax.optimization_barrier(jnp.mean(scaled, axis=-1, keepdims=True)) - normed * lax.optimization_barrier(jnp.mean(scaled * normed, axis=-1, keepdims=True))
    return (inverse * inner_term, lax.optimization_barrier(jnp.sum(grad_norm * normed, axis=0)), lax.optimization_barrier(jnp.sum(grad_norm, axis=0)))

def segment_positions(segments):
    length_all = segments.shape[1]
    index_row = jnp.arange(length_all, dtype=jnp.int32)[None, :]
    changed = jnp.concatenate([jnp.ones((segments.shape[0], 1), dtype=jnp.bool_), segments[:, 1:] != segments[:, :-1]], axis=1)
    seg_start = jnp.where(changed, index_row, jnp.zeros_like(segments))
    seg_first = lax.cummax(seg_start, axis=1)
    return (index_row - seg_first).astype(jnp.int32)

def rotary_tables(positions):
    half_rot = ROT // 2
    frequency = ROTARY_BASE ** (-2.0 * jnp.arange(half_rot, dtype=jnp.float32) / ROT)
    angles = positions.astype(jnp.float32)[:, None] * frequency[None, :]
    cosine_table = jnp.concatenate([jnp.cos(angles), jnp.cos(angles)], axis=-1)
    sine_table = jnp.concatenate([jnp.sin(angles), jnp.sin(angles)], axis=-1)
    return (cosine_table, sine_table)

def rotate(values, cosine_table, sine_table):
    half_rot = ROT // 2
    rot_part = values[..., :ROT]
    turned = jnp.concatenate([-rot_part[..., half_rot:], rot_part[..., :half_rot]], axis=-1)
    rotated = rot_part * cosine_table[:, None, :] + turned * sine_table[:, None, :]
    return jnp.concatenate([rotated, values[..., ROT:]], axis=-1)

def rotate_back(grad_values, cosine_table, sine_table):
    half_rot = ROT // 2
    rot_part = grad_values[..., :ROT]
    moved_part = rot_part * sine_table[:, None, :]
    turned = jnp.concatenate([-moved_part[..., half_rot:], moved_part[..., :half_rot]], axis=-1)
    return jnp.concatenate([rot_part * cosine_table[:, None, :] - turned, grad_values[..., ROT:]], axis=-1)

def gelu_slope(pre_act):
    cdf_part = 0.5 * (1.0 + jax.scipy.special.erf(pre_act / math.sqrt(2.0)))
    return cdf_part + pre_act * jnp.exp(-0.5 * pre_act * pre_act) / math.sqrt(2.0 * math.pi)

def reference(hidden_in, grad_out, segment_ids, group_order, ln1_gain, ln1_bias, qkv_weight, qkv_bias, dense_weight, dense_bias, ln2_gain, ln2_bias, up_weight, up_bias, down_weight, down_bias):
    place_all = (group_order[:, None] * CL + jnp.arange(CL, dtype=jnp.int32)[None, :]).reshape(LEN).astype(jnp.int32)
    positions = segment_positions(segment_ids)
    score_scale = 1.0 / math.sqrt(HD)
    gain_one = ln1_gain.astype(jnp.float32)
    shift_one = ln1_bias.astype(jnp.float32)
    gain_two = ln2_gain.astype(jnp.float32)
    shift_two = ln2_bias.astype(jnp.float32)
    qkv_shift = qkv_bias.reshape(3 * D).astype(jnp.float32)
    up_shift = up_bias.reshape(FF).astype(jnp.float32)
    dense_shift = dense_bias.astype(jnp.float32)
    down_shift = down_bias.astype(jnp.float32)

    def one_row(totals, row_data):
        hidden_row, cotangent_row, seg_row, pos_row = row_data
        seg_stored = seg_row[place_all]
        pos_stored = pos_row[place_all]
        cosine_table, sine_table = rotary_tables(pos_stored)
        x_float = hidden_row.reshape(LEN, D).astype(jnp.float32)
        normed_one, hat_one, inv_one = layer_norm(x_float, gain_one, shift_one)
        acts_one = normed_one.astype(jnp.bfloat16)
        projected = (jnp.dot(acts_one, qkv_weight, preferred_element_type=jnp.float32) + qkv_shift).reshape(LEN, HEADS, 3, HD)
        query_b = rotate(projected[:, :, 0], cosine_table, sine_table).astype(jnp.bfloat16)
        key_b = rotate(projected[:, :, 1], cosine_table, sine_table).astype(jnp.bfloat16)
        value_b = projected[:, :, 2].astype(jnp.bfloat16)
        allowed = (seg_stored[:, None] == seg_stored[None, :]) & (place_all[None, :] <= place_all[:, None])
        scores = jnp.einsum('qhd,khd->hqk', query_b.astype(jnp.float32), key_b.astype(jnp.float32)) * score_scale
        scores = jnp.where(allowed[None], scores, -jnp.inf)
        top_score = lax.optimization_barrier(jnp.max(scores, axis=-1, keepdims=True))
        log_total = top_score + jnp.log(lax.optimization_barrier(jnp.sum(jnp.exp(scores - top_score), axis=-1, keepdims=True)))
        prob_full = jnp.exp(scores - log_total)
        prob_b = prob_full.astype(jnp.bfloat16)
        attn_heads = jnp.einsum('hqk,khd->qhd', prob_b.astype(jnp.float32), value_b.astype(jnp.float32)).astype(jnp.bfloat16)
        attn_out = attn_heads.reshape(LEN, D)
        attn_part = jnp.dot(attn_out, dense_weight.T, preferred_element_type=jnp.float32)
        normed_two, hat_two, inv_two = layer_norm(x_float, gain_two, shift_two)
        acts_two = normed_two.astype(jnp.bfloat16)
        pre_act = jnp.dot(acts_two, up_weight, preferred_element_type=jnp.float32) + up_shift
        hidden_b = jax.nn.gelu(pre_act, approximate=False).astype(jnp.bfloat16)
        mlp_part = jnp.dot(hidden_b, down_weight.T, preferred_element_type=jnp.float32)
        output_row = x_float + attn_part + mlp_part + dense_shift + down_shift
        grad_b = cotangent_row.reshape(LEN, D)
        grad_float = grad_b.astype(jnp.float32)
        bias_grad = lax.optimization_barrier(jnp.sum(grad_float, axis=0))
        down_grad = jnp.dot(grad_b.T, hidden_b, preferred_element_type=jnp.float32)
        pre_grad = jnp.dot(grad_b, down_weight, preferred_element_type=jnp.float32) * gelu_slope(pre_act)
        up_bias_grad = lax.optimization_barrier(jnp.sum(pre_grad, axis=0))
        pre_grad_b = pre_grad.astype(jnp.bfloat16)
        up_grad = jnp.dot(acts_two.T, pre_grad_b, preferred_element_type=jnp.float32)
        norm_two_grad = jnp.dot(pre_grad_b, up_weight.T, preferred_element_type=jnp.float32)
        dense_grad = jnp.dot(grad_b.T, attn_out, preferred_element_type=jnp.float32)
        out_grad = jnp.dot(grad_b, dense_weight, preferred_element_type=jnp.float32).astype(jnp.bfloat16).reshape(LEN, HEADS, HD)
        delta_row = lax.optimization_barrier(jnp.sum(out_grad.astype(jnp.float32) * attn_heads.astype(jnp.float32), axis=-1)).T
        prob_grad = jnp.einsum('qhd,khd->hqk', out_grad.astype(jnp.float32), value_b.astype(jnp.float32))
        score_grad = (prob_full * (prob_grad - delta_row[:, :, None])).astype(jnp.bfloat16).astype(jnp.float32)
        query_grad = jnp.einsum('hqk,khd->qhd', score_grad, key_b.astype(jnp.float32)) * score_scale
        key_grad = jnp.einsum('hqk,qhd->khd', score_grad, query_b.astype(jnp.float32)) * score_scale
        value_grad = jnp.einsum('hqk,qhd->khd', prob_b.astype(jnp.float32), out_grad.astype(jnp.float32))
        query_grad = rotate_back(query_grad, cosine_table, sine_table)
        key_grad = rotate_back(key_grad, cosine_table, sine_table)
        proj_grad = jnp.stack([query_grad, key_grad, value_grad], axis=2).reshape(LEN, 3 * D)
        qkv_bias_grad = lax.optimization_barrier(jnp.sum(proj_grad, axis=0))
        proj_grad_b = proj_grad.astype(jnp.bfloat16)
        qkv_grad = jnp.dot(acts_one.T, proj_grad_b, preferred_element_type=jnp.float32)
        norm_one_grad = jnp.dot(proj_grad_b, qkv_weight.T, preferred_element_type=jnp.float32)
        input_one, gain_one_grad, shift_one_grad = norm_backward(norm_one_grad, hat_one, inv_one, gain_one)
        input_two, gain_two_grad, shift_two_grad = norm_backward(norm_two_grad, hat_two, inv_two, gain_two)
        input_row = grad_float + input_one + input_two
        row_grads = (gain_one_grad, shift_one_grad, qkv_grad, qkv_bias_grad, dense_grad, bias_grad, gain_two_grad, shift_two_grad, up_grad, up_bias_grad, down_grad)
        totals = tuple((acc + new for acc, new in zip(totals, row_grads)))
        return (totals, (output_row.reshape(GROUPS, CL, D), input_row.reshape(GROUPS, CL, D)))
    start_totals = (jnp.zeros((D,), jnp.float32), jnp.zeros((D,), jnp.float32), jnp.zeros((D, 3 * D), jnp.float32), jnp.zeros((3 * D,), jnp.float32), jnp.zeros((D, D), jnp.float32), jnp.zeros((D,), jnp.float32), jnp.zeros((D,), jnp.float32), jnp.zeros((D,), jnp.float32), jnp.zeros((D, FF), jnp.float32), jnp.zeros((FF,), jnp.float32), jnp.zeros((D, FF), jnp.float32))
    totals, (outputs, input_grads) = lax.scan(one_row, start_totals, (hidden_in, grad_out, segment_ids, positions))
    gain_one_grad, shift_one_grad, qkv_grad, qkv_bias_grad, dense_grad, bias_grad, gain_two_grad, shift_two_grad, up_grad, up_bias_grad, down_grad = totals
    return (outputs, input_grads, gain_one_grad, shift_one_grad, qkv_grad, qkv_bias_grad.reshape(N_TP, 3 * D // N_TP), dense_grad, bias_grad, gain_two_grad, shift_two_grad, up_grad, up_bias_grad.reshape(N_TP, FF // N_TP), down_grad)
```

```python
import functools
import math

import jax
import jax.numpy as jnp
from jax import lax
from jax.experimental import pallas as pl
from jax.experimental.pallas import tpu as pltpu
from jax.sharding import PartitionSpec as P

HD = 256
ROT = 64
LANES = 128

EPSILON = 1e-05
ROTARY_BASE = 10000.0
NEG = -1e30
VMEM_LIMIT = 56 * 1024 * 1024


def segment_positions(segments):
    length_all = segments.shape[0]
    index_row = jnp.arange(length_all, dtype=jnp.int32)
    changed = jnp.concatenate(
        [jnp.ones((1,), dtype=jnp.bool_), segments[1:] != segments[:-1]]
    )
    seg_start = jnp.where(changed, index_row, jnp.zeros_like(segments))
    return index_row - lax.cummax(seg_start, axis=0)


def rotary_tables(positions):
    half_rot = ROT // 2
    frequency = ROTARY_BASE ** (-2.0 * jnp.arange(half_rot, dtype=jnp.float32) / ROT)
    angles = positions.astype(jnp.float32)[:, None] * frequency[None, :]
    cosine, sine = jnp.cos(angles), jnp.sin(angles)
    count = positions.shape[0]
    rest_one = jnp.ones((count, LANES - ROT), jnp.float32)
    rest_zero = jnp.zeros((count, LANES - half_rot), jnp.float32)
    cosine_table = jnp.concatenate([cosine, cosine, rest_one], axis=1)
    low_table = jnp.concatenate([-sine, rest_zero], axis=1)
    high_table = jnp.concatenate(
        [jnp.zeros_like(sine), sine, rest_zero[:, : LANES - ROT]], axis=1
    )
    return cosine_table, low_table, high_table


def turn(values, cosine, low, high, sign):
    half_rot = ROT // 2
    down = pltpu.roll(values, LANES - half_rot, 1)
    up = pltpu.roll(values, half_rot, 1)
    return values * cosine + sign * (down * low + up * high)


def contract_first(left_mat, right_mat):
    return lax.dot_general(
        left_mat, right_mat, (((0,), (0,)), ((), ())), preferred_element_type=jnp.float32
    )


def contract_last(left_mat, right_mat):
    return lax.dot_general(
        left_mat, right_mat, (((1,), (1,)), ((), ())), preferred_element_type=jnp.float32
    )


def block_meets(bounds_ref, order_ref, q_index, k_index):
    return (
        (order_ref[k_index] <= order_ref[q_index])
        & (bounds_ref[0, k_index] <= bounds_ref[1, q_index])
        & (bounds_ref[1, k_index] >= bounds_ref[0, q_index])
    )


def pair_mask(order_ref, seg_col_ref, seg_row_ref, q_index, k_index, block):
    q_place = order_ref[q_index] * block + lax.broadcasted_iota(jnp.int32, (block, block), 0)
    k_place = order_ref[k_index] * block + lax.broadcasted_iota(jnp.int32, (block, block), 1)
    seg_q = seg_col_ref[pl.ds(q_index * block, block), :]
    seg_k = seg_row_ref[:, pl.ds(pl.multiple_of(k_index * block, block), block)]
    return (k_place <= q_place) & (seg_q == seg_k)


def attend_kernel(
    order_ref,
    bounds_ref,
    proj_ref,
    cos_ref,
    low_ref,
    high_ref,
    seg_col_ref,
    seg_row_ref,
    query_ref,
    key_ref,
    value_ref,
    attn_ref,
    lse_ref,
    top_ref,
    sum_ref,
    acc_ref,
    *,
    block,
    count,
):
    score_scale = 1.0 / math.sqrt(HD)
    for index in range(count):
        rows = pl.ds(index * block, block)
        tables = (cos_ref[rows, :], low_ref[rows, :], high_ref[rows, :])
        for start, out in ((0, query_ref), (HD, key_ref)):
            out[rows, :LANES] = turn(
                proj_ref[rows, start : start + LANES], *tables, 1.0
            ).astype(jnp.bfloat16)
            out[rows, LANES:] = proj_ref[rows, start + LANES : start + HD].astype(jnp.bfloat16)
        value_ref[rows, :] = proj_ref[rows, 2 * HD :].astype(jnp.bfloat16)

    @pl.loop(0, count)
    def _(q_index):
        rows = pl.ds(pl.multiple_of(q_index * block, block), block)
        top_ref[...] = jnp.full_like(top_ref, NEG)
        sum_ref[...] = jnp.zeros_like(sum_ref)
        acc_ref[...] = jnp.zeros_like(acc_ref)

        @pl.loop(0, count)
        def _(k_index):
            @pl.when(block_meets(bounds_ref, order_ref, q_index, k_index))
            def _():
                keys = pl.ds(pl.multiple_of(k_index * block, block), block)
                scores = contract_last(query_ref[rows, :], key_ref[keys, :]) * score_scale
                allowed = pair_mask(order_ref, seg_col_ref, seg_row_ref, q_index, k_index, block)
                scores = jnp.where(allowed, scores, NEG)
                old_top = top_ref[...]
                new_top = jnp.maximum(old_top, jnp.max(scores, axis=1, keepdims=True))
                shrink = jnp.exp(old_top - new_top)
                weights = jnp.where(allowed, jnp.exp(scores - new_top), 0.0)
                top_ref[...] = new_top
                sum_ref[...] = sum_ref[...] * shrink + jnp.sum(weights, axis=1, keepdims=True)
                acc_ref[...] = acc_ref[...] * shrink + jnp.dot(
                    weights.astype(jnp.bfloat16),
                    value_ref[keys, :],
                    preferred_element_type=jnp.float32,
                )

        attn_ref[rows, :] = (acc_ref[...] / sum_ref[...]).astype(jnp.bfloat16)
        lse_ref[rows, :] = top_ref[...] + jnp.log(sum_ref[...])


def attend_grad_kernel(
    order_ref,
    bounds_ref,
    query_ref,
    key_ref,
    value_ref,
    attn_ref,
    grad_ref,
    lse_ref,
    cos_ref,
    low_ref,
    high_ref,
    seg_col_ref,
    seg_row_ref,
    out_ref,
    sums_ref,
    query_acc,
    key_acc,
    value_acc,
    delta_ref,
    *,
    block,
    count,
):
    score_scale = 1.0 / math.sqrt(HD)
    query_acc[...] = jnp.zeros_like(query_acc)
    delta_ref[...] = jnp.sum(
        grad_ref[...].astype(jnp.float32) * attn_ref[...].astype(jnp.float32),
        axis=1,
        keepdims=True,
    )

    @pl.loop(0, count)
    def _(k_index):
        keys = pl.ds(pl.multiple_of(k_index * block, block), block)
        key_acc[...] = jnp.zeros_like(key_acc)
        value_acc[...] = jnp.zeros_like(value_acc)

        @pl.loop(0, count)
        def _(q_index):
            @pl.when(block_meets(bounds_ref, order_ref, q_index, k_index))
            def _():
                rows = pl.ds(pl.multiple_of(q_index * block, block), block)
                query, key_rows = query_ref[rows, :], key_ref[keys, :]
                grad_rows = grad_ref[rows, :]
                scores = contract_last(query, key_rows) * score_scale
                allowed = pair_mask(order_ref, seg_col_ref, seg_row_ref, q_index, k_index, block)
                probs = jnp.where(allowed, jnp.exp(scores - lse_ref[rows, :]), 0.0)
                prob_grad = contract_last(grad_rows, value_ref[keys, :])
                score_grad = (probs * (prob_grad - delta_ref[rows, :])).astype(jnp.bfloat16)
                value_acc[...] += contract_first(probs.astype(jnp.bfloat16), grad_rows)
                key_acc[...] += contract_first(score_grad, query)
                query_acc[rows, :] += jnp.dot(
                    score_grad, key_rows, preferred_element_type=jnp.float32
                )

        tables = (cos_ref[keys, :], low_ref[keys, :], high_ref[keys, :])
        key_low = turn(key_acc[:, :LANES] * score_scale, *tables, -1.0)
        key_high = key_acc[:, LANES:] * score_scale
        first = k_index == 0
        for start, part in ((HD, key_low), (HD + LANES, key_high), (2 * HD, value_acc[...])):
            columns = slice(start, start + part.shape[1])
            out_ref[keys, columns] = part.astype(jnp.bfloat16)
            sums_ref[:, columns] = jnp.where(first, 0.0, sums_ref[:, columns]) + jnp.sum(
                part, axis=0, keepdims=True
            )

    sums_ref[:, :HD] = jnp.zeros((1, HD), jnp.float32)

    @pl.loop(0, count)
    def _(q_index):
        rows = pl.ds(pl.multiple_of(q_index * block, block), block)
        tables = (cos_ref[rows, :], low_ref[rows, :], high_ref[rows, :])
        query_low = turn(query_acc[rows, :LANES] * score_scale, *tables, -1.0)
        query_high = query_acc[rows, LANES:] * score_scale
        for start, part in ((0, query_low), (LANES, query_high)):
            columns = slice(start, start + part.shape[1])
            out_ref[rows, columns] = part.astype(jnp.bfloat16)
            sums_ref[:, columns] += jnp.sum(part, axis=0, keepdims=True)


SCALAR = pl.BlockSpec(memory_space=pltpu.SMEM)
VECTOR = pl.BlockSpec(memory_space=pltpu.VMEM)


def attend(order, bounds, proj, tables, seg_col, seg_row, block, count):
    length = proj.shape[0]
    pairs = length * length
    return pl.pallas_call(
        functools.partial(attend_kernel, block=block, count=count),
        out_shape=(
            jax.ShapeDtypeStruct((length, HD), jnp.bfloat16),
            jax.ShapeDtypeStruct((length, HD), jnp.bfloat16),
            jax.ShapeDtypeStruct((length, HD), jnp.bfloat16),
            jax.ShapeDtypeStruct((length, HD), jnp.bfloat16),
            jax.ShapeDtypeStruct((length, 1), jnp.float32),
        ),
        in_specs=[SCALAR] * 2 + [VECTOR] * 6,
        out_specs=(VECTOR,) * 5,
        scratch_shapes=[
            pltpu.VMEM((block, 1), jnp.float32),
            pltpu.VMEM((block, 1), jnp.float32),
            pltpu.VMEM((block, HD), jnp.float32),
        ],
        compiler_params=pltpu.CompilerParams(vmem_limit_bytes=VMEM_LIMIT),
        cost_estimate=pl.CostEstimate(
            flops=2 * pairs * HD, bytes_accessed=16 * length * HD, transcendentals=pairs // 2
        ),
        name="attend",
    )(order, bounds, proj, *tables, seg_col, seg_row)


def attend_grad(
    order, bounds, query, key, value, attn, grad, lse, tables, seg_col, seg_row, block, count
):
    length = query.shape[0]
    pairs = length * length
    return pl.pallas_call(
        functools.partial(attend_grad_kernel, block=block, count=count),
        out_shape=(
            jax.ShapeDtypeStruct((length, 3 * HD), jnp.bfloat16),
            jax.ShapeDtypeStruct((1, 3 * HD), jnp.float32),
        ),
        in_specs=[SCALAR] * 2 + [VECTOR] * 11,
        out_specs=(VECTOR,) * 2,
        scratch_shapes=[
            pltpu.VMEM((length, HD), jnp.float32),
            pltpu.VMEM((block, HD), jnp.float32),
            pltpu.VMEM((block, HD), jnp.float32),
            pltpu.VMEM((length, 1), jnp.float32),
        ],
        compiler_params=pltpu.CompilerParams(vmem_limit_bytes=VMEM_LIMIT),
        cost_estimate=pl.CostEstimate(
            flops=5 * pairs * HD, bytes_accessed=16 * length * HD, transcendentals=pairs // 2
        ),
        name="attend_grad",
    )(order, bounds, query, key, value, attn, grad, lse, *tables, seg_col, seg_row)


def ring_shift(value, axis, step):
    count = lax.axis_size(axis)
    return lax.ppermute(value, axis, [(i, (i + step) % count) for i in range(count)])


def local(
    hidden_in,
    grad_out,
    segment_ids,
    group_order,
    ln1_gain,
    ln1_bias,
    qkv_weight,
    qkv_bias,
    dense_weight,
    dense_bias,
    ln2_gain,
    ln2_bias,
    up_weight,
    up_bias,
    down_weight,
    down_bias,
):
    _, groups_dev, block_len, width = hidden_in.shape
    tokens = groups_dev * block_len
    seq_len = segment_ids.shape[1]
    groups = seq_len // block_len
    ctx_count, tp_count = lax.axis_size("ctx"), lax.axis_size("tp")
    shard_count = lax.axis_size("shard")
    ctx_rank, tp_rank = lax.axis_index("ctx"), lax.axis_index("tp")
    shard_rank = lax.axis_index("shard")
    slice_width = width // tp_count
    bf16, f32 = jnp.bfloat16, jnp.float32

    def my_columns(matrix):
        columns = matrix.shape[1] // ctx_count
        return lax.dynamic_slice_in_dim(matrix, ctx_rank * columns, columns, 1)

    def gather_rows(matrix):
        return lax.all_gather(my_columns(matrix), "shard", axis=0, tiled=True)

    def whole_row(part):
        return jnp.concatenate(
            [part] + [ring_shift(part, "ctx", ctx_count - k) for k in range(1, ctx_count)], axis=0
        )

    x_mine = hidden_in.reshape(tokens, width)
    g_mine = grad_out.reshape(tokens, width)
    x_row = whole_row(x_mine)
    g_row = whole_row(g_mine)

    vectors = [
        ln1_gain, ln1_bias, ln2_gain, ln2_bias, dense_bias, down_bias, qkv_bias[0], up_bias[0],
    ]
    sizes = [v.shape[0] for v in vectors]
    packed = lax.all_gather(jnp.concatenate(vectors)[None], "shard", axis=0, tiled=True)
    spread, offset = [], 0
    for size in sizes:
        spread.append(packed[:, offset : offset + size].reshape(-1).astype(f32))
        offset += size
    gain_one, shift_one, gain_two, shift_two, bias_dense, bias_down, bias_qkv, bias_up = spread
    bias_qkv = my_columns(bias_qkv[None])
    bias_up = my_columns(bias_up[None])

    w_qkv = gather_rows(qkv_weight)
    w_dense = gather_rows(dense_weight)
    w_up = gather_rows(up_weight)
    w_down = gather_rows(down_weight)
    heads_here = w_qkv.shape[1] // (3 * HD)

    own_order = jnp.concatenate(
        [
            lax.dynamic_slice_in_dim(
                group_order, lax.rem(ctx_rank + k, ctx_count) * groups_dev, groups_dev
            )
            for k in range(ctx_count)
        ]
    )
    segments = segment_ids[0]
    positions = segment_positions(segments)

    def stored(values):
        return jnp.concatenate(
            [
                lax.dynamic_slice_in_dim(values, own_order[k] * block_len, block_len)
                for k in range(groups)
            ]
        )

    seg_stored = stored(segments)
    tables = rotary_tables(stored(positions))
    seg_blocks = seg_stored.reshape(groups, block_len)
    bounds = jnp.stack([seg_blocks[:, 0], seg_blocks[:, -1]])
    seg_col, seg_row = seg_stored[:, None], seg_stored[None, :]

    x_float = x_row.astype(f32)
    centered = x_float - jnp.mean(x_float, axis=-1, keepdims=True)
    inverse = lax.rsqrt(jnp.mean(centered * centered, axis=-1, keepdims=True) + EPSILON)
    hat = centered * inverse
    acts_one = (hat * gain_one + shift_one).astype(bf16)
    acts_two = (hat * gain_two + shift_two).astype(bf16)

    projected = jnp.dot(acts_one, w_qkv, preferred_element_type=f32) + bias_qkv
    heads = []
    for h in range(heads_here):
        heads.append(
            attend(
                own_order,
                bounds,
                projected[:, 3 * HD * h : 3 * HD * (h + 1)],
                tables,
                seg_col,
                seg_row,
                block_len,
                groups,
            )
        )
    attn = jnp.concatenate([head[3] for head in heads], axis=1)

    pre_act = jnp.dot(acts_two, w_up, preferred_element_type=f32) + bias_up
    cdf = 0.5 * (1.0 + lax.erf(pre_act * (1.0 / math.sqrt(2.0))))
    hidden = (pre_act * cdf).astype(bf16)
    slope = cdf + pre_act * jnp.exp(-0.5 * pre_act * pre_act) * (1.0 / math.sqrt(2.0 * math.pi))

    def reduce_partial(partial):
        total = partial[:tokens]
        for k in range(1, ctx_count):
            piece = partial[k * tokens : (k + 1) * tokens].astype(bf16)
            total = total + ring_shift(piece, "ctx", k).astype(f32)
        return lax.psum_scatter(
            total.astype(bf16), "tp", scatter_dimension=1, tiled=True
        ).astype(f32)

    partial_out = contract_last(attn, w_dense) + contract_last(hidden, w_down)
    summed_out = reduce_partial(partial_out)
    out_shift = lax.dynamic_slice_in_dim(bias_dense + bias_down, tp_rank * slice_width, slice_width)
    x_slice = lax.dynamic_slice_in_dim(x_mine, tp_rank * slice_width, slice_width, 1)
    output = x_slice.astype(f32) + summed_out + out_shift

    def reduce_weight(grad):
        mine = lax.psum_scatter(grad.astype(bf16), "shard", scatter_dimension=0, tiled=True)
        rows, columns = mine.shape
        whole = jnp.zeros((rows, columns * ctx_count), f32)
        for k in range(ctx_count):
            part = mine if k == 0 else ring_shift(mine, "ctx", ctx_count - k)
            place = lax.rem(ctx_rank + k, ctx_count) * columns
            whole = lax.dynamic_update_slice_in_dim(whole, part.astype(f32), place, 1)
        return whole

    bias_grad = jnp.sum(g_row.astype(f32), axis=0)
    down_grad = reduce_weight(contract_first(g_row, hidden))
    pre_grad = jnp.dot(g_row, w_down, preferred_element_type=f32) * slope
    up_bias_grad = jnp.sum(pre_grad, axis=0)
    pre_grad_b = pre_grad.astype(bf16)
    up_grad = reduce_weight(contract_first(acts_two, pre_grad_b))
    norm_two_grad = contract_last(pre_grad_b, w_up)

    dense_grad = reduce_weight(contract_first(g_row, attn))
    attn_grad = jnp.dot(g_row, w_dense, preferred_element_type=f32).astype(bf16)
    proj_parts, sum_parts = [], []
    for h, (query, key, value, attn_head, lse) in enumerate(heads):
        part, sums = attend_grad(
            own_order,
            bounds,
            query,
            key,
            value,
            attn_head,
            attn_grad[:, HD * h : HD * (h + 1)],
            lse,
            tables,
            seg_col,
            seg_row,
            block_len,
            groups,
        )
        proj_parts.append(part)
        sum_parts.append(sums[0])
    proj_grad_b = jnp.concatenate(proj_parts, axis=1)
    qkv_bias_grad = jnp.concatenate(sum_parts)
    qkv_grad = reduce_weight(contract_first(acts_one, proj_grad_b))
    norm_one_grad = contract_last(proj_grad_b, w_qkv)

    scaled = norm_one_grad * gain_one + norm_two_grad * gain_two
    inner = (
        scaled
        - jnp.mean(scaled, axis=-1, keepdims=True)
        - hat * jnp.mean(scaled * hat, axis=-1, keepdims=True)
    )
    input_sum = reduce_partial(inverse * inner)
    g_slice = lax.dynamic_slice_in_dim(g_mine, tp_rank * slice_width, slice_width, 1)
    input_grad = g_slice.astype(f32) + input_sum

    def at_slot(vector, slot, count):
        whole = jnp.zeros((vector.shape[0] * count,), f32)
        return lax.dynamic_update_slice_in_dim(whole, vector, slot * vector.shape[0], 0)

    slot = tp_rank * ctx_count + ctx_rank
    slots = tp_count * ctx_count
    pieces = [
        at_slot(up_bias_grad, slot, slots),
        at_slot(qkv_bias_grad, slot, slots),
        jnp.where(slot == 0, bias_grad, 0.0),
        jnp.sum(norm_one_grad * hat, axis=0),
        jnp.sum(norm_one_grad, axis=0),
        jnp.sum(norm_two_grad * hat, axis=0),
        jnp.sum(norm_two_grad, axis=0),
    ]
    reduced = lax.psum(jnp.concatenate(pieces), ("shard", "ctx", "tp"))
    results, offset = [], 0
    for number, piece in enumerate(pieces):
        size = piece.shape[0]
        if number < 2:
            own = size // (tp_count * shard_count)
            start = offset + (tp_rank * shard_count + shard_rank) * own
        else:
            own = size // shard_count
            start = offset + shard_rank * own
        results.append(lax.dynamic_slice_in_dim(reduced, start, own))
        offset += size
    up_bias_grad, qkv_bias_grad, bias_grad = results[:3]
    gain_one_grad, shift_one_grad, gain_two_grad, shift_two_grad = results[3:]
    out_shape = hidden_in.shape[:3] + (slice_width,)
    return (
        output.reshape(out_shape),
        input_grad.reshape(out_shape),
        gain_one_grad,
        shift_one_grad,
        qkv_grad,
        qkv_bias_grad[None],
        dense_grad,
        bias_grad,
        gain_two_grad,
        shift_two_grad,
        up_grad,
        up_bias_grad[None],
        down_grad,
    )


def solution(mesh):
    return jax.shard_map(
        local,
        mesh=mesh,
        in_specs=(
            P("shard", "ctx", None, None),
            P("shard", "ctx", None, None),
            P("shard", None),
            P(),
            P("shard"),
            P("shard"),
            P("shard", "tp"),
            P("tp", "shard"),
            P("shard", "tp"),
            P("shard"),
            P("shard"),
            P("shard"),
            P("shard", "tp"),
            P("tp", "shard"),
            P("shard", "tp"),
            P("shard"),
        ),
        out_specs=(
            P("shard", "ctx", None, "tp"),
            P("shard", "ctx", None, "tp"),
            P("shard"),
            P("shard"),
            P("shard", "tp"),
            P("tp", "shard"),
            P("shard", "tp"),
            P("shard"),
            P("shard"),
            P("shard"),
            P("shard", "tp"),
            P("tp", "shard"),
            P("shard", "tp"),
        ),
        check_vma=False,
    )
```

```python
import functools
import math

import jax
import jax.numpy as jnp
from jax import lax
from jax.experimental import pallas as pl
from jax.experimental.pallas import tpu as pltpu
from jax.sharding import PartitionSpec as P

HD = 256
ROT = 64
LANES = 128

EPSILON = 1e-05
ROTARY_BASE = 10000.0
NEG = -1e30
VMEM_LIMIT = 56 * 1024 * 1024


def segment_positions(segments):
    length_all = segments.shape[0]
    index_row = jnp.arange(length_all, dtype=jnp.int32)
    changed = jnp.concatenate(
        [jnp.ones((1,), dtype=jnp.bool_), segments[1:] != segments[:-1]]
    )
    seg_start = jnp.where(changed, index_row, jnp.zeros_like(segments))
    return index_row - lax.cummax(seg_start, axis=0)


def rotary_tables(positions):
    half_rot = ROT // 2
    frequency = ROTARY_BASE ** (-2.0 * jnp.arange(half_rot, dtype=jnp.float32) / ROT)
    angles = positions.astype(jnp.float32)[:, None] * frequency[None, :]
    cosine, sine = jnp.cos(angles), jnp.sin(angles)
    count = positions.shape[0]
    rest_one = jnp.ones((count, LANES - ROT), jnp.float32)
    rest_zero = jnp.zeros((count, LANES - half_rot), jnp.float32)
    cosine_table = jnp.concatenate([cosine, cosine, rest_one], axis=1)
    low_table = jnp.concatenate([-sine, rest_zero], axis=1)
    high_table = jnp.concatenate(
        [jnp.zeros_like(sine), sine, rest_zero[:, : LANES - ROT]], axis=1
    )
    return cosine_table, low_table, high_table


def turn(values, cosine, low, high, sign):
    half_rot = ROT // 2
    down = pltpu.roll(values, LANES - half_rot, 1)
    up = pltpu.roll(values, half_rot, 1)
    return values * cosine + sign * (down * low + up * high)


def contract_first(left_mat, right_mat):
    return lax.dot_general(
        left_mat, right_mat, (((0,), (0,)), ((), ())), preferred_element_type=jnp.float32
    )


def contract_last(left_mat, right_mat):
    return lax.dot_general(
        left_mat, right_mat, (((1,), (1,)), ((), ())), preferred_element_type=jnp.float32
    )


def block_meets(bounds_ref, order_ref, q_index, k_index):
    return (
        (order_ref[k_index] <= order_ref[q_index])
        & (bounds_ref[0, k_index] <= bounds_ref[1, q_index])
        & (bounds_ref[1, k_index] >= bounds_ref[0, q_index])
    )


def pair_mask(order_ref, seg_col_ref, seg_row_ref, q_index, k_index, block):
    q_place = order_ref[q_index] * block + lax.broadcasted_iota(jnp.int32, (block, block), 0)
    k_place = order_ref[k_index] * block + lax.broadcasted_iota(jnp.int32, (block, block), 1)
    seg_q = seg_col_ref[pl.ds(q_index * block, block), :]
    seg_k = seg_row_ref[:, pl.ds(pl.multiple_of(k_index * block, block), block)]
    return (k_place <= q_place) & (seg_q == seg_k)


def attend_kernel(
    order_ref,
    bounds_ref,
    proj_ref,
    cos_ref,
    low_ref,
    high_ref,
    seg_col_ref,
    seg_row_ref,
    query_ref,
    key_ref,
    value_ref,
    attn_ref,
    lse_ref,
    top_ref,
    sum_ref,
    acc_ref,
    *,
    block,
    count,
):
    score_scale = 1.0 / math.sqrt(HD)
    for index in range(count):
        rows = pl.ds(index * block, block)
        tables = (cos_ref[rows, :], low_ref[rows, :], high_ref[rows, :])
        for start, out in ((0, query_ref), (HD, key_ref)):
            out[rows, :LANES] = turn(
                proj_ref[rows, start : start + LANES], *tables, 1.0
            ).astype(jnp.bfloat16)
            out[rows, LANES:] = proj_ref[rows, start + LANES : start + HD].astype(jnp.bfloat16)
        value_ref[rows, :] = proj_ref[rows, 2 * HD :].astype(jnp.bfloat16)

    @pl.loop(0, count)
    def _(q_index):
        rows = pl.ds(pl.multiple_of(q_index * block, block), block)
        top_ref[...] = jnp.full_like(top_ref, NEG)
        sum_ref[...] = jnp.zeros_like(sum_ref)
        acc_ref[...] = jnp.zeros_like(acc_ref)

        @pl.loop(0, count)
        def _(k_index):
            @pl.when(block_meets(bounds_ref, order_ref, q_index, k_index))
            def _():
                keys = pl.ds(pl.multiple_of(k_index * block, block), block)
                scores = contract_last(query_ref[rows, :], key_ref[keys, :]) * score_scale
                allowed = pair_mask(order_ref, seg_col_ref, seg_row_ref, q_index, k_index, block)
                scores = jnp.where(allowed, scores, NEG)
                old_top = top_ref[...]
                new_top = jnp.maximum(old_top, jnp.max(scores, axis=1, keepdims=True))
                shrink = jnp.exp(old_top - new_top)
                weights = jnp.where(allowed, jnp.exp(scores - new_top), 0.0)
                top_ref[...] = new_top
                sum_ref[...] = sum_ref[...] * shrink + jnp.sum(weights, axis=1, keepdims=True)
                acc_ref[...] = acc_ref[...] * shrink + jnp.dot(
                    weights.astype(jnp.bfloat16),
                    value_ref[keys, :],
                    preferred_element_type=jnp.float32,
                )

        attn_ref[rows, :] = (acc_ref[...] / sum_ref[...]).astype(jnp.bfloat16)
        lse_ref[rows, :] = top_ref[...] + jnp.log(sum_ref[...])


def attend_grad_kernel(
    order_ref,
    bounds_ref,
    query_ref,
    key_ref,
    value_ref,
    attn_ref,
    grad_ref,
    lse_ref,
    cos_ref,
    low_ref,
    high_ref,
    seg_col_ref,
    seg_row_ref,
    out_ref,
    sums_ref,
    query_acc,
    key_acc,
    value_acc,
    delta_ref,
    *,
    block,
    count,
):
    score_scale = 1.0 / math.sqrt(HD)
    query_acc[...] = jnp.zeros_like(query_acc)
    delta_ref[...] = jnp.sum(
        grad_ref[...].astype(jnp.float32) * attn_ref[...].astype(jnp.float32),
        axis=1,
        keepdims=True,
    )

    @pl.loop(0, count)
    def _(k_index):
        keys = pl.ds(pl.multiple_of(k_index * block, block), block)
        key_acc[...] = jnp.zeros_like(key_acc)
        value_acc[...] = jnp.zeros_like(value_acc)

        @pl.loop(0, count)
        def _(q_index):
            @pl.when(block_meets(bounds_ref, order_ref, q_index, k_index))
            def _():
                rows = pl.ds(pl.multiple_of(q_index * block, block), block)
                query, key_rows = query_ref[rows, :], key_ref[keys, :]
                grad_rows = grad_ref[rows, :]
                scores = contract_last(query, key_rows) * score_scale
                allowed = pair_mask(order_ref, seg_col_ref, seg_row_ref, q_index, k_index, block)
                probs = jnp.where(allowed, jnp.exp(scores - lse_ref[rows, :]), 0.0)
                prob_grad = contract_last(grad_rows, value_ref[keys, :])
                score_grad = (probs * (prob_grad - delta_ref[rows, :])).astype(jnp.bfloat16)
                value_acc[...] += contract_first(probs.astype(jnp.bfloat16), grad_rows)
                key_acc[...] += contract_first(score_grad, query)
                query_acc[rows, :] += jnp.dot(
                    score_grad, key_rows, preferred_element_type=jnp.float32
                )

        tables = (cos_ref[keys, :], low_ref[keys, :], high_ref[keys, :])
        key_low = turn(key_acc[:, :LANES] * score_scale, *tables, -1.0)
        key_high = key_acc[:, LANES:] * score_scale
        first = k_index == 0
        for start, part in ((HD, key_low), (HD + LANES, key_high), (2 * HD, value_acc[...])):
            columns = slice(start, start + part.shape[1])
            out_ref[keys, columns] = part.astype(jnp.bfloat16)
            sums_ref[:, columns] = jnp.where(first, 0.0, sums_ref[:, columns]) + jnp.sum(
                part, axis=0, keepdims=True
            )

    sums_ref[:, :HD] = jnp.zeros((1, HD), jnp.float32)

    @pl.loop(0, count)
    def _(q_index):
        rows = pl.ds(pl.multiple_of(q_index * block, block), block)
        tables = (cos_ref[rows, :], low_ref[rows, :], high_ref[rows, :])
        query_low = turn(query_acc[rows, :LANES] * score_scale, *tables, -1.0)
        query_high = query_acc[rows, LANES:] * score_scale
        for start, part in ((0, query_low), (LANES, query_high)):
            columns = slice(start, start + part.shape[1])
            out_ref[rows, columns] = part.astype(jnp.bfloat16)
            sums_ref[:, columns] += jnp.sum(part, axis=0, keepdims=True)


SCALAR = pl.BlockSpec(memory_space=pltpu.SMEM)
VECTOR = pl.BlockSpec(memory_space=pltpu.VMEM)


def attend(order, bounds, proj, tables, seg_col, seg_row, block, count):
    length = proj.shape[0]
    pairs = length * length
    return pl.pallas_call(
        functools.partial(attend_kernel, block=block, count=count),
        out_shape=(
            jax.ShapeDtypeStruct((length, HD), jnp.bfloat16),
            jax.ShapeDtypeStruct((length, HD), jnp.bfloat16),
            jax.ShapeDtypeStruct((length, HD), jnp.bfloat16),
            jax.ShapeDtypeStruct((length, HD), jnp.bfloat16),
            jax.ShapeDtypeStruct((length, 1), jnp.float32),
        ),
        in_specs=[SCALAR] * 2 + [VECTOR] * 6,
        out_specs=(VECTOR,) * 5,
        scratch_shapes=[
            pltpu.VMEM((block, 1), jnp.float32),
            pltpu.VMEM((block, 1), jnp.float32),
            pltpu.VMEM((block, HD), jnp.float32),
        ],
        compiler_params=pltpu.CompilerParams(vmem_limit_bytes=VMEM_LIMIT),
        cost_estimate=pl.CostEstimate(
            flops=2 * pairs * HD, bytes_accessed=16 * length * HD, transcendentals=pairs // 2
        ),
        name="attend",
    )(order, bounds, proj, *tables, seg_col, seg_row)


def attend_grad(
    order, bounds, query, key, value, attn, grad, lse, tables, seg_col, seg_row, block, count
):
    length = query.shape[0]
    pairs = length * length
    return pl.pallas_call(
        functools.partial(attend_grad_kernel, block=block, count=count),
        out_shape=(
            jax.ShapeDtypeStruct((length, 3 * HD), jnp.bfloat16),
            jax.ShapeDtypeStruct((1, 3 * HD), jnp.float32),
        ),
        in_specs=[SCALAR] * 2 + [VECTOR] * 11,
        out_specs=(VECTOR,) * 2,
        scratch_shapes=[
            pltpu.VMEM((length, HD), jnp.float32),
            pltpu.VMEM((block, HD), jnp.float32),
            pltpu.VMEM((block, HD), jnp.float32),
            pltpu.VMEM((length, 1), jnp.float32),
        ],
        compiler_params=pltpu.CompilerParams(vmem_limit_bytes=VMEM_LIMIT),
        cost_estimate=pl.CostEstimate(
            flops=5 * pairs * HD, bytes_accessed=16 * length * HD, transcendentals=pairs // 2
        ),
        name="attend_grad",
    )(order, bounds, query, key, value, attn, grad, lse, *tables, seg_col, seg_row)


def ring_shift(value, axis, step):
    count = lax.axis_size(axis)
    return lax.ppermute(value, axis, [(i, (i + step) % count) for i in range(count)])


class Plane:
    def __init__(self):
        self.count = lax.axis_size("shard")
        side = math.isqrt(self.count)
        self.square = side * side == self.count
        self.first, self.second = (side, side) if self.square else (1, self.count)
        self.ranks = lax.axis_size("ctx")
        shard = lax.axis_index("shard")
        self.flip = (lax.axis_index("ctx") % 2 == 1) if self.square else False
        slow, fast = shard // self.second, shard % self.second
        if self.square:
            self.here = (jnp.where(self.flip, slow, fast), jnp.where(self.flip, fast, slow))
        else:
            self.here = (slow, fast)

    def index(self, first_step, second_step):
        first = lax.rem(self.here[0] + first_step + self.first, self.first)
        second = lax.rem(self.here[1] + second_step + self.second, self.second)
        if not self.square:
            return first * self.second + second
        side = self.first
        return jnp.where(self.flip, first * side + second, second * side + first)

    def move(self, value, first_step, second_step):
        pairs = []
        for shard in range(self.count):
            for rank in range(self.ranks):
                slow, fast = divmod(shard, self.second)
                if self.square and rank % 2 == 0:
                    slow = (slow + second_step) % self.second
                    fast = (fast + first_step) % self.first
                else:
                    slow = (slow + first_step) % self.first
                    fast = (fast + second_step) % self.second
                target = slow * self.second + fast
                pairs.append((shard * self.ranks + rank, target * self.ranks + rank))
        return lax.ppermute(value, ("shard", "ctx"), pairs)

    def gather(self, own):
        blocks = {(0, 0): own}
        for a in range(1, self.first):
            blocks[a, 0] = self.move(own, a, 0)
        for b in range(1, self.second):
            for a in range(self.first):
                blocks[a, b] = self.move(blocks[a, 0], 0, b)
        rows = own.shape[0]
        whole = jnp.zeros((rows * self.count,) + own.shape[1:], own.dtype)
        for (a, b), block in blocks.items():
            whole = lax.dynamic_update_slice_in_dim(whole, block, self.index(-a, -b) * rows, 0)
        return whole

    def scatter_sum(self, partial):
        rows = partial.shape[0] // self.count

        def block(a, b):
            return lax.dynamic_slice_in_dim(partial, self.index(a, b) * rows, rows)

        sums = {}
        for b in list(range(1, self.second)) + [0]:
            sums[b] = block(0, b).astype(jnp.float32)
            for a in range(1, self.first):
                sums[b] = sums[b] + self.move(block(a, b), a, 0).astype(jnp.float32)
        total = sums[0]
        for b in range(1, self.second):
            total = total + self.move(sums[b].astype(partial.dtype), 0, b).astype(jnp.float32)
        return total

    def full_sum(self, value):
        total = value
        for a in range(1, self.first):
            total = total + self.move(value, a, 0)
        value = total
        for b in range(1, self.second):
            total = total + self.move(value, 0, b)
        return total


def local(
    hidden_in,
    grad_out,
    segment_ids,
    group_order,
    ln1_gain,
    ln1_bias,
    qkv_weight,
    qkv_bias,
    dense_weight,
    dense_bias,
    ln2_gain,
    ln2_bias,
    up_weight,
    up_bias,
    down_weight,
    down_bias,
):
    _, groups_dev, block_len, width = hidden_in.shape
    tokens = groups_dev * block_len
    seq_len = segment_ids.shape[1]
    groups = seq_len // block_len
    ctx_count, tp_count = lax.axis_size("ctx"), lax.axis_size("tp")
    shard_count = lax.axis_size("shard")
    ctx_rank, tp_rank = lax.axis_index("ctx"), lax.axis_index("tp")
    shard_rank = lax.axis_index("shard")
    slice_width = width // tp_count
    bf16, f32 = jnp.bfloat16, jnp.float32

    def my_columns(matrix):
        columns = matrix.shape[1] // ctx_count
        return lax.dynamic_slice_in_dim(matrix, ctx_rank * columns, columns, 1)

    plane = Plane()

    def gather_rows(matrix):
        return plane.gather(my_columns(matrix))

    def whole_row(part):
        return jnp.concatenate(
            [part] + [ring_shift(part, "ctx", ctx_count - k) for k in range(1, ctx_count)], axis=0
        )

    x_mine = hidden_in.reshape(tokens, width)
    g_mine = grad_out.reshape(tokens, width)
    x_row = whole_row(x_mine)
    g_row = whole_row(g_mine)

    vectors = [
        ln1_gain, ln1_bias, ln2_gain, ln2_bias, dense_bias, down_bias, qkv_bias[0], up_bias[0],
    ]
    sizes = [v.shape[0] for v in vectors]
    packed = plane.gather(jnp.concatenate(vectors)[None])
    spread, offset = [], 0
    for size in sizes:
        spread.append(packed[:, offset : offset + size].reshape(-1).astype(f32))
        offset += size
    gain_one, shift_one, gain_two, shift_two, bias_dense, bias_down, bias_qkv, bias_up = spread
    bias_qkv = my_columns(bias_qkv[None])
    bias_up = my_columns(bias_up[None])

    w_qkv = gather_rows(qkv_weight)
    w_dense = gather_rows(dense_weight)
    w_up = gather_rows(up_weight)
    w_down = gather_rows(down_weight)
    heads_here = w_qkv.shape[1] // (3 * HD)

    own_order = jnp.concatenate(
        [
            lax.dynamic_slice_in_dim(
                group_order, lax.rem(ctx_rank + k, ctx_count) * groups_dev, groups_dev
            )
            for k in range(ctx_count)
        ]
    )
    segments = segment_ids[0]
    positions = segment_positions(segments)

    def stored(values):
        return jnp.concatenate(
            [
                lax.dynamic_slice_in_dim(values, own_order[k] * block_len, block_len)
                for k in range(groups)
            ]
        )

    seg_stored = stored(segments)
    tables = rotary_tables(stored(positions))
    seg_blocks = seg_stored.reshape(groups, block_len)
    bounds = jnp.stack([seg_blocks[:, 0], seg_blocks[:, -1]])
    seg_col, seg_row = seg_stored[:, None], seg_stored[None, :]

    x_float = x_row.astype(f32)
    centered = x_float - jnp.mean(x_float, axis=-1, keepdims=True)
    inverse = lax.rsqrt(jnp.mean(centered * centered, axis=-1, keepdims=True) + EPSILON)
    hat = centered * inverse
    acts_one = (hat * gain_one + shift_one).astype(bf16)
    acts_two = (hat * gain_two + shift_two).astype(bf16)

    projected = jnp.dot(acts_one, w_qkv, preferred_element_type=f32) + bias_qkv
    heads = []
    for h in range(heads_here):
        heads.append(
            attend(
                own_order,
                bounds,
                projected[:, 3 * HD * h : 3 * HD * (h + 1)],
                tables,
                seg_col,
                seg_row,
                block_len,
                groups,
            )
        )
    attn = jnp.concatenate([head[3] for head in heads], axis=1)

    pre_act = jnp.dot(acts_two, w_up, preferred_element_type=f32) + bias_up
    cdf = 0.5 * (1.0 + lax.erf(pre_act * (1.0 / math.sqrt(2.0))))
    hidden = (pre_act * cdf).astype(bf16)
    slope = cdf + pre_act * jnp.exp(-0.5 * pre_act * pre_act) * (1.0 / math.sqrt(2.0 * math.pi))

    def reduce_partial(partial):
        total = partial[:tokens]
        for k in range(1, ctx_count):
            piece = partial[k * tokens : (k + 1) * tokens].astype(bf16)
            total = total + ring_shift(piece, "ctx", k).astype(f32)
        return lax.psum_scatter(
            total.astype(bf16), "tp", scatter_dimension=1, tiled=True
        ).astype(f32)

    partial_out = contract_last(attn, w_dense) + contract_last(hidden, w_down)
    summed_out = reduce_partial(partial_out)
    out_shift = lax.dynamic_slice_in_dim(bias_dense + bias_down, tp_rank * slice_width, slice_width)
    x_slice = lax.dynamic_slice_in_dim(x_mine, tp_rank * slice_width, slice_width, 1)
    output = x_slice.astype(f32) + summed_out + out_shift

    def reduce_weight(grad):
        mine = plane.scatter_sum(grad.astype(bf16))
        rows, columns = mine.shape
        whole = jnp.zeros((rows, columns * ctx_count), f32)
        for k in range(ctx_count):
            part = mine if k == 0 else ring_shift(mine.astype(bf16), "ctx", ctx_count - k)
            place = lax.rem(ctx_rank + k, ctx_count) * columns
            whole = lax.dynamic_update_slice_in_dim(whole, part.astype(f32), place, 1)
        return whole

    bias_grad = jnp.sum(g_row.astype(f32), axis=0)
    down_grad = reduce_weight(contract_first(g_row, hidden))
    pre_grad = jnp.dot(g_row, w_down, preferred_element_type=f32) * slope
    up_bias_grad = jnp.sum(pre_grad, axis=0)
    pre_grad_b = pre_grad.astype(bf16)
    up_grad = reduce_weight(contract_first(acts_two, pre_grad_b))
    norm_two_grad = contract_last(pre_grad_b, w_up)

    dense_grad = reduce_weight(contract_first(g_row, attn))
    attn_grad = jnp.dot(g_row, w_dense, preferred_element_type=f32).astype(bf16)
    proj_parts, sum_parts = [], []
    for h, (query, key, value, attn_head, lse) in enumerate(heads):
        part, sums = attend_grad(
            own_order,
            bounds,
            query,
            key,
            value,
            attn_head,
            attn_grad[:, HD * h : HD * (h + 1)],
            lse,
            tables,
            seg_col,
            seg_row,
            block_len,
            groups,
        )
        proj_parts.append(part)
        sum_parts.append(sums[0])
    proj_grad_b = jnp.concatenate(proj_parts, axis=1)
    qkv_bias_grad = jnp.concatenate(sum_parts)
    qkv_grad = reduce_weight(contract_first(acts_one, proj_grad_b))
    norm_one_grad = contract_last(proj_grad_b, w_qkv)

    scaled = norm_one_grad * gain_one + norm_two_grad * gain_two
    inner = (
        scaled
        - jnp.mean(scaled, axis=-1, keepdims=True)
        - hat * jnp.mean(scaled * hat, axis=-1, keepdims=True)
    )
    input_sum = reduce_partial(inverse * inner)
    g_slice = lax.dynamic_slice_in_dim(g_mine, tp_rank * slice_width, slice_width, 1)
    input_grad = g_slice.astype(f32) + input_sum

    norm_sums = jnp.concatenate(
        [
            jnp.sum(norm_one_grad * hat, axis=0),
            jnp.sum(norm_one_grad, axis=0),
            jnp.sum(norm_two_grad * hat, axis=0),
            jnp.sum(norm_two_grad, axis=0),
        ]
    )
    column_sums = [up_bias_grad, qkv_bias_grad]
    packed = jnp.concatenate([norm_sums] + column_sums)
    wholes = [jnp.zeros((v.shape[0] * ctx_count,), f32) for v in column_sums]
    total = jnp.zeros_like(norm_sums)
    for k in range(ctx_count):
        part = packed if k == 0 else ring_shift(packed, "ctx", ctx_count - k)
        total = total + part[: norm_sums.shape[0]]
        offset = norm_sums.shape[0]
        for number, vector in enumerate(column_sums):
            size = vector.shape[0]
            wholes[number] = lax.dynamic_update_slice_in_dim(
                wholes[number],
                part[offset : offset + size],
                lax.rem(ctx_rank + k, ctx_count) * size,
                0,
            )
            offset += size
    norm_sums = total
    for k in range(1, tp_count):
        norm_sums = norm_sums + ring_shift(total, "tp", k)
    pieces = [bias_grad] + wholes + [
        norm_sums[k * width : (k + 1) * width] for k in range(4)
    ]
    reduced = plane.full_sum(jnp.concatenate(pieces))
    results, offset = [], 0
    for piece in pieces:
        own = piece.shape[0] // shard_count
        results.append(lax.dynamic_slice_in_dim(reduced, offset + shard_rank * own, own))
        offset += piece.shape[0]
    bias_grad, up_bias_grad, qkv_bias_grad = results[:3]
    gain_one_grad, shift_one_grad, gain_two_grad, shift_two_grad = results[3:]
    out_shape = hidden_in.shape[:3] + (slice_width,)
    return (
        output.reshape(out_shape),
        input_grad.reshape(out_shape),
        gain_one_grad,
        shift_one_grad,
        qkv_grad,
        qkv_bias_grad[None],
        dense_grad,
        bias_grad,
        gain_two_grad,
        shift_two_grad,
        up_grad,
        up_bias_grad[None],
        down_grad,
    )


def solution(mesh):
    return jax.shard_map(
        local,
        mesh=mesh,
        in_specs=(
            P("shard", "ctx", None, None),
            P("shard", "ctx", None, None),
            P("shard", None),
            P(),
            P("shard"),
            P("shard"),
            P("shard", "tp"),
            P("tp", "shard"),
            P("shard", "tp"),
            P("shard"),
            P("shard"),
            P("shard"),
            P("shard", "tp"),
            P("tp", "shard"),
            P("shard", "tp"),
            P("shard"),
        ),
        out_specs=(
            P("shard", "ctx", None, "tp"),
            P("shard", "ctx", None, "tp"),
            P("shard"),
            P("shard"),
            P("shard", "tp"),
            P("tp", "shard"),
            P("shard", "tp"),
            P("shard"),
            P("shard"),
            P("shard"),
            P("shard", "tp"),
            P("tp", "shard"),
            P("shard", "tp"),
        ),
        check_vma=False,
    )
```

```python
import functools
import math

import jax
import jax.numpy as jnp
from jax import lax
from jax.experimental import pallas as pl
from jax.experimental.pallas import tpu as pltpu
from jax.sharding import PartitionSpec as P

HD = 256
ROT = 64
LANES = 128

EPSILON = 1e-05
ROTARY_BASE = 10000.0
NEG = -1e30
VMEM_LIMIT = 56 * 1024 * 1024


def segment_positions(segments):
    length_all = segments.shape[0]
    index_row = jnp.arange(length_all, dtype=jnp.int32)
    changed = jnp.concatenate(
        [jnp.ones((1,), dtype=jnp.bool_), segments[1:] != segments[:-1]]
    )
    seg_start = jnp.where(changed, index_row, jnp.zeros_like(segments))
    return index_row - lax.cummax(seg_start, axis=0)


def rotary_tables(positions):
    half_rot = ROT // 2
    frequency = ROTARY_BASE ** (-2.0 * jnp.arange(half_rot, dtype=jnp.float32) / ROT)
    angles = positions.astype(jnp.float32)[:, None] * frequency[None, :]
    cosine, sine = jnp.cos(angles), jnp.sin(angles)
    count = positions.shape[0]
    rest_one = jnp.ones((count, LANES - ROT), jnp.float32)
    rest_zero = jnp.zeros((count, LANES - half_rot), jnp.float32)
    cosine_table = jnp.concatenate([cosine, cosine, rest_one], axis=1)
    low_table = jnp.concatenate([-sine, rest_zero], axis=1)
    high_table = jnp.concatenate(
        [jnp.zeros_like(sine), sine, rest_zero[:, : LANES - ROT]], axis=1
    )
    return cosine_table, low_table, high_table


def turn(values, cosine, low, high, sign):
    half_rot = ROT // 2
    down = pltpu.roll(values, LANES - half_rot, 1)
    up = pltpu.roll(values, half_rot, 1)
    return values * cosine + sign * (down * low + up * high)


def contract_first(left_mat, right_mat):
    return lax.dot_general(
        left_mat, right_mat, (((0,), (0,)), ((), ())), preferred_element_type=jnp.float32
    )


def contract_last(left_mat, right_mat):
    return lax.dot_general(
        left_mat, right_mat, (((1,), (1,)), ((), ())), preferred_element_type=jnp.float32
    )


def block_meets(bounds_ref, order_ref, q_index, k_index):
    return (
        (order_ref[k_index] <= order_ref[q_index])
        & (bounds_ref[0, k_index] <= bounds_ref[1, q_index])
        & (bounds_ref[1, k_index] >= bounds_ref[0, q_index])
    )


def pair_mask(order_ref, seg_col_ref, seg_row_ref, q_index, k_index, block):
    q_place = order_ref[q_index] * block + lax.broadcasted_iota(jnp.int32, (block, block), 0)
    k_place = order_ref[k_index] * block + lax.broadcasted_iota(jnp.int32, (block, block), 1)
    seg_q = seg_col_ref[pl.ds(q_index * block, block), :]
    seg_k = seg_row_ref[:, pl.ds(pl.multiple_of(k_index * block, block), block)]
    return (k_place <= q_place) & (seg_q == seg_k)


def attend_kernel(
    order_ref,
    bounds_ref,
    proj_ref,
    cos_ref,
    low_ref,
    high_ref,
    seg_col_ref,
    seg_row_ref,
    query_ref,
    key_ref,
    value_ref,
    attn_ref,
    lse_ref,
    top_ref,
    sum_ref,
    acc_ref,
    *,
    block,
    count,
):
    score_scale = 1.0 / math.sqrt(HD)
    for index in range(count):
        rows = pl.ds(index * block, block)
        tables = (cos_ref[rows, :], low_ref[rows, :], high_ref[rows, :])
        for start, out in ((0, query_ref), (HD, key_ref)):
            out[rows, :LANES] = turn(
                proj_ref[rows, start : start + LANES], *tables, 1.0
            ).astype(jnp.bfloat16)
            out[rows, LANES:] = proj_ref[rows, start + LANES : start + HD].astype(jnp.bfloat16)
        value_ref[rows, :] = proj_ref[rows, 2 * HD :].astype(jnp.bfloat16)

    @pl.loop(0, count)
    def _(q_index):
        rows = pl.ds(pl.multiple_of(q_index * block, block), block)
        top_ref[...] = jnp.full_like(top_ref, NEG)
        sum_ref[...] = jnp.zeros_like(sum_ref)
        acc_ref[...] = jnp.zeros_like(acc_ref)

        @pl.loop(0, count)
        def _(k_index):
            @pl.when(block_meets(bounds_ref, order_ref, q_index, k_index))
            def _():
                keys = pl.ds(pl.multiple_of(k_index * block, block), block)
                scores = contract_last(query_ref[rows, :], key_ref[keys, :]) * score_scale
                allowed = pair_mask(order_ref, seg_col_ref, seg_row_ref, q_index, k_index, block)
                scores = jnp.where(allowed, scores, NEG)
                old_top = top_ref[...]
                new_top = jnp.maximum(old_top, jnp.max(scores, axis=1, keepdims=True))
                shrink = jnp.exp(old_top - new_top)
                weights = jnp.where(allowed, jnp.exp(scores - new_top), 0.0)
                top_ref[...] = new_top
                sum_ref[...] = sum_ref[...] * shrink + jnp.sum(weights, axis=1, keepdims=True)
                acc_ref[...] = acc_ref[...] * shrink + jnp.dot(
                    weights.astype(jnp.bfloat16),
                    value_ref[keys, :],
                    preferred_element_type=jnp.float32,
                )

        attn_ref[rows, :] = (acc_ref[...] / sum_ref[...]).astype(jnp.bfloat16)
        lse_ref[rows, :] = top_ref[...] + jnp.log(sum_ref[...])


def attend_grad_kernel(
    order_ref,
    bounds_ref,
    query_ref,
    key_ref,
    value_ref,
    attn_ref,
    grad_ref,
    lse_ref,
    cos_ref,
    low_ref,
    high_ref,
    seg_col_ref,
    seg_row_ref,
    out_ref,
    sums_ref,
    query_acc,
    key_acc,
    value_acc,
    delta_ref,
    *,
    block,
    count,
):
    score_scale = 1.0 / math.sqrt(HD)
    query_acc[...] = jnp.zeros_like(query_acc)
    delta_ref[...] = jnp.sum(
        grad_ref[...].astype(jnp.float32) * attn_ref[...].astype(jnp.float32),
        axis=1,
        keepdims=True,
    )

    @pl.loop(0, count)
    def _(k_index):
        keys = pl.ds(pl.multiple_of(k_index * block, block), block)
        key_acc[...] = jnp.zeros_like(key_acc)
        value_acc[...] = jnp.zeros_like(value_acc)

        @pl.loop(0, count)
        def _(q_index):
            @pl.when(block_meets(bounds_ref, order_ref, q_index, k_index))
            def _():
                rows = pl.ds(pl.multiple_of(q_index * block, block), block)
                query, key_rows = query_ref[rows, :], key_ref[keys, :]
                grad_rows = grad_ref[rows, :]
                scores = contract_last(query, key_rows) * score_scale
                allowed = pair_mask(order_ref, seg_col_ref, seg_row_ref, q_index, k_index, block)
                probs = jnp.where(allowed, jnp.exp(scores - lse_ref[rows, :]), 0.0)
                prob_grad = contract_last(grad_rows, value_ref[keys, :])
                score_grad = (probs * (prob_grad - delta_ref[rows, :])).astype(jnp.bfloat16)
                value_acc[...] += contract_first(probs.astype(jnp.bfloat16), grad_rows)
                key_acc[...] += contract_first(score_grad, query)
                query_acc[rows, :] += jnp.dot(
                    score_grad, key_rows, preferred_element_type=jnp.float32
                )

        tables = (cos_ref[keys, :], low_ref[keys, :], high_ref[keys, :])
        key_low = turn(key_acc[:, :LANES] * score_scale, *tables, -1.0)
        key_high = key_acc[:, LANES:] * score_scale
        first = k_index == 0
        for start, part in ((HD, key_low), (HD + LANES, key_high), (2 * HD, value_acc[...])):
            columns = slice(start, start + part.shape[1])
            out_ref[keys, columns] = part.astype(jnp.bfloat16)
            sums_ref[:, columns] = jnp.where(first, 0.0, sums_ref[:, columns]) + jnp.sum(
                part, axis=0, keepdims=True
            )

    sums_ref[:, :HD] = jnp.zeros((1, HD), jnp.float32)

    @pl.loop(0, count)
    def _(q_index):
        rows = pl.ds(pl.multiple_of(q_index * block, block), block)
        tables = (cos_ref[rows, :], low_ref[rows, :], high_ref[rows, :])
        query_low = turn(query_acc[rows, :LANES] * score_scale, *tables, -1.0)
        query_high = query_acc[rows, LANES:] * score_scale
        for start, part in ((0, query_low), (LANES, query_high)):
            columns = slice(start, start + part.shape[1])
            out_ref[rows, columns] = part.astype(jnp.bfloat16)
            sums_ref[:, columns] += jnp.sum(part, axis=0, keepdims=True)


def pair_product_kernel(left_ref, right_ref, left_weight, right_weight, out_ref):
    out_ref[...] = (
        contract_last(left_ref[...], left_weight[...])
        + contract_last(right_ref[...], right_weight[...])
    ).astype(out_ref.dtype)


def norm_grad_kernel(
    left_ref,
    right_ref,
    x_ref,
    left_weight,
    right_weight,
    left_gain,
    right_gain,
    after_ref,
    out_ref,
    sums_ref,
):
    del after_ref
    x = x_ref[...].astype(jnp.float32)
    centered = x - jnp.mean(x, axis=-1, keepdims=True)
    inverse = lax.rsqrt(jnp.mean(centered * centered, axis=-1, keepdims=True) + EPSILON)
    hat = centered * inverse
    left = contract_last(left_ref[...], left_weight[...])
    right = contract_last(right_ref[...], right_weight[...])
    scaled = left * left_gain[...] + right * right_gain[...]
    first = pl.program_id(0) == 0
    for row, part in enumerate((left * hat, left, right * hat, right)):
        total = jnp.sum(part, axis=0, keepdims=True)
        sums_ref[row : row + 1, :] = jnp.where(first, 0.0, sums_ref[row : row + 1, :]) + total
    inner = (
        scaled
        - jnp.mean(scaled, axis=-1, keepdims=True)
        - hat * jnp.mean(scaled * hat, axis=-1, keepdims=True)
    )
    out_ref[...] = (inverse * inner).astype(out_ref.dtype)


ROWS_STEP = 256


def row_specs(arrays, start, rows):
    step = min(ROWS_STEP, rows)
    return step, [
        pl.BlockSpec((step, v.shape[1]), lambda i, first=start // step: (first + i, 0))
        for v in arrays
    ]


def whole_spec(array):
    return pl.BlockSpec(array.shape, lambda i: (0, 0))


def pair_product(left, right, left_weight, right_weight, start, rows):
    step, specs = row_specs((left, right), start, rows)
    width = left_weight.shape[0]
    return pl.pallas_call(
        pair_product_kernel,
        grid=(rows // step,),
        out_shape=jax.ShapeDtypeStruct((rows, width), jnp.bfloat16),
        in_specs=specs + [whole_spec(left_weight), whole_spec(right_weight)],
        out_specs=pl.BlockSpec((step, width), lambda i: (i, 0)),
        compiler_params=pltpu.CompilerParams(vmem_limit_bytes=VMEM_LIMIT),
        cost_estimate=pl.CostEstimate(
            flops=2 * rows * width * (left.shape[1] + right.shape[1]),
            bytes_accessed=2 * rows * (width + left.shape[1] + right.shape[1]),
            transcendentals=0,
        ),
        name="pair_product",
    )(left, right, left_weight, right_weight)


def norm_grad(
    left, right, x, left_weight, right_weight, left_gain, right_gain, after, start, rows
):
    step, specs = row_specs((left, right, x), start, rows)
    width = left_weight.shape[0]
    rest = [left_weight, right_weight, left_gain, right_gain]
    return pl.pallas_call(
        norm_grad_kernel,
        grid=(rows // step,),
        out_shape=(
            jax.ShapeDtypeStruct((rows, width), jnp.bfloat16),
            jax.ShapeDtypeStruct((4, width), jnp.float32),
        ),
        in_specs=specs + [whole_spec(v) for v in rest] + [pl.BlockSpec(memory_space=pl.ANY)],
        out_specs=(
            pl.BlockSpec((step, width), lambda i: (i, 0)),
            pl.BlockSpec((4, width), lambda i: (0, 0)),
        ),
        compiler_params=pltpu.CompilerParams(vmem_limit_bytes=VMEM_LIMIT),
        cost_estimate=pl.CostEstimate(
            flops=2 * rows * width * (left.shape[1] + right.shape[1]),
            bytes_accessed=2 * rows * (2 * width + left.shape[1] + right.shape[1]),
            transcendentals=0,
        ),
        name="norm_grad",
    )(left, right, x, *rest, after)


SCALAR = pl.BlockSpec(memory_space=pltpu.SMEM)
VECTOR = pl.BlockSpec(memory_space=pltpu.VMEM)


def attend(order, bounds, proj, tables, seg_col, seg_row, block, count):
    length = proj.shape[0]
    pairs = length * length
    return pl.pallas_call(
        functools.partial(attend_kernel, block=block, count=count),
        out_shape=(
            jax.ShapeDtypeStruct((length, HD), jnp.bfloat16),
            jax.ShapeDtypeStruct((length, HD), jnp.bfloat16),
            jax.ShapeDtypeStruct((length, HD), jnp.bfloat16),
            jax.ShapeDtypeStruct((length, HD), jnp.bfloat16),
            jax.ShapeDtypeStruct((length, 1), jnp.float32),
        ),
        in_specs=[SCALAR] * 2 + [VECTOR] * 6,
        out_specs=(VECTOR,) * 5,
        scratch_shapes=[
            pltpu.VMEM((block, 1), jnp.float32),
            pltpu.VMEM((block, 1), jnp.float32),
            pltpu.VMEM((block, HD), jnp.float32),
        ],
        compiler_params=pltpu.CompilerParams(vmem_limit_bytes=VMEM_LIMIT),
        cost_estimate=pl.CostEstimate(
            flops=2 * pairs * HD, bytes_accessed=16 * length * HD, transcendentals=pairs // 2
        ),
        name="attend",
    )(order, bounds, proj, *tables, seg_col, seg_row)


def attend_grad(
    order, bounds, query, key, value, attn, grad, lse, tables, seg_col, seg_row, block, count
):
    length = query.shape[0]
    pairs = length * length
    return pl.pallas_call(
        functools.partial(attend_grad_kernel, block=block, count=count),
        out_shape=(
            jax.ShapeDtypeStruct((length, 3 * HD), jnp.bfloat16),
            jax.ShapeDtypeStruct((1, 3 * HD), jnp.float32),
        ),
        in_specs=[SCALAR] * 2 + [VECTOR] * 11,
        out_specs=(VECTOR,) * 2,
        scratch_shapes=[
            pltpu.VMEM((length, HD), jnp.float32),
            pltpu.VMEM((block, HD), jnp.float32),
            pltpu.VMEM((block, HD), jnp.float32),
            pltpu.VMEM((length, 1), jnp.float32),
        ],
        compiler_params=pltpu.CompilerParams(vmem_limit_bytes=VMEM_LIMIT),
        cost_estimate=pl.CostEstimate(
            flops=5 * pairs * HD, bytes_accessed=16 * length * HD, transcendentals=pairs // 2
        ),
        name="attend_grad",
    )(order, bounds, query, key, value, attn, grad, lse, *tables, seg_col, seg_row)


def ring_shift(value, axis, step):
    count = lax.axis_size(axis)
    return lax.ppermute(value, axis, [(i, (i + step) % count) for i in range(count)])


class Plane:
    def __init__(self):
        self.count = lax.axis_size("shard")
        side = math.isqrt(self.count)
        self.square = side * side == self.count
        self.first, self.second = (side, side) if self.square else (1, self.count)
        self.ranks = lax.axis_size("ctx")
        shard = lax.axis_index("shard")
        self.flip = (lax.axis_index("ctx") % 2 == 1) if self.square else False
        slow, fast = shard // self.second, shard % self.second
        if self.square:
            self.here = (jnp.where(self.flip, slow, fast), jnp.where(self.flip, fast, slow))
        else:
            self.here = (slow, fast)

    def index(self, first_step, second_step):
        first = lax.rem(self.here[0] + first_step + self.first, self.first)
        second = lax.rem(self.here[1] + second_step + self.second, self.second)
        if not self.square:
            return first * self.second + second
        side = self.first
        return jnp.where(self.flip, first * side + second, second * side + first)

    def move(self, value, first_step, second_step):
        pairs = []
        for shard in range(self.count):
            for rank in range(self.ranks):
                slow, fast = divmod(shard, self.second)
                if self.square and rank % 2 == 0:
                    slow = (slow + second_step) % self.second
                    fast = (fast + first_step) % self.first
                else:
                    slow = (slow + first_step) % self.first
                    fast = (fast + second_step) % self.second
                target = slow * self.second + fast
                pairs.append((shard * self.ranks + rank, target * self.ranks + rank))
        return lax.ppermute(value, ("shard", "ctx"), pairs)

    def gather(self, own):
        blocks = {(0, 0): own}
        for a in range(1, self.first):
            blocks[a, 0] = self.move(own, a, 0)
        for b in range(1, self.second):
            for a in range(self.first):
                blocks[a, b] = self.move(blocks[a, 0], 0, b)
        rows = own.shape[0]
        whole = jnp.zeros((rows * self.count,) + own.shape[1:], own.dtype)
        for (a, b), block in blocks.items():
            whole = lax.dynamic_update_slice_in_dim(whole, block, self.index(-a, -b) * rows, 0)
        return whole

    def scatter_sum(self, partial):
        rows = partial.shape[0] // self.count

        def block(a, b):
            return lax.dynamic_slice_in_dim(partial, self.index(a, b) * rows, rows)

        sums = {}
        for b in list(range(1, self.second)) + [0]:
            sums[b] = block(0, b).astype(jnp.float32)
            for a in range(1, self.first):
                sums[b] = sums[b] + self.move(block(a, b), a, 0).astype(jnp.float32)
        total = sums[0]
        for b in range(1, self.second):
            total = total + self.move(sums[b].astype(partial.dtype), 0, b).astype(jnp.float32)
        return total

    def full_sum(self, value):
        total = value
        for a in range(1, self.first):
            total = total + self.move(value, a, 0)
        value = total
        for b in range(1, self.second):
            total = total + self.move(value, 0, b)
        return total


def local(
    hidden_in,
    grad_out,
    segment_ids,
    group_order,
    ln1_gain,
    ln1_bias,
    qkv_weight,
    qkv_bias,
    dense_weight,
    dense_bias,
    ln2_gain,
    ln2_bias,
    up_weight,
    up_bias,
    down_weight,
    down_bias,
):
    _, groups_dev, block_len, width = hidden_in.shape
    tokens = groups_dev * block_len
    seq_len = segment_ids.shape[1]
    groups = seq_len // block_len
    ctx_count, tp_count = lax.axis_size("ctx"), lax.axis_size("tp")
    shard_count = lax.axis_size("shard")
    ctx_rank, tp_rank = lax.axis_index("ctx"), lax.axis_index("tp")
    shard_rank = lax.axis_index("shard")
    slice_width = width // tp_count
    bf16, f32 = jnp.bfloat16, jnp.float32

    def my_columns(matrix):
        columns = matrix.shape[1] // ctx_count
        return lax.dynamic_slice_in_dim(matrix, ctx_rank * columns, columns, 1)

    plane = Plane()

    def gather_rows(matrix):
        return plane.gather(my_columns(matrix))

    def whole_row(part):
        return jnp.concatenate(
            [part] + [ring_shift(part, "ctx", ctx_count - k) for k in range(1, ctx_count)], axis=0
        )

    x_mine = hidden_in.reshape(tokens, width)
    g_mine = grad_out.reshape(tokens, width)
    x_row = whole_row(x_mine)
    g_row = whole_row(g_mine)

    vectors = [
        ln1_gain, ln1_bias, ln2_gain, ln2_bias, dense_bias, down_bias, qkv_bias[0], up_bias[0],
    ]
    sizes = [v.shape[0] for v in vectors]
    packed = plane.gather(jnp.concatenate(vectors)[None])
    spread, offset = [], 0
    for size in sizes:
        spread.append(packed[:, offset : offset + size].reshape(-1).astype(f32))
        offset += size
    gain_one, shift_one, gain_two, shift_two, bias_dense, bias_down, bias_qkv, bias_up = spread
    bias_qkv = my_columns(bias_qkv[None])
    bias_up = my_columns(bias_up[None])

    w_qkv = gather_rows(qkv_weight)
    w_dense = gather_rows(dense_weight)
    w_up = lax.all_gather(my_columns(up_weight), "shard", axis=0, tiled=True)
    w_down = lax.all_gather(my_columns(down_weight), "shard", axis=0, tiled=True)
    heads_here = w_qkv.shape[1] // (3 * HD)

    own_order = jnp.concatenate(
        [
            lax.dynamic_slice_in_dim(
                group_order, lax.rem(ctx_rank + k, ctx_count) * groups_dev, groups_dev
            )
            for k in range(ctx_count)
        ]
    )
    segments = segment_ids[0]
    positions = segment_positions(segments)

    def stored(values):
        return jnp.concatenate(
            [
                lax.dynamic_slice_in_dim(values, own_order[k] * block_len, block_len)
                for k in range(groups)
            ]
        )

    seg_stored = stored(segments)
    tables = rotary_tables(stored(positions))
    seg_blocks = seg_stored.reshape(groups, block_len)
    bounds = jnp.stack([seg_blocks[:, 0], seg_blocks[:, -1]])
    seg_col, seg_row = seg_stored[:, None], seg_stored[None, :]

    x_float = x_row.astype(f32)
    centered = x_float - jnp.mean(x_float, axis=-1, keepdims=True)
    inverse = lax.rsqrt(jnp.mean(centered * centered, axis=-1, keepdims=True) + EPSILON)
    hat = centered * inverse
    acts_one = (hat * gain_one + shift_one).astype(bf16)
    acts_two = (hat * gain_two + shift_two).astype(bf16)

    projected = jnp.dot(acts_one, w_qkv, preferred_element_type=f32) + bias_qkv
    heads = []
    for h in range(heads_here):
        heads.append(
            attend(
                own_order,
                bounds,
                projected[:, 3 * HD * h : 3 * HD * (h + 1)],
                tables,
                seg_col,
                seg_row,
                block_len,
                groups,
            )
        )
    attn = jnp.concatenate([head[3] for head in heads], axis=1)

    attn_grad = jnp.dot(g_row, w_dense, preferred_element_type=f32).astype(bf16)
    proj_parts, sum_parts = [], []
    for h, (query, key, value, attn_head, lse) in enumerate(heads):
        part, sums = attend_grad(
            own_order,
            bounds,
            query,
            key,
            value,
            attn_head,
            attn_grad[:, HD * h : HD * (h + 1)],
            lse,
            tables,
            seg_col,
            seg_row,
            block_len,
            groups,
        )
        proj_parts.append(part)
        sum_parts.append(sums[0])
    proj_grad_b = jnp.concatenate(proj_parts, axis=1)
    qkv_bias_grad = jnp.concatenate(sum_parts)

    pre_act = jnp.dot(acts_two, w_up, preferred_element_type=f32) + bias_up
    cdf = 0.5 * (1.0 + lax.erf(pre_act * (1.0 / math.sqrt(2.0))))
    hidden = (pre_act * cdf).astype(bf16)
    slope = cdf + pre_act * jnp.exp(-0.5 * pre_act * pre_act) * (1.0 / math.sqrt(2.0 * math.pi))

    def reduce_partial(parts):
        total = parts[0].astype(f32)
        for k in range(1, ctx_count):
            total = total + ring_shift(parts[k], "ctx", k).astype(f32)
        total = total.astype(bf16)
        return total, lax.psum_scatter(total, "tp", scatter_dimension=1, tiled=True).astype(f32)

    out_parts = {}
    for k in reversed(range(ctx_count)):
        out_parts[k] = pair_product(attn, hidden, w_dense, w_down, k * tokens, tokens)
    out_total, summed_out = reduce_partial(out_parts)
    out_shift = lax.dynamic_slice_in_dim(bias_dense + bias_down, tp_rank * slice_width, slice_width)
    x_slice = lax.dynamic_slice_in_dim(x_mine, tp_rank * slice_width, slice_width, 1)
    output = x_slice.astype(f32) + summed_out + out_shift

    def reduce_weight(grad):
        mine = plane.scatter_sum(grad.astype(bf16))
        rows, columns = mine.shape
        whole = jnp.zeros((rows, columns * ctx_count), f32)
        for k in range(ctx_count):
            part = mine if k == 0 else ring_shift(mine.astype(bf16), "ctx", ctx_count - k)
            place = lax.rem(ctx_rank + k, ctx_count) * columns
            whole = lax.dynamic_update_slice_in_dim(whole, part.astype(f32), place, 1)
        return whole

    bias_grad = jnp.sum(g_row.astype(f32), axis=0)
    dense_grad = reduce_weight(contract_first(g_row, attn))
    qkv_grad = reduce_weight(contract_first(acts_one, proj_grad_b))

    pre_grad = jnp.dot(g_row, w_down, preferred_element_type=f32) * slope
    up_bias_grad = jnp.sum(pre_grad, axis=0)
    pre_grad_b = pre_grad.astype(bf16)

    in_parts, norm_sums = {}, jnp.zeros((4, width), f32)
    for k in reversed(range(ctx_count)):
        in_parts[k], sums = norm_grad(
            proj_grad_b,
            pre_grad_b,
            x_row,
            w_qkv,
            w_up,
            gain_one[None],
            gain_two[None],
            out_total,
            k * tokens,
            tokens,
        )
        norm_sums = norm_sums + sums
    _, input_sum = reduce_partial(in_parts)
    g_slice = lax.dynamic_slice_in_dim(g_mine, tp_rank * slice_width, slice_width, 1)
    input_grad = g_slice.astype(f32) + input_sum

    down_grad = reduce_weight(contract_first(g_row, hidden))
    up_grad = reduce_weight(contract_first(acts_two, pre_grad_b))

    norm_sums = norm_sums.reshape(-1)
    column_sums = [up_bias_grad, qkv_bias_grad]
    packed = jnp.concatenate([norm_sums] + column_sums)
    wholes = [jnp.zeros((v.shape[0] * ctx_count,), f32) for v in column_sums]
    total = jnp.zeros_like(norm_sums)
    for k in range(ctx_count):
        part = packed if k == 0 else ring_shift(packed, "ctx", ctx_count - k)
        total = total + part[: norm_sums.shape[0]]
        offset = norm_sums.shape[0]
        for number, vector in enumerate(column_sums):
            size = vector.shape[0]
            wholes[number] = lax.dynamic_update_slice_in_dim(
                wholes[number],
                part[offset : offset + size],
                lax.rem(ctx_rank + k, ctx_count) * size,
                0,
            )
            offset += size
    norm_sums = total
    for k in range(1, tp_count):
        norm_sums = norm_sums + ring_shift(total, "tp", k)
    pieces = [bias_grad] + wholes + [
        norm_sums[k * width : (k + 1) * width] for k in range(4)
    ]
    reduced = plane.full_sum(jnp.concatenate(pieces))
    results, offset = [], 0
    for piece in pieces:
        own = piece.shape[0] // shard_count
        results.append(lax.dynamic_slice_in_dim(reduced, offset + shard_rank * own, own))
        offset += piece.shape[0]
    bias_grad, up_bias_grad, qkv_bias_grad = results[:3]
    gain_one_grad, shift_one_grad, gain_two_grad, shift_two_grad = results[3:]
    out_shape = hidden_in.shape[:3] + (slice_width,)
    return (
        output.reshape(out_shape),
        input_grad.reshape(out_shape),
        gain_one_grad,
        shift_one_grad,
        qkv_grad,
        qkv_bias_grad[None],
        dense_grad,
        bias_grad,
        gain_two_grad,
        shift_two_grad,
        up_grad,
        up_bias_grad[None],
        down_grad,
    )


def solution(mesh):
    return jax.shard_map(
        local,
        mesh=mesh,
        in_specs=(
            P("shard", "ctx", None, None),
            P("shard", "ctx", None, None),
            P("shard", None),
            P(),
            P("shard"),
            P("shard"),
            P("shard", "tp"),
            P("tp", "shard"),
            P("shard", "tp"),
            P("shard"),
            P("shard"),
            P("shard"),
            P("shard", "tp"),
            P("tp", "shard"),
            P("shard", "tp"),
            P("shard"),
        ),
        out_specs=(
            P("shard", "ctx", None, "tp"),
            P("shard", "ctx", None, "tp"),
            P("shard"),
            P("shard"),
            P("shard", "tp"),
            P("tp", "shard"),
            P("shard", "tp"),
            P("shard"),
            P("shard"),
            P("shard"),
            P("shard", "tp"),
            P("tp", "shard"),
            P("shard", "tp"),
        ),
        check_vma=False,
    )
```

```python
import functools
import math

import jax
import jax.numpy as jnp
from jax import lax
from jax.experimental import pallas as pl
from jax.experimental.pallas import tpu as pltpu
from jax.sharding import PartitionSpec as P

HD = 256
ROT = 64
LANES = 128

EPSILON = 1e-05
ROTARY_BASE = 10000.0
NEG = -1e30
VMEM_LIMIT = 56 * 1024 * 1024


def segment_positions(segments):
    length_all = segments.shape[0]
    index_row = jnp.arange(length_all, dtype=jnp.int32)
    changed = jnp.concatenate(
        [jnp.ones((1,), dtype=jnp.bool_), segments[1:] != segments[:-1]]
    )
    seg_start = jnp.where(changed, index_row, jnp.zeros_like(segments))
    return index_row - lax.cummax(seg_start, axis=0)


def rotary_tables(positions):
    half_rot = ROT // 2
    frequency = ROTARY_BASE ** (-2.0 * jnp.arange(half_rot, dtype=jnp.float32) / ROT)
    angles = positions.astype(jnp.float32)[:, None] * frequency[None, :]
    cosine, sine = jnp.cos(angles), jnp.sin(angles)
    count = positions.shape[0]
    rest_one = jnp.ones((count, LANES - ROT), jnp.float32)
    rest_zero = jnp.zeros((count, LANES - half_rot), jnp.float32)
    cosine_table = jnp.concatenate([cosine, cosine, rest_one], axis=1)
    low_table = jnp.concatenate([-sine, rest_zero], axis=1)
    high_table = jnp.concatenate(
        [jnp.zeros_like(sine), sine, rest_zero[:, : LANES - ROT]], axis=1
    )
    return cosine_table, low_table, high_table


def turn(values, cosine, low, high, sign):
    half_rot = ROT // 2
    down = pltpu.roll(values, LANES - half_rot, 1)
    up = pltpu.roll(values, half_rot, 1)
    return values * cosine + sign * (down * low + up * high)


def contract_first(left_mat, right_mat):
    return lax.dot_general(
        left_mat, right_mat, (((0,), (0,)), ((), ())), preferred_element_type=jnp.float32
    )


def contract_last(left_mat, right_mat):
    return lax.dot_general(
        left_mat, right_mat, (((1,), (1,)), ((), ())), preferred_element_type=jnp.float32
    )


def block_meets(bounds_ref, order_ref, q_index, k_index):
    return (
        (order_ref[k_index] <= order_ref[q_index])
        & (bounds_ref[0, k_index] <= bounds_ref[1, q_index])
        & (bounds_ref[1, k_index] >= bounds_ref[0, q_index])
    )


def pair_mask(order_ref, seg_col_ref, seg_row_ref, q_index, k_index, block):
    q_place = order_ref[q_index] * block + lax.broadcasted_iota(jnp.int32, (block, block), 0)
    k_place = order_ref[k_index] * block + lax.broadcasted_iota(jnp.int32, (block, block), 1)
    seg_q = seg_col_ref[pl.ds(q_index * block, block), :]
    seg_k = seg_row_ref[:, pl.ds(pl.multiple_of(k_index * block, block), block)]
    return (k_place <= q_place) & (seg_q == seg_k)


def attend_kernel(
    order_ref,
    bounds_ref,
    proj_ref,
    cos_ref,
    low_ref,
    high_ref,
    seg_col_ref,
    seg_row_ref,
    query_ref,
    key_ref,
    value_ref,
    attn_ref,
    lse_ref,
    top_ref,
    sum_ref,
    acc_ref,
    *,
    block,
    count,
):
    score_scale = 1.0 / math.sqrt(HD)
    for index in range(count):
        rows = pl.ds(index * block, block)
        tables = (cos_ref[rows, :], low_ref[rows, :], high_ref[rows, :])
        for start, out in ((0, query_ref), (HD, key_ref)):
            out[rows, :LANES] = turn(
                proj_ref[rows, start : start + LANES], *tables, 1.0
            ).astype(jnp.bfloat16)
            out[rows, LANES:] = proj_ref[rows, start + LANES : start + HD].astype(jnp.bfloat16)
        value_ref[rows, :] = proj_ref[rows, 2 * HD :].astype(jnp.bfloat16)

    @pl.loop(0, count)
    def _(q_index):
        rows = pl.ds(pl.multiple_of(q_index * block, block), block)
        top_ref[...] = jnp.full_like(top_ref, NEG)
        sum_ref[...] = jnp.zeros_like(sum_ref)
        acc_ref[...] = jnp.zeros_like(acc_ref)

        @pl.loop(0, count)
        def _(k_index):
            @pl.when(block_meets(bounds_ref, order_ref, q_index, k_index))
            def _():
                keys = pl.ds(pl.multiple_of(k_index * block, block), block)
                scores = contract_last(query_ref[rows, :], key_ref[keys, :]) * score_scale
                allowed = pair_mask(order_ref, seg_col_ref, seg_row_ref, q_index, k_index, block)
                scores = jnp.where(allowed, scores, NEG)
                old_top = top_ref[...]
                new_top = jnp.maximum(old_top, jnp.max(scores, axis=1, keepdims=True))
                shrink = jnp.exp(old_top - new_top)
                weights = jnp.where(allowed, jnp.exp(scores - new_top), 0.0)
                top_ref[...] = new_top
                sum_ref[...] = sum_ref[...] * shrink + jnp.sum(weights, axis=1, keepdims=True)
                acc_ref[...] = acc_ref[...] * shrink + jnp.dot(
                    weights.astype(jnp.bfloat16),
                    value_ref[keys, :],
                    preferred_element_type=jnp.float32,
                )

        attn_ref[rows, :] = (acc_ref[...] / sum_ref[...]).astype(jnp.bfloat16)
        lse_ref[rows, :] = top_ref[...] + jnp.log(sum_ref[...])


def attend_grad_kernel(
    order_ref,
    bounds_ref,
    query_ref,
    key_ref,
    value_ref,
    attn_ref,
    grad_ref,
    lse_ref,
    cos_ref,
    low_ref,
    high_ref,
    seg_col_ref,
    seg_row_ref,
    out_ref,
    sums_ref,
    query_acc,
    key_acc,
    value_acc,
    delta_ref,
    *,
    block,
    count,
):
    score_scale = 1.0 / math.sqrt(HD)
    query_acc[...] = jnp.zeros_like(query_acc)
    delta_ref[...] = jnp.sum(
        grad_ref[...].astype(jnp.float32) * attn_ref[...].astype(jnp.float32),
        axis=1,
        keepdims=True,
    )

    @pl.loop(0, count)
    def _(k_index):
        keys = pl.ds(pl.multiple_of(k_index * block, block), block)
        key_acc[...] = jnp.zeros_like(key_acc)
        value_acc[...] = jnp.zeros_like(value_acc)

        @pl.loop(0, count)
        def _(q_index):
            @pl.when(block_meets(bounds_ref, order_ref, q_index, k_index))
            def _():
                rows = pl.ds(pl.multiple_of(q_index * block, block), block)
                query, key_rows = query_ref[rows, :], key_ref[keys, :]
                grad_rows = grad_ref[rows, :]
                scores = contract_last(query, key_rows) * score_scale
                allowed = pair_mask(order_ref, seg_col_ref, seg_row_ref, q_index, k_index, block)
                probs = jnp.where(allowed, jnp.exp(scores - lse_ref[rows, :]), 0.0)
                prob_grad = contract_last(grad_rows, value_ref[keys, :])
                score_grad = (probs * (prob_grad - delta_ref[rows, :])).astype(jnp.bfloat16)
                value_acc[...] += contract_first(probs.astype(jnp.bfloat16), grad_rows)
                key_acc[...] += contract_first(score_grad, query)
                query_acc[rows, :] += jnp.dot(
                    score_grad, key_rows, preferred_element_type=jnp.float32
                )

        tables = (cos_ref[keys, :], low_ref[keys, :], high_ref[keys, :])
        key_low = turn(key_acc[:, :LANES] * score_scale, *tables, -1.0)
        key_high = key_acc[:, LANES:] * score_scale
        first = k_index == 0
        for start, part in ((HD, key_low), (HD + LANES, key_high), (2 * HD, value_acc[...])):
            columns = slice(start, start + part.shape[1])
            out_ref[keys, columns] = part.astype(jnp.bfloat16)
            sums_ref[:, columns] = jnp.where(first, 0.0, sums_ref[:, columns]) + jnp.sum(
                part, axis=0, keepdims=True
            )

    sums_ref[:, :HD] = jnp.zeros((1, HD), jnp.float32)

    @pl.loop(0, count)
    def _(q_index):
        rows = pl.ds(pl.multiple_of(q_index * block, block), block)
        tables = (cos_ref[rows, :], low_ref[rows, :], high_ref[rows, :])
        query_low = turn(query_acc[rows, :LANES] * score_scale, *tables, -1.0)
        query_high = query_acc[rows, LANES:] * score_scale
        for start, part in ((0, query_low), (LANES, query_high)):
            columns = slice(start, start + part.shape[1])
            out_ref[rows, columns] = part.astype(jnp.bfloat16)
            sums_ref[:, columns] += jnp.sum(part, axis=0, keepdims=True)


MESH = pl.DeviceIdType.MESH


def opening_kernel(*refs, side, second, ranks, square, sizes):
    count = len(sizes)
    gathered_in, refs = refs[:count], refs[count:]
    rows_in, refs = refs[:2], refs[2:]
    later_in, refs = refs[:2], refs[2:]
    gathered_out, refs = refs[:count], refs[count:]
    rows_out, refs = refs[:2], refs[2:]
    later_out, refs = refs[:2], refs[2:]
    held, refs = refs[:count], refs[count:]
    held_rows, refs = refs[:2], refs[2:]
    held_later, refs = refs[:2], refs[2:]
    load_sem, store_sem, send_sem, recv_sem, row_send, row_recv = refs

    shard, rank = lax.axis_index("shard"), lax.axis_index("ctx")
    slow, fast = shard // second, shard % second
    flip = rank % 2 if square else 1
    here_first = fast * (1 - flip) + slow * flip
    here_second = slow * (1 - flip) + fast * flip

    def peer(first_step, second_step):
        first = (here_first + first_step + side) % side
        other = (here_second + second_step + second) % second
        return (other * side + first) * (1 - flip) + (first * second + other) * flip

    first_peers = [peer(a, 0) for a in range(1, side)]
    second_peers = [peer(0, b) for b in range(1, second)]
    rank_peers = [(rank + j) % ranks for j in range(1, ranks)]
    barrier = pltpu.get_barrier_semaphore()
    for target in first_peers + second_peers:
        pl.semaphore_signal(barrier, inc=1, device_id={"shard": target}, device_id_type=MESH)
    for target in rank_peers:
        pl.semaphore_signal(barrier, inc=1, device_id={"ctx": target}, device_id_type=MESH)

    loads = []
    for number in range(count):
        source = gathered_in[number]
        if sizes[number] is not None:
            columns = pl.ds(pl.multiple_of(rank * sizes[number], LANES), sizes[number])
            source = source.at[:, columns]
        loads.append(pltpu.make_async_copy(source, held[number], load_sem.at[number]))
    for number in range(2):
        loads.append(
            pltpu.make_async_copy(rows_in[number], held_rows[number], load_sem.at[count + number])
        )
    for number in range(2):
        size = held_later[number].shape[1]
        columns = pl.ds(pl.multiple_of(rank * size, LANES), size)
        loads.append(
            pltpu.make_async_copy(
                later_in[number].at[:, columns], held_later[number], load_sem.at[count + 2 + number]
            )
        )
    for load in loads:
        load.start()
    pl.semaphore_wait(barrier, len(first_peers) + len(second_peers) + len(rank_peers))

    def place(number, first_step, second_step):
        rows = held[number].shape[0]
        start = pl.multiple_of(peer(first_step, second_step) * rows, 16)
        return gathered_out[number].at[pl.ds(start, rows), :]

    copies, slot = {}, 0
    steps = side - 1 + (second - 1) * side

    def send(number, source, a, b, target, key):
        slot = number * steps + key
        copy = pltpu.make_async_remote_copy(
            src_ref=source,
            dst_ref=place(number, a, b),
            send_sem=send_sem.at[slot],
            recv_sem=recv_sem.at[slot],
            device_id={"shard": target},
            device_id_type=MESH,
        )
        copy.start()
        copies[number, key] = copy

    for number in range(count):
        loads[number].wait()
        for a in range(1, side):
            send(number, held[number], 0, 0, first_peers[a - 1], a - 1)
        for b in range(1, second):
            send(number, held[number], 0, 0, second_peers[b - 1], side - 1 + (b - 1) * side)
    row_copies = []
    for number in range(2):
        loads[count + number].wait()
        rows = held_rows[number].shape[0]
        for j in range(1, ranks):
            slot = number * (ranks - 1) + j - 1
            copy = pltpu.make_async_remote_copy(
                src_ref=held_rows[number],
                dst_ref=rows_out[number].at[pl.ds((ranks - j) * rows, rows), :],
                send_sem=row_send.at[slot],
                recv_sem=row_recv.at[slot],
                device_id={"ctx": rank_peers[j - 1]},
                device_id_type=MESH,
            )
            copy.start()
            row_copies.append(copy)
    stores = []
    for number in range(count):
        stores.append(
            pltpu.make_async_copy(held[number], place(number, 0, 0), store_sem.at[number])
        )
    for number in range(2):
        rows = held_rows[number].shape[0]
        stores.append(
            pltpu.make_async_copy(
                held_rows[number],
                rows_out[number].at[pl.ds(0, rows), :],
                store_sem.at[count + number],
            )
        )
    for number in range(2):
        loads[count + 2 + number].wait()
        stores.append(
            pltpu.make_async_copy(
                held_later[number], later_out[number], store_sem.at[count + 2 + number]
            )
        )
    for store in stores:
        store.start()
    for number in range(count):
        for a in range(1, side):
            copies[number, a - 1].wait_recv()
            for b in range(1, second):
                key = side - 1 + (b - 1) * side + a
                send(number, place(number, -a, 0), -a, 0, second_peers[b - 1], key)
    for store in stores:
        store.wait()
    for (number, key), copy in copies.items():
        copy.wait_send()
        if key >= side - 1:
            copy.wait_recv()
    for copy in row_copies:
        copy.wait_send()
        copy.wait_recv()


def opening(gathered, split, rows, later, ranks):
    shards = lax.axis_size("shard")
    side = math.isqrt(shards)
    square = side * side == shards
    if not square:
        side = 1
    second = shards // side
    sizes = [v.shape[1] // ranks if cut else None for v, cut in zip(gathered, split)]
    held = [(v.shape[0], size or v.shape[1]) for v, size in zip(gathered, sizes)]
    held_later = [(v.shape[0], v.shape[1] // ranks) for v in later]
    count, steps = len(gathered), side - 1 + (second - 1) * side
    bf16 = jnp.bfloat16
    out_shapes = (
        [jax.ShapeDtypeStruct((h[0] * shards, h[1]), bf16) for h in held]
        + [jax.ShapeDtypeStruct((v.shape[0] * ranks, v.shape[1]), bf16) for v in rows]
        + [jax.ShapeDtypeStruct(h, bf16) for h in held_later]
    )
    hbm = pl.BlockSpec(memory_space=pl.ANY)
    total = count + 4
    row_slots = max(1, 2 * (ranks - 1))
    outs = pl.pallas_call(
        functools.partial(
            opening_kernel, side=side, second=second, ranks=ranks, square=square, sizes=sizes
        ),
        out_shape=tuple(out_shapes),
        in_specs=[hbm] * total,
        out_specs=(hbm,) * total,
        scratch_shapes=[pltpu.VMEM(h, bf16) for h in held]
        + [pltpu.VMEM(v.shape, bf16) for v in rows]
        + [pltpu.VMEM(h, bf16) for h in held_later]
        + [
            pltpu.SemaphoreType.DMA((total,)),
            pltpu.SemaphoreType.DMA((total,)),
            pltpu.SemaphoreType.DMA((count * steps,)),
            pltpu.SemaphoreType.DMA((count * steps,)),
            pltpu.SemaphoreType.DMA((row_slots,)),
            pltpu.SemaphoreType.DMA((row_slots,)),
        ],
        compiler_params=pltpu.CompilerParams(
            collective_id=0, has_side_effects=True, vmem_limit_bytes=VMEM_LIMIT
        ),
        name="opening",
    )(*gathered, *rows, *later)
    return outs[:count], outs[count : count + 2], outs[count + 2 :]


def pair_product_kernel(left_ref, right_ref, left_weight, right_weight, *refs):
    out_ref = refs[-1]
    out_ref[...] = (
        contract_last(left_ref[...], left_weight[...])
        + contract_last(right_ref[...], right_weight[...])
    ).astype(out_ref.dtype)


def norm_grad_kernel(
    left_ref,
    right_ref,
    x_ref,
    left_weight,
    right_weight,
    left_gain,
    right_gain,
    after_ref,
    out_ref,
    sums_ref,
):
    del after_ref
    x = x_ref[...].astype(jnp.float32)
    centered = x - jnp.mean(x, axis=-1, keepdims=True)
    inverse = lax.rsqrt(jnp.mean(centered * centered, axis=-1, keepdims=True) + EPSILON)
    hat = centered * inverse
    left = contract_last(left_ref[...], left_weight[...])
    right = contract_last(right_ref[...], right_weight[...])
    scaled = left * left_gain[...] + right * right_gain[...]
    first = pl.program_id(0) == 0
    for row, part in enumerate((left * hat, left, right * hat, right)):
        total = jnp.sum(part, axis=0, keepdims=True)
        sums_ref[row : row + 1, :] = jnp.where(first, 0.0, sums_ref[row : row + 1, :]) + total
    inner = (
        scaled
        - jnp.mean(scaled, axis=-1, keepdims=True)
        - hat * jnp.mean(scaled * hat, axis=-1, keepdims=True)
    )
    out_ref[...] = (inverse * inner).astype(out_ref.dtype)


ROWS_STEP = 256


def row_specs(arrays, start, rows):
    step = min(ROWS_STEP, rows)
    return step, [
        pl.BlockSpec((step, v.shape[1]), lambda i, first=start // step: (first + i, 0))
        for v in arrays
    ]


def whole_spec(array):
    return pl.BlockSpec(array.shape, lambda i: (0, 0))


def pair_product(left, right, left_weight, right_weight, after, start, rows):
    step, specs = row_specs((left, right), start, rows)
    width = left_weight.shape[0]
    return pl.pallas_call(
        pair_product_kernel,
        grid=(rows // step,),
        out_shape=jax.ShapeDtypeStruct((rows, width), jnp.bfloat16),
        in_specs=specs
        + [whole_spec(left_weight), whole_spec(right_weight)]
        + [pl.BlockSpec(memory_space=pl.ANY)] * len(after),
        out_specs=pl.BlockSpec((step, width), lambda i: (i, 0)),
        compiler_params=pltpu.CompilerParams(vmem_limit_bytes=VMEM_LIMIT),
        cost_estimate=pl.CostEstimate(
            flops=2 * rows * width * (left.shape[1] + right.shape[1]),
            bytes_accessed=2 * rows * (width + left.shape[1] + right.shape[1]),
            transcendentals=0,
        ),
        name="pair_product",
    )(left, right, left_weight, right_weight, *after)


def norm_grad(
    left, right, x, left_weight, right_weight, left_gain, right_gain, after, start, rows
):
    step, specs = row_specs((left, right, x), start, rows)
    width = left_weight.shape[0]
    rest = [left_weight, right_weight, left_gain, right_gain]
    return pl.pallas_call(
        norm_grad_kernel,
        grid=(rows // step,),
        out_shape=(
            jax.ShapeDtypeStruct((rows, width), jnp.bfloat16),
            jax.ShapeDtypeStruct((4, width), jnp.float32),
        ),
        in_specs=specs + [whole_spec(v) for v in rest] + [pl.BlockSpec(memory_space=pl.ANY)],
        out_specs=(
            pl.BlockSpec((step, width), lambda i: (i, 0)),
            pl.BlockSpec((4, width), lambda i: (0, 0)),
        ),
        compiler_params=pltpu.CompilerParams(vmem_limit_bytes=VMEM_LIMIT),
        cost_estimate=pl.CostEstimate(
            flops=2 * rows * width * (left.shape[1] + right.shape[1]),
            bytes_accessed=2 * rows * (2 * width + left.shape[1] + right.shape[1]),
            transcendentals=0,
        ),
        name="norm_grad",
    )(left, right, x, *rest, after)


SCALAR = pl.BlockSpec(memory_space=pltpu.SMEM)
VECTOR = pl.BlockSpec(memory_space=pltpu.VMEM)


def attend(order, bounds, proj, tables, seg_col, seg_row, block, count):
    length = proj.shape[0]
    pairs = length * length
    return pl.pallas_call(
        functools.partial(attend_kernel, block=block, count=count),
        out_shape=(
            jax.ShapeDtypeStruct((length, HD), jnp.bfloat16),
            jax.ShapeDtypeStruct((length, HD), jnp.bfloat16),
            jax.ShapeDtypeStruct((length, HD), jnp.bfloat16),
            jax.ShapeDtypeStruct((length, HD), jnp.bfloat16),
            jax.ShapeDtypeStruct((length, 1), jnp.float32),
        ),
        in_specs=[SCALAR] * 2 + [VECTOR] * 6,
        out_specs=(VECTOR,) * 5,
        scratch_shapes=[
            pltpu.VMEM((block, 1), jnp.float32),
            pltpu.VMEM((block, 1), jnp.float32),
            pltpu.VMEM((block, HD), jnp.float32),
        ],
        compiler_params=pltpu.CompilerParams(vmem_limit_bytes=VMEM_LIMIT),
        cost_estimate=pl.CostEstimate(
            flops=2 * pairs * HD, bytes_accessed=16 * length * HD, transcendentals=pairs // 2
        ),
        name="attend",
    )(order, bounds, proj, *tables, seg_col, seg_row)


def attend_grad(
    order, bounds, query, key, value, attn, grad, lse, tables, seg_col, seg_row, block, count
):
    length = query.shape[0]
    pairs = length * length
    return pl.pallas_call(
        functools.partial(attend_grad_kernel, block=block, count=count),
        out_shape=(
            jax.ShapeDtypeStruct((length, 3 * HD), jnp.bfloat16),
            jax.ShapeDtypeStruct((1, 3 * HD), jnp.float32),
        ),
        in_specs=[SCALAR] * 2 + [VECTOR] * 11,
        out_specs=(VECTOR,) * 2,
        scratch_shapes=[
            pltpu.VMEM((length, HD), jnp.float32),
            pltpu.VMEM((block, HD), jnp.float32),
            pltpu.VMEM((block, HD), jnp.float32),
            pltpu.VMEM((length, 1), jnp.float32),
        ],
        compiler_params=pltpu.CompilerParams(vmem_limit_bytes=VMEM_LIMIT),
        cost_estimate=pl.CostEstimate(
            flops=5 * pairs * HD, bytes_accessed=16 * length * HD, transcendentals=pairs // 2
        ),
        name="attend_grad",
    )(order, bounds, query, key, value, attn, grad, lse, *tables, seg_col, seg_row)


def ring_shift(value, axis, step):
    count = lax.axis_size(axis)
    return lax.ppermute(value, axis, [(i, (i + step) % count) for i in range(count)])


class Plane:
    def __init__(self):
        self.count = lax.axis_size("shard")
        side = math.isqrt(self.count)
        self.square = side * side == self.count
        self.first, self.second = (side, side) if self.square else (1, self.count)
        self.ranks = lax.axis_size("ctx")
        shard = lax.axis_index("shard")
        self.flip = (lax.axis_index("ctx") % 2 == 1) if self.square else False
        slow, fast = shard // self.second, shard % self.second
        if self.square:
            self.here = (jnp.where(self.flip, slow, fast), jnp.where(self.flip, fast, slow))
        else:
            self.here = (slow, fast)

    def index(self, first_step, second_step):
        first = lax.rem(self.here[0] + first_step + self.first, self.first)
        second = lax.rem(self.here[1] + second_step + self.second, self.second)
        if not self.square:
            return first * self.second + second
        side = self.first
        return jnp.where(self.flip, first * side + second, second * side + first)

    def move(self, value, first_step, second_step):
        pairs = []
        for shard in range(self.count):
            for rank in range(self.ranks):
                slow, fast = divmod(shard, self.second)
                if self.square and rank % 2 == 0:
                    slow = (slow + second_step) % self.second
                    fast = (fast + first_step) % self.first
                else:
                    slow = (slow + first_step) % self.first
                    fast = (fast + second_step) % self.second
                target = slow * self.second + fast
                pairs.append((shard * self.ranks + rank, target * self.ranks + rank))
        return lax.ppermute(value, ("shard", "ctx"), pairs)

    def scatter_sum(self, partial):
        rows = partial.shape[0] // self.count

        def block(a, b):
            return lax.dynamic_slice_in_dim(partial, self.index(a, b) * rows, rows)

        sums = {}
        for b in list(range(1, self.second)) + [0]:
            sums[b] = block(0, b).astype(jnp.float32)
            for a in range(1, self.first):
                sums[b] = sums[b] + self.move(block(a, b), a, 0).astype(jnp.float32)
        total = sums[0]
        for b in range(1, self.second):
            total = total + self.move(sums[b].astype(partial.dtype), 0, b).astype(jnp.float32)
        return total

    def full_sum(self, value):
        total = value
        for a in range(1, self.first):
            total = total + self.move(value, a, 0)
        value = total
        for b in range(1, self.second):
            total = total + self.move(value, 0, b)
        return total


def local(
    hidden_in,
    grad_out,
    segment_ids,
    group_order,
    ln1_gain,
    ln1_bias,
    qkv_weight,
    qkv_bias,
    dense_weight,
    dense_bias,
    ln2_gain,
    ln2_bias,
    up_weight,
    up_bias,
    down_weight,
    down_bias,
):
    _, groups_dev, block_len, width = hidden_in.shape
    tokens = groups_dev * block_len
    seq_len = segment_ids.shape[1]
    groups = seq_len // block_len
    ctx_count, tp_count = lax.axis_size("ctx"), lax.axis_size("tp")
    shard_count = lax.axis_size("shard")
    ctx_rank, tp_rank = lax.axis_index("ctx"), lax.axis_index("tp")
    shard_rank = lax.axis_index("shard")
    slice_width = width // tp_count
    bf16, f32 = jnp.bfloat16, jnp.float32

    def my_columns(matrix):
        columns = matrix.shape[1] // ctx_count
        return lax.dynamic_slice_in_dim(matrix, ctx_rank * columns, columns, 1)

    plane = Plane()

    x_mine = hidden_in.reshape(tokens, width)
    g_mine = grad_out.reshape(tokens, width)
    vectors = [
        ln1_gain, ln1_bias, ln2_gain, ln2_bias, dense_bias, down_bias, qkv_bias[0], up_bias[0],
    ]
    sizes = [v.shape[0] for v in vectors]
    wide = -(-max(sizes) // LANES) * LANES
    packed = jnp.stack([jnp.pad(v, (0, wide - v.shape[0])) for v in vectors])
    packed = jnp.concatenate([packed, jnp.zeros_like(packed)], axis=0)
    (w_vectors, w_qkv, w_dense), (x_row, g_row), (up_mine, down_mine) = opening(
        [packed, qkv_weight, dense_weight],
        [False, True, True],
        [x_mine, g_mine],
        [up_weight, down_weight],
        ctx_count,
    )
    w_up = lax.all_gather(up_mine, "shard", axis=0, tiled=True)
    w_down = lax.all_gather(down_mine, "shard", axis=0, tiled=True)
    w_vectors = w_vectors.reshape(shard_count, packed.shape[0], wide)
    spread = [
        w_vectors[:, number, :size].reshape(-1).astype(f32) for number, size in enumerate(sizes)
    ]
    gain_one, shift_one, gain_two, shift_two, bias_dense, bias_down, bias_qkv, bias_up = spread
    bias_qkv = my_columns(bias_qkv[None])
    bias_up = my_columns(bias_up[None])
    plane = Plane()
    heads_here = w_qkv.shape[1] // (3 * HD)

    own_order = jnp.concatenate(
        [
            lax.dynamic_slice_in_dim(
                group_order, lax.rem(ctx_rank + k, ctx_count) * groups_dev, groups_dev
            )
            for k in range(ctx_count)
        ]
    )
    segments = segment_ids[0]
    positions = segment_positions(segments)

    def stored(values):
        return jnp.concatenate(
            [
                lax.dynamic_slice_in_dim(values, own_order[k] * block_len, block_len)
                for k in range(groups)
            ]
        )

    seg_stored = stored(segments)
    tables = rotary_tables(stored(positions))
    seg_blocks = seg_stored.reshape(groups, block_len)
    bounds = jnp.stack([seg_blocks[:, 0], seg_blocks[:, -1]])
    seg_col, seg_row = seg_stored[:, None], seg_stored[None, :]

    x_float = x_row.astype(f32)
    centered = x_float - jnp.mean(x_float, axis=-1, keepdims=True)
    inverse = lax.rsqrt(jnp.mean(centered * centered, axis=-1, keepdims=True) + EPSILON)
    hat = centered * inverse
    acts_one = (hat * gain_one + shift_one).astype(bf16)
    acts_two = (hat * gain_two + shift_two).astype(bf16)

    projected = jnp.dot(acts_one, w_qkv, preferred_element_type=f32) + bias_qkv
    heads = []
    for h in range(heads_here):
        heads.append(
            attend(
                own_order,
                bounds,
                projected[:, 3 * HD * h : 3 * HD * (h + 1)],
                tables,
                seg_col,
                seg_row,
                block_len,
                groups,
            )
        )
    attn = jnp.concatenate([head[3] for head in heads], axis=1)

    attn_grad = jnp.dot(g_row, w_dense, preferred_element_type=f32).astype(bf16)
    proj_parts, sum_parts = [], []
    for h, (query, key, value, attn_head, lse) in enumerate(heads):
        part, sums = attend_grad(
            own_order,
            bounds,
            query,
            key,
            value,
            attn_head,
            attn_grad[:, HD * h : HD * (h + 1)],
            lse,
            tables,
            seg_col,
            seg_row,
            block_len,
            groups,
        )
        proj_parts.append(part)
        sum_parts.append(sums[0])
    proj_grad_b = jnp.concatenate(proj_parts, axis=1)
    qkv_bias_grad = jnp.concatenate(sum_parts)

    pre_act = jnp.dot(acts_two, w_up, preferred_element_type=f32) + bias_up
    cdf = 0.5 * (1.0 + lax.erf(pre_act * (1.0 / math.sqrt(2.0))))
    hidden = (pre_act * cdf).astype(bf16)
    slope = cdf + pre_act * jnp.exp(-0.5 * pre_act * pre_act) * (1.0 / math.sqrt(2.0 * math.pi))

    def reduce_partial(parts):
        total = parts[0].astype(f32)
        for k in range(1, ctx_count):
            total = total + ring_shift(parts[k], "ctx", k).astype(f32)
        total = total.astype(bf16)
        return total, lax.psum_scatter(total, "tp", scatter_dimension=1, tiled=True).astype(f32)

    dense_local = contract_first(g_row, attn).astype(bf16)
    qkv_local = contract_first(acts_one, proj_grad_b).astype(bf16)
    out_parts = {}
    for k in reversed(range(ctx_count)):
        out_parts[k] = pair_product(
            attn, hidden, w_dense, w_down, [dense_local, qkv_local], k * tokens, tokens
        )
    out_total, summed_out = reduce_partial(out_parts)
    out_shift = lax.dynamic_slice_in_dim(bias_dense + bias_down, tp_rank * slice_width, slice_width)
    x_slice = lax.dynamic_slice_in_dim(x_mine, tp_rank * slice_width, slice_width, 1)
    output = x_slice.astype(f32) + summed_out + out_shift

    def reduce_weight(grad):
        mine = plane.scatter_sum(grad.astype(bf16))
        rows, columns = mine.shape
        whole = jnp.zeros((rows, columns * ctx_count), f32)
        for k in range(ctx_count):
            part = mine if k == 0 else ring_shift(mine.astype(bf16), "ctx", ctx_count - k)
            place = lax.rem(ctx_rank + k, ctx_count) * columns
            whole = lax.dynamic_update_slice_in_dim(whole, part.astype(f32), place, 1)
        return whole

    bias_grad = jnp.sum(g_row.astype(f32), axis=0)
    dense_grad = reduce_weight(dense_local)
    qkv_grad = reduce_weight(qkv_local)

    pre_grad = jnp.dot(g_row, w_down, preferred_element_type=f32) * slope
    up_bias_grad = jnp.sum(pre_grad, axis=0)
    pre_grad_b = pre_grad.astype(bf16)

    in_parts, norm_sums = {}, jnp.zeros((4, width), f32)
    for k in reversed(range(ctx_count)):
        in_parts[k], sums = norm_grad(
            proj_grad_b,
            pre_grad_b,
            x_row,
            w_qkv,
            w_up,
            gain_one[None],
            gain_two[None],
            out_total,
            k * tokens,
            tokens,
        )
        norm_sums = norm_sums + sums
    _, input_sum = reduce_partial(in_parts)
    g_slice = lax.dynamic_slice_in_dim(g_mine, tp_rank * slice_width, slice_width, 1)
    input_grad = g_slice.astype(f32) + input_sum

    down_grad = reduce_weight(contract_first(g_row, hidden))
    up_grad = reduce_weight(contract_first(acts_two, pre_grad_b))

    norm_sums = norm_sums.reshape(-1)
    column_sums = [up_bias_grad, qkv_bias_grad]
    packed = jnp.concatenate([norm_sums] + column_sums)
    wholes = [jnp.zeros((v.shape[0] * ctx_count,), f32) for v in column_sums]
    total = jnp.zeros_like(norm_sums)
    for k in range(ctx_count):
        part = packed if k == 0 else ring_shift(packed, "ctx", ctx_count - k)
        total = total + part[: norm_sums.shape[0]]
        offset = norm_sums.shape[0]
        for number, vector in enumerate(column_sums):
            size = vector.shape[0]
            wholes[number] = lax.dynamic_update_slice_in_dim(
                wholes[number],
                part[offset : offset + size],
                lax.rem(ctx_rank + k, ctx_count) * size,
                0,
            )
            offset += size
    norm_sums = total
    for k in range(1, tp_count):
        norm_sums = norm_sums + ring_shift(total, "tp", k)
    pieces = [bias_grad] + wholes + [
        norm_sums[k * width : (k + 1) * width] for k in range(4)
    ]
    reduced = plane.full_sum(jnp.concatenate(pieces))
    results, offset = [], 0
    for piece in pieces:
        own = piece.shape[0] // shard_count
        results.append(lax.dynamic_slice_in_dim(reduced, offset + shard_rank * own, own))
        offset += piece.shape[0]
    bias_grad, up_bias_grad, qkv_bias_grad = results[:3]
    gain_one_grad, shift_one_grad, gain_two_grad, shift_two_grad = results[3:]
    out_shape = hidden_in.shape[:3] + (slice_width,)
    return (
        output.reshape(out_shape),
        input_grad.reshape(out_shape),
        gain_one_grad,
        shift_one_grad,
        qkv_grad,
        qkv_bias_grad[None],
        dense_grad,
        bias_grad,
        gain_two_grad,
        shift_two_grad,
        up_grad,
        up_bias_grad[None],
        down_grad,
    )


def solution(mesh):
    return jax.shard_map(
        local,
        mesh=mesh,
        in_specs=(
            P("shard", "ctx", None, None),
            P("shard", "ctx", None, None),
            P("shard", None),
            P(),
            P("shard"),
            P("shard"),
            P("shard", "tp"),
            P("tp", "shard"),
            P("shard", "tp"),
            P("shard"),
            P("shard"),
            P("shard"),
            P("shard", "tp"),
            P("tp", "shard"),
            P("shard", "tp"),
            P("shard"),
        ),
        out_specs=(
            P("shard", "ctx", None, "tp"),
            P("shard", "ctx", None, "tp"),
            P("shard"),
            P("shard"),
            P("shard", "tp"),
            P("tp", "shard"),
            P("shard", "tp"),
            P("shard"),
            P("shard"),
            P("shard"),
            P("shard", "tp"),
            P("tp", "shard"),
            P("shard", "tp"),
        ),
        check_vma=False,
    )
```

```python
import functools
import math

import jax
import jax.numpy as jnp
from jax import lax
from jax.experimental import pallas as pl
from jax.experimental.pallas import tpu as pltpu
from jax.sharding import PartitionSpec as P


HD = 256
ROT = 64
LANES = 128

EPSILON = 1e-05
ROTARY_BASE = 10000.0
NEG = -1e30
VMEM_LIMIT = 56 * 1024 * 1024


def segment_positions(segments):
    length_all = segments.shape[0]
    index_row = jnp.arange(length_all, dtype=jnp.int32)
    changed = jnp.concatenate(
        [jnp.ones((1,), dtype=jnp.bool_), segments[1:] != segments[:-1]]
    )
    seg_start = jnp.where(changed, index_row, jnp.zeros_like(segments))
    return index_row - lax.cummax(seg_start, axis=0)


def rotary_tables(positions):
    half_rot = ROT // 2
    frequency = ROTARY_BASE ** (-2.0 * jnp.arange(half_rot, dtype=jnp.float32) / ROT)
    angles = positions.astype(jnp.float32)[:, None] * frequency[None, :]
    cosine, sine = jnp.cos(angles), jnp.sin(angles)
    count = positions.shape[0]
    rest_one = jnp.ones((count, LANES - ROT), jnp.float32)
    rest_zero = jnp.zeros((count, LANES - half_rot), jnp.float32)
    cosine_table = jnp.concatenate([cosine, cosine, rest_one], axis=1)
    low_table = jnp.concatenate([-sine, rest_zero], axis=1)
    high_table = jnp.concatenate(
        [jnp.zeros_like(sine), sine, rest_zero[:, : LANES - ROT]], axis=1
    )
    return cosine_table, low_table, high_table


def turn(values, cosine, low, high, sign):
    half_rot = ROT // 2
    down = pltpu.roll(values, LANES - half_rot, 1)
    up = pltpu.roll(values, half_rot, 1)
    return values * cosine + sign * (down * low + up * high)


def contract_first(left_mat, right_mat):
    return lax.dot_general(
        left_mat, right_mat, (((0,), (0,)), ((), ())), preferred_element_type=jnp.float32
    )


def contract_last(left_mat, right_mat):
    return lax.dot_general(
        left_mat, right_mat, (((1,), (1,)), ((), ())), preferred_element_type=jnp.float32
    )


def block_meets(bounds_ref, order_ref, q_index, k_index):
    return (
        (order_ref[k_index] <= order_ref[q_index])
        & (bounds_ref[0, k_index] <= bounds_ref[1, q_index])
        & (bounds_ref[1, k_index] >= bounds_ref[0, q_index])
    )


def pair_mask(order_ref, seg_col_ref, seg_row_ref, q_index, k_index, block):
    q_place = order_ref[q_index] * block + lax.broadcasted_iota(jnp.int32, (block, block), 0)
    k_place = order_ref[k_index] * block + lax.broadcasted_iota(jnp.int32, (block, block), 1)
    seg_q = seg_col_ref[pl.ds(q_index * block, block), :]
    seg_k = seg_row_ref[:, pl.ds(pl.multiple_of(k_index * block, block), block)]
    return (k_place <= q_place) & (seg_q == seg_k)


def attend_kernel(
    order_ref,
    bounds_ref,
    proj_ref,
    cos_ref,
    low_ref,
    high_ref,
    seg_col_ref,
    seg_row_ref,
    query_ref,
    key_ref,
    value_ref,
    attn_ref,
    lse_ref,
    top_ref,
    sum_ref,
    acc_ref,
    *,
    block,
    count,
):
    score_scale = 1.0 / math.sqrt(HD)
    for index in range(count):
        rows = pl.ds(index * block, block)
        tables = (cos_ref[rows, :], low_ref[rows, :], high_ref[rows, :])
        for start, out in ((0, query_ref), (HD, key_ref)):
            out[rows, :LANES] = turn(
                proj_ref[rows, start : start + LANES], *tables, 1.0
            ).astype(jnp.bfloat16)
            out[rows, LANES:] = proj_ref[rows, start + LANES : start + HD].astype(jnp.bfloat16)
        value_ref[rows, :] = proj_ref[rows, 2 * HD :].astype(jnp.bfloat16)

    @pl.loop(0, count)
    def _(q_index):
        rows = pl.ds(pl.multiple_of(q_index * block, block), block)
        top_ref[...] = jnp.full_like(top_ref, NEG)
        sum_ref[...] = jnp.zeros_like(sum_ref)
        acc_ref[...] = jnp.zeros_like(acc_ref)

        @pl.loop(0, count)
        def _(k_index):
            @pl.when(block_meets(bounds_ref, order_ref, q_index, k_index))
            def _():
                keys = pl.ds(pl.multiple_of(k_index * block, block), block)
                scores = contract_last(query_ref[rows, :], key_ref[keys, :]) * score_scale
                allowed = pair_mask(order_ref, seg_col_ref, seg_row_ref, q_index, k_index, block)
                scores = jnp.where(allowed, scores, NEG)
                old_top = top_ref[...]
                new_top = jnp.maximum(old_top, jnp.max(scores, axis=1, keepdims=True))
                shrink = jnp.exp(old_top - new_top)
                weights = jnp.where(allowed, jnp.exp(scores - new_top), 0.0)
                top_ref[...] = new_top
                sum_ref[...] = sum_ref[...] * shrink + jnp.sum(weights, axis=1, keepdims=True)
                acc_ref[...] = acc_ref[...] * shrink + jnp.dot(
                    weights.astype(jnp.bfloat16),
                    value_ref[keys, :],
                    preferred_element_type=jnp.float32,
                )

        attn_ref[rows, :] = (acc_ref[...] / sum_ref[...]).astype(jnp.bfloat16)
        lse_ref[rows, :] = top_ref[...] + jnp.log(sum_ref[...])


def attend_grad_kernel(
    order_ref,
    bounds_ref,
    query_ref,
    key_ref,
    value_ref,
    attn_ref,
    grad_ref,
    lse_ref,
    cos_ref,
    low_ref,
    high_ref,
    seg_col_ref,
    seg_row_ref,
    out_ref,
    sums_ref,
    query_acc,
    key_acc,
    value_acc,
    delta_ref,
    *,
    block,
    count,
):
    score_scale = 1.0 / math.sqrt(HD)
    query_acc[...] = jnp.zeros_like(query_acc)
    delta_ref[...] = jnp.sum(
        grad_ref[...].astype(jnp.float32) * attn_ref[...].astype(jnp.float32),
        axis=1,
        keepdims=True,
    )

    @pl.loop(0, count)
    def _(k_index):
        keys = pl.ds(pl.multiple_of(k_index * block, block), block)
        key_acc[...] = jnp.zeros_like(key_acc)
        value_acc[...] = jnp.zeros_like(value_acc)

        @pl.loop(0, count)
        def _(q_index):
            @pl.when(block_meets(bounds_ref, order_ref, q_index, k_index))
            def _():
                rows = pl.ds(pl.multiple_of(q_index * block, block), block)
                query, key_rows = query_ref[rows, :], key_ref[keys, :]
                grad_rows = grad_ref[rows, :]
                scores = contract_last(query, key_rows) * score_scale
                allowed = pair_mask(order_ref, seg_col_ref, seg_row_ref, q_index, k_index, block)
                probs = jnp.where(allowed, jnp.exp(scores - lse_ref[rows, :]), 0.0)
                prob_grad = contract_last(grad_rows, value_ref[keys, :])
                score_grad = (probs * (prob_grad - delta_ref[rows, :])).astype(jnp.bfloat16)
                value_acc[...] += contract_first(probs.astype(jnp.bfloat16), grad_rows)
                key_acc[...] += contract_first(score_grad, query)
                query_acc[rows, :] += jnp.dot(
                    score_grad, key_rows, preferred_element_type=jnp.float32
                )

        tables = (cos_ref[keys, :], low_ref[keys, :], high_ref[keys, :])
        key_low = turn(key_acc[:, :LANES] * score_scale, *tables, -1.0)
        key_high = key_acc[:, LANES:] * score_scale
        first = k_index == 0
        for start, part in ((HD, key_low), (HD + LANES, key_high), (2 * HD, value_acc[...])):
            columns = slice(start, start + part.shape[1])
            out_ref[keys, columns] = part.astype(jnp.bfloat16)
            sums_ref[:, columns] = jnp.where(first, 0.0, sums_ref[:, columns]) + jnp.sum(
                part, axis=0, keepdims=True
            )

    sums_ref[:, :HD] = jnp.zeros((1, HD), jnp.float32)

    @pl.loop(0, count)
    def _(q_index):
        rows = pl.ds(pl.multiple_of(q_index * block, block), block)
        tables = (cos_ref[rows, :], low_ref[rows, :], high_ref[rows, :])
        query_low = turn(query_acc[rows, :LANES] * score_scale, *tables, -1.0)
        query_high = query_acc[rows, LANES:] * score_scale
        for start, part in ((0, query_low), (LANES, query_high)):
            columns = slice(start, start + part.shape[1])
            out_ref[rows, columns] = part.astype(jnp.bfloat16)
            sums_ref[:, columns] += jnp.sum(part, axis=0, keepdims=True)


MESH = pl.DeviceIdType.MESH


def opening_kernel(*refs, side, second, ranks, square, sizes):
    count = len(sizes)
    gathered_in, refs = refs[:count], refs[count:]
    rows_in, refs = refs[:2], refs[2:]
    later_in, refs = refs[:2], refs[2:]
    gathered_out, refs = refs[:count], refs[count:]
    rows_out, refs = refs[:2], refs[2:]
    later_out, refs = refs[:2], refs[2:]
    held, refs = refs[:count], refs[count:]
    held_rows, refs = refs[:2], refs[2:]
    held_later, refs = refs[:2], refs[2:]
    load_sem, store_sem, send_sem, recv_sem, row_send, row_recv = refs

    shard, rank = lax.axis_index("shard"), lax.axis_index("ctx")
    slow, fast = shard // second, shard % second
    flip = rank % 2 if square else 1
    here_first = fast * (1 - flip) + slow * flip
    here_second = slow * (1 - flip) + fast * flip

    def peer(first_step, second_step):
        first = (here_first + first_step + side) % side
        other = (here_second + second_step + second) % second
        return (other * side + first) * (1 - flip) + (first * second + other) * flip

    first_peers = [peer(a, 0) for a in range(1, side)]
    second_peers = [peer(0, b) for b in range(1, second)]
    rank_peers = [(rank + j) % ranks for j in range(1, ranks)]
    barrier = pltpu.get_barrier_semaphore()
    for target in first_peers + second_peers:
        pl.semaphore_signal(barrier, inc=1, device_id={"shard": target}, device_id_type=MESH)
    for target in rank_peers:
        pl.semaphore_signal(barrier, inc=1, device_id={"ctx": target}, device_id_type=MESH)

    loads = []
    for number in range(count):
        source = gathered_in[number]
        if sizes[number] is not None:
            columns = pl.ds(pl.multiple_of(rank * sizes[number], LANES), sizes[number])
            source = source.at[:, columns]
        loads.append(pltpu.make_async_copy(source, held[number], load_sem.at[number]))
    for number in range(2):
        loads.append(
            pltpu.make_async_copy(rows_in[number], held_rows[number], load_sem.at[count + number])
        )
    for number in range(2):
        size = held_later[number].shape[1]
        columns = pl.ds(pl.multiple_of(rank * size, LANES), size)
        loads.append(
            pltpu.make_async_copy(
                later_in[number].at[:, columns], held_later[number], load_sem.at[count + 2 + number]
            )
        )
    for load in loads:
        load.start()
    pl.semaphore_wait(barrier, len(first_peers) + len(second_peers) + len(rank_peers))

    def place(number, first_step, second_step):
        rows = held[number].shape[0]
        start = pl.multiple_of(peer(first_step, second_step) * rows, 16)
        return gathered_out[number].at[pl.ds(start, rows), :]

    copies, slot = {}, 0
    steps = side - 1 + (second - 1) * side

    def send(number, source, a, b, target, key):
        slot = number * steps + key
        copy = pltpu.make_async_remote_copy(
            src_ref=source,
            dst_ref=place(number, a, b),
            send_sem=send_sem.at[slot],
            recv_sem=recv_sem.at[slot],
            device_id={"shard": target},
            device_id_type=MESH,
        )
        copy.start()
        copies[number, key] = copy

    for number in range(count):
        loads[number].wait()
        for a in range(1, side):
            send(number, held[number], 0, 0, first_peers[a - 1], a - 1)
        for b in range(1, second):
            send(number, held[number], 0, 0, second_peers[b - 1], side - 1 + (b - 1) * side)
    row_copies = []
    for number in range(2):
        loads[count + number].wait()
        rows = held_rows[number].shape[0]
        for j in range(1, ranks):
            slot = number * (ranks - 1) + j - 1
            copy = pltpu.make_async_remote_copy(
                src_ref=held_rows[number],
                dst_ref=rows_out[number].at[pl.ds((ranks - j) * rows, rows), :],
                send_sem=row_send.at[slot],
                recv_sem=row_recv.at[slot],
                device_id={"ctx": rank_peers[j - 1]},
                device_id_type=MESH,
            )
            copy.start()
            row_copies.append(copy)
    stores = []
    for number in range(count):
        stores.append(
            pltpu.make_async_copy(held[number], place(number, 0, 0), store_sem.at[number])
        )
    for number in range(2):
        rows = held_rows[number].shape[0]
        stores.append(
            pltpu.make_async_copy(
                held_rows[number],
                rows_out[number].at[pl.ds(0, rows), :],
                store_sem.at[count + number],
            )
        )
    for number in range(2):
        loads[count + 2 + number].wait()
        stores.append(
            pltpu.make_async_copy(
                held_later[number], later_out[number], store_sem.at[count + 2 + number]
            )
        )
    for store in stores:
        store.start()
    for number in range(count):
        for a in range(1, side):
            copies[number, a - 1].wait_recv()
            for b in range(1, second):
                key = side - 1 + (b - 1) * side + a
                send(number, place(number, -a, 0), -a, 0, second_peers[b - 1], key)
    for store in stores:
        store.wait()
    for (number, key), copy in copies.items():
        copy.wait_send()
        if key >= side - 1:
            copy.wait_recv()
    for copy in row_copies:
        copy.wait_send()
        copy.wait_recv()


def opening(gathered, split, rows, later, ranks):
    shards = lax.axis_size("shard")
    side = math.isqrt(shards)
    square = side * side == shards
    if not square:
        side = 1
    second = shards // side
    sizes = [v.shape[1] // ranks if cut else None for v, cut in zip(gathered, split)]
    held = [(v.shape[0], size or v.shape[1]) for v, size in zip(gathered, sizes)]
    held_later = [(v.shape[0], v.shape[1] // ranks) for v in later]
    count, steps = len(gathered), side - 1 + (second - 1) * side
    bf16 = jnp.bfloat16
    out_shapes = (
        [jax.ShapeDtypeStruct((h[0] * shards, h[1]), bf16) for h in held]
        + [jax.ShapeDtypeStruct((v.shape[0] * ranks, v.shape[1]), bf16) for v in rows]
        + [jax.ShapeDtypeStruct(h, bf16) for h in held_later]
    )
    hbm = pl.BlockSpec(memory_space=pl.ANY)
    total = count + 4
    row_slots = max(1, 2 * (ranks - 1))
    outs = pl.pallas_call(
        functools.partial(
            opening_kernel, side=side, second=second, ranks=ranks, square=square, sizes=sizes
        ),
        out_shape=tuple(out_shapes),
        in_specs=[hbm] * total,
        out_specs=(hbm,) * total,
        scratch_shapes=[pltpu.VMEM(h, bf16) for h in held]
        + [pltpu.VMEM(v.shape, bf16) for v in rows]
        + [pltpu.VMEM(h, bf16) for h in held_later]
        + [
            pltpu.SemaphoreType.DMA((total,)),
            pltpu.SemaphoreType.DMA((total,)),
            pltpu.SemaphoreType.DMA((count * steps,)),
            pltpu.SemaphoreType.DMA((count * steps,)),
            pltpu.SemaphoreType.DMA((row_slots,)),
            pltpu.SemaphoreType.DMA((row_slots,)),
        ],
        compiler_params=pltpu.CompilerParams(
            collective_id=0, has_side_effects=True, vmem_limit_bytes=VMEM_LIMIT
        ),
        name="opening",
    )(*gathered, *rows, *later)
    return outs[:count], outs[count : count + 2], outs[count + 2 :]


def pair_product_kernel(left_ref, right_ref, left_weight, right_weight, *refs):
    out_ref = refs[-1]
    out_ref[...] = (
        contract_last(left_ref[...], left_weight[...])
        + contract_last(right_ref[...], right_weight[...])
    ).astype(out_ref.dtype)


def block_sum_kernel(index_ref, whole_ref, *refs, count):
    del index_ref
    total = whole_ref[...].astype(jnp.float32)
    for ref in refs[:count]:
        total = total + ref[...].astype(jnp.float32)
    refs[-1][...] = total.astype(refs[-1].dtype)


def block_sum(whole, index, received, after, dtype):
    rows, columns = received[0].shape
    step = min(rows, 256)
    tiles = rows // step
    tile = pl.BlockSpec((step, columns), lambda i, index: (i, 0))
    return pl.pallas_call(
        functools.partial(block_sum_kernel, count=len(received)),
        grid_spec=pltpu.PrefetchScalarGridSpec(
            num_scalar_prefetch=1,
            grid=(tiles,),
            in_specs=[pl.BlockSpec((step, columns), lambda i, index: (index[0] * tiles + i, 0))]
            + [tile] * len(received)
            + [pl.BlockSpec(memory_space=pl.ANY)] * len(after),
            out_specs=tile,
        ),
        out_shape=jax.ShapeDtypeStruct((rows, columns), dtype),
        cost_estimate=pl.CostEstimate(
            flops=rows * columns, bytes_accessed=6 * rows * columns, transcendentals=0
        ),
        name="block_sum",
    )(jnp.asarray(index, jnp.int32).reshape(1), whole, *received, *after)


def norm_grad_kernel(
    left_ref,
    right_ref,
    x_ref,
    left_weight,
    right_weight,
    left_gain,
    right_gain,
    after_ref,
    out_ref,
    sums_ref,
):
    del after_ref
    x = x_ref[...].astype(jnp.float32)
    centered = x - jnp.mean(x, axis=-1, keepdims=True)
    inverse = lax.rsqrt(jnp.mean(centered * centered, axis=-1, keepdims=True) + EPSILON)
    hat = centered * inverse
    left = contract_last(left_ref[...], left_weight[...])
    right = contract_last(right_ref[...], right_weight[...])
    scaled = left * left_gain[...] + right * right_gain[...]
    first = pl.program_id(0) == 0
    for row, part in enumerate((left * hat, left, right * hat, right)):
        total = jnp.sum(part, axis=0, keepdims=True)
        sums_ref[row : row + 1, :] = jnp.where(first, 0.0, sums_ref[row : row + 1, :]) + total
    inner = (
        scaled
        - jnp.mean(scaled, axis=-1, keepdims=True)
        - hat * jnp.mean(scaled * hat, axis=-1, keepdims=True)
    )
    out_ref[...] = (inverse * inner).astype(out_ref.dtype)


ROWS_STEP = 256


def row_specs(arrays, start, rows):
    step = min(ROWS_STEP, rows)
    return step, [
        pl.BlockSpec((step, v.shape[1]), lambda i, first=start // step: (first + i, 0))
        for v in arrays
    ]


def whole_spec(array):
    return pl.BlockSpec(array.shape, lambda i: (0, 0))


def pair_product(left, right, left_weight, right_weight, after, start, rows):
    step, specs = row_specs((left, right), start, rows)
    width = left_weight.shape[0]
    return pl.pallas_call(
        pair_product_kernel,
        grid=(rows // step,),
        out_shape=jax.ShapeDtypeStruct((rows, width), jnp.bfloat16),
        in_specs=specs
        + [whole_spec(left_weight), whole_spec(right_weight)]
        + [pl.BlockSpec(memory_space=pl.ANY)] * len(after),
        out_specs=pl.BlockSpec((step, width), lambda i: (i, 0)),
        compiler_params=pltpu.CompilerParams(vmem_limit_bytes=VMEM_LIMIT),
        cost_estimate=pl.CostEstimate(
            flops=2 * rows * width * (left.shape[1] + right.shape[1]),
            bytes_accessed=2 * rows * (width + left.shape[1] + right.shape[1]),
            transcendentals=0,
        ),
        name="pair_product",
    )(left, right, left_weight, right_weight, *after)


def norm_grad(
    left, right, x, left_weight, right_weight, left_gain, right_gain, after, start, rows
):
    step, specs = row_specs((left, right, x), start, rows)
    width = left_weight.shape[0]
    rest = [left_weight, right_weight, left_gain, right_gain]
    return pl.pallas_call(
        norm_grad_kernel,
        grid=(rows // step,),
        out_shape=(
            jax.ShapeDtypeStruct((rows, width), jnp.bfloat16),
            jax.ShapeDtypeStruct((4, width), jnp.float32),
        ),
        in_specs=specs + [whole_spec(v) for v in rest] + [pl.BlockSpec(memory_space=pl.ANY)],
        out_specs=(
            pl.BlockSpec((step, width), lambda i: (i, 0)),
            pl.BlockSpec((4, width), lambda i: (0, 0)),
        ),
        compiler_params=pltpu.CompilerParams(vmem_limit_bytes=VMEM_LIMIT),
        cost_estimate=pl.CostEstimate(
            flops=2 * rows * width * (left.shape[1] + right.shape[1]),
            bytes_accessed=2 * rows * (2 * width + left.shape[1] + right.shape[1]),
            transcendentals=0,
        ),
        name="norm_grad",
    )(left, right, x, *rest, after)


SCALAR = pl.BlockSpec(memory_space=pltpu.SMEM)
VECTOR = pl.BlockSpec(memory_space=pltpu.VMEM)


def attend(order, bounds, proj, tables, seg_col, seg_row, block, count):
    length = proj.shape[0]
    pairs = length * length
    return pl.pallas_call(
        functools.partial(attend_kernel, block=block, count=count),
        out_shape=(
            jax.ShapeDtypeStruct((length, HD), jnp.bfloat16),
            jax.ShapeDtypeStruct((length, HD), jnp.bfloat16),
            jax.ShapeDtypeStruct((length, HD), jnp.bfloat16),
            jax.ShapeDtypeStruct((length, HD), jnp.bfloat16),
            jax.ShapeDtypeStruct((length, 1), jnp.float32),
        ),
        in_specs=[SCALAR] * 2 + [VECTOR] * 6,
        out_specs=(VECTOR,) * 5,
        scratch_shapes=[
            pltpu.VMEM((block, 1), jnp.float32),
            pltpu.VMEM((block, 1), jnp.float32),
            pltpu.VMEM((block, HD), jnp.float32),
        ],
        compiler_params=pltpu.CompilerParams(vmem_limit_bytes=VMEM_LIMIT),
        cost_estimate=pl.CostEstimate(
            flops=2 * pairs * HD, bytes_accessed=16 * length * HD, transcendentals=pairs // 2
        ),
        name="attend",
    )(order, bounds, proj, *tables, seg_col, seg_row)


def attend_grad(
    order, bounds, query, key, value, attn, grad, lse, tables, seg_col, seg_row, block, count
):
    length = query.shape[0]
    pairs = length * length
    return pl.pallas_call(
        functools.partial(attend_grad_kernel, block=block, count=count),
        out_shape=(
            jax.ShapeDtypeStruct((length, 3 * HD), jnp.bfloat16),
            jax.ShapeDtypeStruct((1, 3 * HD), jnp.float32),
        ),
        in_specs=[SCALAR] * 2 + [VECTOR] * 11,
        out_specs=(VECTOR,) * 2,
        scratch_shapes=[
            pltpu.VMEM((length, HD), jnp.float32),
            pltpu.VMEM((block, HD), jnp.float32),
            pltpu.VMEM((block, HD), jnp.float32),
            pltpu.VMEM((length, 1), jnp.float32),
        ],
        compiler_params=pltpu.CompilerParams(vmem_limit_bytes=VMEM_LIMIT),
        cost_estimate=pl.CostEstimate(
            flops=5 * pairs * HD, bytes_accessed=16 * length * HD, transcendentals=pairs // 2
        ),
        name="attend_grad",
    )(order, bounds, query, key, value, attn, grad, lse, *tables, seg_col, seg_row)


def ring_shift(value, axis, step):
    count = lax.axis_size(axis)
    return lax.ppermute(value, axis, [(i, (i + step) % count) for i in range(count)])


class Plane:
    def __init__(self):
        self.count = lax.axis_size("shard")
        side = math.isqrt(self.count)
        self.square = side * side == self.count
        self.first, self.second = (side, side) if self.square else (1, self.count)
        self.ranks = lax.axis_size("ctx")
        shard = lax.axis_index("shard")
        self.flip = (lax.axis_index("ctx") % 2 == 1) if self.square else False
        slow, fast = shard // self.second, shard % self.second
        if self.square:
            self.here = (jnp.where(self.flip, slow, fast), jnp.where(self.flip, fast, slow))
        else:
            self.here = (slow, fast)

    def index(self, first_step, second_step):
        first = lax.rem(self.here[0] + first_step + self.first, self.first)
        second = lax.rem(self.here[1] + second_step + self.second, self.second)
        if not self.square:
            return first * self.second + second
        side = self.first
        return jnp.where(self.flip, first * side + second, second * side + first)

    def move(self, value, first_step, second_step):
        pairs = []
        for shard in range(self.count):
            for rank in range(self.ranks):
                slow, fast = divmod(shard, self.second)
                if self.square and rank % 2 == 0:
                    slow = (slow + second_step) % self.second
                    fast = (fast + first_step) % self.first
                else:
                    slow = (slow + first_step) % self.first
                    fast = (fast + second_step) % self.second
                target = slow * self.second + fast
                pairs.append((shard * self.ranks + rank, target * self.ranks + rank))
        return lax.ppermute(value, ("shard", "ctx"), pairs)

    def scatter_sum(self, partial, after):
        rows = partial.shape[0] // self.count
        sums, final = {}, []
        for b in list(range(1, self.second)) + [0]:
            received = []
            for a in range(1, self.first):
                block = lax.dynamic_slice_in_dim(partial, self.index(a, b) * rows, rows)
                received.append(self.move(block, a, 0))
            if b == 0:
                final = received
            elif received:
                sums[b] = block_sum(partial, self.index(0, b), received, after, partial.dtype)
            else:
                sums[b] = lax.dynamic_slice_in_dim(partial, self.index(0, b) * rows, rows)
        final = final + [self.move(sums[b], 0, b) for b in range(1, self.second)]
        return block_sum(partial, self.index(0, 0), final, after, jnp.float32)

    def full_sum(self, value):
        total = value
        for a in range(1, self.first):
            total = total + self.move(value, a, 0)
        value = total
        for b in range(1, self.second):
            total = total + self.move(value, 0, b)
        return total


def local(
    hidden_in,
    grad_out,
    segment_ids,
    group_order,
    ln1_gain,
    ln1_bias,
    qkv_weight,
    qkv_bias,
    dense_weight,
    dense_bias,
    ln2_gain,
    ln2_bias,
    up_weight,
    up_bias,
    down_weight,
    down_bias,
):
    _, groups_dev, block_len, width = hidden_in.shape
    tokens = groups_dev * block_len
    seq_len = segment_ids.shape[1]
    groups = seq_len // block_len
    ctx_count, tp_count = lax.axis_size("ctx"), lax.axis_size("tp")
    shard_count = lax.axis_size("shard")
    ctx_rank, tp_rank = lax.axis_index("ctx"), lax.axis_index("tp")
    shard_rank = lax.axis_index("shard")
    slice_width = width // tp_count
    bf16, f32 = jnp.bfloat16, jnp.float32

    def my_columns(matrix):
        columns = matrix.shape[1] // ctx_count
        return lax.dynamic_slice_in_dim(matrix, ctx_rank * columns, columns, 1)

    plane = Plane()

    x_mine = hidden_in.reshape(tokens, width)
    g_mine = grad_out.reshape(tokens, width)
    vectors = [
        ln1_gain, ln1_bias, ln2_gain, ln2_bias, dense_bias, down_bias, qkv_bias[0], up_bias[0],
    ]
    sizes = [v.shape[0] for v in vectors]
    wide = -(-max(sizes) // LANES) * LANES
    packed = jnp.stack([jnp.pad(v, (0, wide - v.shape[0])) for v in vectors])
    packed = jnp.concatenate([packed, jnp.zeros_like(packed)], axis=0)
    (w_vectors, w_qkv, w_dense), (x_row, g_row), (up_mine, down_mine) = opening(
        [packed, qkv_weight, dense_weight],
        [False, True, True],
        [x_mine, g_mine],
        [up_weight, down_weight],
        ctx_count,
    )
    w_up = lax.all_gather(up_mine, "shard", axis=0, tiled=True)
    w_down = lax.all_gather(down_mine, "shard", axis=0, tiled=True)
    w_vectors = w_vectors.reshape(shard_count, packed.shape[0], wide)
    spread = [
        w_vectors[:, number, :size].reshape(-1).astype(f32) for number, size in enumerate(sizes)
    ]
    gain_one, shift_one, gain_two, shift_two, bias_dense, bias_down, bias_qkv, bias_up = spread
    bias_qkv = my_columns(bias_qkv[None])
    bias_up = my_columns(bias_up[None])
    plane = Plane()
    heads_here = w_qkv.shape[1] // (3 * HD)

    own_order = jnp.concatenate(
        [
            lax.dynamic_slice_in_dim(
                group_order, lax.rem(ctx_rank + k, ctx_count) * groups_dev, groups_dev
            )
            for k in range(ctx_count)
        ]
    )
    segments = segment_ids[0]
    positions = segment_positions(segments)

    def stored(values):
        return jnp.concatenate(
            [
                lax.dynamic_slice_in_dim(values, own_order[k] * block_len, block_len)
                for k in range(groups)
            ]
        )

    seg_stored = stored(segments)
    tables = rotary_tables(stored(positions))
    seg_blocks = seg_stored.reshape(groups, block_len)
    bounds = jnp.stack([seg_blocks[:, 0], seg_blocks[:, -1]])
    seg_col, seg_row = seg_stored[:, None], seg_stored[None, :]

    x_float = x_row.astype(f32)
    centered = x_float - jnp.mean(x_float, axis=-1, keepdims=True)
    inverse = lax.rsqrt(jnp.mean(centered * centered, axis=-1, keepdims=True) + EPSILON)
    hat = centered * inverse
    acts_one = (hat * gain_one + shift_one).astype(bf16)
    acts_two = (hat * gain_two + shift_two).astype(bf16)

    projected = jnp.dot(acts_one, w_qkv, preferred_element_type=f32) + bias_qkv
    heads = []
    for h in range(heads_here):
        heads.append(
            attend(
                own_order,
                bounds,
                projected[:, 3 * HD * h : 3 * HD * (h + 1)],
                tables,
                seg_col,
                seg_row,
                block_len,
                groups,
            )
        )
    attn = jnp.concatenate([head[3] for head in heads], axis=1)

    attn_grad = jnp.dot(g_row, w_dense, preferred_element_type=f32).astype(bf16)
    proj_parts, sum_parts = [], []
    for h, (query, key, value, attn_head, lse) in enumerate(heads):
        part, sums = attend_grad(
            own_order,
            bounds,
            query,
            key,
            value,
            attn_head,
            attn_grad[:, HD * h : HD * (h + 1)],
            lse,
            tables,
            seg_col,
            seg_row,
            block_len,
            groups,
        )
        proj_parts.append(part)
        sum_parts.append(sums[0])
    proj_grad_b = jnp.concatenate(proj_parts, axis=1)
    qkv_bias_grad = jnp.concatenate(sum_parts)

    pre_act = jnp.dot(acts_two, w_up, preferred_element_type=f32) + bias_up
    cdf = 0.5 * (1.0 + lax.erf(pre_act * (1.0 / math.sqrt(2.0))))
    hidden = (pre_act * cdf).astype(bf16)
    slope = cdf + pre_act * jnp.exp(-0.5 * pre_act * pre_act) * (1.0 / math.sqrt(2.0 * math.pi))

    def reduce_partial(parts):
        received = [ring_shift(parts[k], "ctx", k) for k in range(1, ctx_count)]
        total = block_sum(parts[0], 0, received, [], bf16)
        return total, lax.psum_scatter(total, "tp", scatter_dimension=1, tiled=True).astype(f32)

    dense_local = contract_first(g_row, attn).astype(bf16)
    qkv_local = contract_first(acts_one, proj_grad_b).astype(bf16)
    out_parts = {}
    for k in reversed(range(ctx_count)):
        out_parts[k] = pair_product(
            attn,
            hidden,
            w_dense,
            w_down,
            [dense_local, qkv_local] if k + 1 == ctx_count else [out_parts[k + 1]],
            k * tokens,
            tokens,
        )
    out_total, summed_out = reduce_partial(out_parts)
    out_shift = lax.dynamic_slice_in_dim(bias_dense + bias_down, tp_rank * slice_width, slice_width)
    x_slice = lax.dynamic_slice_in_dim(x_mine, tp_rank * slice_width, slice_width, 1)
    output = x_slice.astype(f32) + summed_out + out_shift

    def reduce_weight(grad, after):
        mine = plane.scatter_sum(grad, after)
        rows, columns = mine.shape
        whole = jnp.zeros((rows, columns * ctx_count), f32)
        for k in range(ctx_count):
            part = mine if k == 0 else ring_shift(mine.astype(bf16), "ctx", ctx_count - k)
            place = lax.rem(ctx_rank + k, ctx_count) * columns
            whole = lax.dynamic_update_slice_in_dim(whole, part.astype(f32), place, 1)
        return whole

    bias_grad = jnp.sum(g_row.astype(f32), axis=0)

    pre_grad = jnp.dot(g_row, w_down, preferred_element_type=f32) * slope
    up_bias_grad = jnp.sum(pre_grad, axis=0)
    pre_grad_b = pre_grad.astype(bf16)

    in_parts, norm_sums = {}, jnp.zeros((4, width), f32)
    for k in reversed(range(ctx_count)):
        in_parts[k], sums = norm_grad(
            proj_grad_b,
            pre_grad_b,
            x_row,
            w_qkv,
            w_up,
            gain_one[None],
            gain_two[None],
            in_parts[k + 1] if k + 1 in in_parts else out_total,
            k * tokens,
            tokens,
        )
        norm_sums = norm_sums + sums
    _, input_sum = reduce_partial(in_parts)
    g_slice = lax.dynamic_slice_in_dim(g_mine, tp_rank * slice_width, slice_width, 1)
    input_grad = g_slice.astype(f32) + input_sum

    dense_grad = reduce_weight(dense_local, [in_parts[0]])
    qkv_grad = reduce_weight(qkv_local, [in_parts[0]])
    down_local = contract_first(g_row, hidden).astype(bf16)
    up_local = contract_first(acts_two, pre_grad_b).astype(bf16)
    down_grad = reduce_weight(down_local, [up_local])
    up_grad = reduce_weight(up_local, [])

    norm_sums = norm_sums.reshape(-1)
    column_sums = [up_bias_grad, qkv_bias_grad]
    packed = jnp.concatenate([norm_sums] + column_sums)
    wholes = [jnp.zeros((v.shape[0] * ctx_count,), f32) for v in column_sums]
    total = jnp.zeros_like(norm_sums)
    for k in range(ctx_count):
        part = packed if k == 0 else ring_shift(packed, "ctx", ctx_count - k)
        total = total + part[: norm_sums.shape[0]]
        offset = norm_sums.shape[0]
        for number, vector in enumerate(column_sums):
            size = vector.shape[0]
            wholes[number] = lax.dynamic_update_slice_in_dim(
                wholes[number],
                part[offset : offset + size],
                lax.rem(ctx_rank + k, ctx_count) * size,
                0,
            )
            offset += size
    norm_sums = total
    for k in range(1, tp_count):
        norm_sums = norm_sums + ring_shift(total, "tp", k)
    pieces = [bias_grad] + wholes + [
        norm_sums[k * width : (k + 1) * width] for k in range(4)
    ]
    reduced = plane.full_sum(jnp.concatenate(pieces))
    results, offset = [], 0
    for piece in pieces:
        own = piece.shape[0] // shard_count
        results.append(lax.dynamic_slice_in_dim(reduced, offset + shard_rank * own, own))
        offset += piece.shape[0]
    bias_grad, up_bias_grad, qkv_bias_grad = results[:3]
    gain_one_grad, shift_one_grad, gain_two_grad, shift_two_grad = results[3:]
    out_shape = hidden_in.shape[:3] + (slice_width,)
    return (
        output.reshape(out_shape),
        input_grad.reshape(out_shape),
        gain_one_grad,
        shift_one_grad,
        qkv_grad,
        qkv_bias_grad[None],
        dense_grad,
        bias_grad,
        gain_two_grad,
        shift_two_grad,
        up_grad,
        up_bias_grad[None],
        down_grad,
    )


def solution(mesh):
    return jax.shard_map(
        local,
        mesh=mesh,
        in_specs=(
            P("shard", "ctx", None, None),
            P("shard", "ctx", None, None),
            P("shard", None),
            P(),
            P("shard"),
            P("shard"),
            P("shard", "tp"),
            P("tp", "shard"),
            P("shard", "tp"),
            P("shard"),
            P("shard"),
            P("shard"),
            P("shard", "tp"),
            P("tp", "shard"),
            P("shard", "tp"),
            P("shard"),
        ),
        out_specs=(
            P("shard", "ctx", None, "tp"),
            P("shard", "ctx", None, "tp"),
            P("shard"),
            P("shard"),
            P("shard", "tp"),
            P("tp", "shard"),
            P("shard", "tp"),
            P("shard"),
            P("shard"),
            P("shard"),
            P("shard", "tp"),
            P("tp", "shard"),
            P("shard", "tp"),
        ),
        check_vma=False,
    )
```

```python
import functools
import math

import jax
import jax.numpy as jnp
from jax import lax
from jax.experimental import pallas as pl
from jax.experimental.pallas import tpu as pltpu
from jax.sharding import PartitionSpec as P


HD = 256
ROT = 64
LANES = 128

EPSILON = 1e-05
ROTARY_BASE = 10000.0
NEG = -1e30
VMEM_LIMIT = 56 * 1024 * 1024


def segment_positions(segments):
    length_all = segments.shape[0]
    index_row = jnp.arange(length_all, dtype=jnp.int32)
    changed = jnp.concatenate(
        [jnp.ones((1,), dtype=jnp.bool_), segments[1:] != segments[:-1]]
    )
    seg_start = jnp.where(changed, index_row, jnp.zeros_like(segments))
    return index_row - lax.cummax(seg_start, axis=0)


def rotary_tables(positions):
    half_rot = ROT // 2
    frequency = ROTARY_BASE ** (-2.0 * jnp.arange(half_rot, dtype=jnp.float32) / ROT)
    angles = positions.astype(jnp.float32)[:, None] * frequency[None, :]
    cosine, sine = jnp.cos(angles), jnp.sin(angles)
    count = positions.shape[0]
    rest_one = jnp.ones((count, LANES - ROT), jnp.float32)
    rest_zero = jnp.zeros((count, LANES - half_rot), jnp.float32)
    cosine_table = jnp.concatenate([cosine, cosine, rest_one], axis=1)
    low_table = jnp.concatenate([-sine, rest_zero], axis=1)
    high_table = jnp.concatenate(
        [jnp.zeros_like(sine), sine, rest_zero[:, : LANES - ROT]], axis=1
    )
    return cosine_table, low_table, high_table


def turn(values, cosine, low, high, sign):
    half_rot = ROT // 2
    down = pltpu.roll(values, LANES - half_rot, 1)
    up = pltpu.roll(values, half_rot, 1)
    return values * cosine + sign * (down * low + up * high)


def contract_first(left_mat, right_mat):
    return lax.dot_general(
        left_mat, right_mat, (((0,), (0,)), ((), ())), preferred_element_type=jnp.float32
    )


def contract_last(left_mat, right_mat):
    return lax.dot_general(
        left_mat, right_mat, (((1,), (1,)), ((), ())), preferred_element_type=jnp.float32
    )


def block_meets(bounds_ref, order_ref, q_index, k_index):
    return (
        (order_ref[k_index] <= order_ref[q_index])
        & (bounds_ref[0, k_index] <= bounds_ref[1, q_index])
        & (bounds_ref[1, k_index] >= bounds_ref[0, q_index])
    )


def pair_mask(order_ref, seg_col_ref, seg_row_ref, q_index, k_index, block):
    q_place = order_ref[q_index] * block + lax.broadcasted_iota(jnp.int32, (block, block), 0)
    k_place = order_ref[k_index] * block + lax.broadcasted_iota(jnp.int32, (block, block), 1)
    seg_q = seg_col_ref[pl.ds(q_index * block, block), :]
    seg_k = seg_row_ref[:, pl.ds(pl.multiple_of(k_index * block, block), block)]
    return (k_place <= q_place) & (seg_q == seg_k)


def attend_kernel(
    order_ref,
    bounds_ref,
    proj_ref,
    cos_ref,
    low_ref,
    high_ref,
    seg_col_ref,
    seg_row_ref,
    query_ref,
    key_ref,
    value_ref,
    attn_ref,
    lse_ref,
    top_ref,
    sum_ref,
    acc_ref,
    *,
    block,
    count,
):
    score_scale = 1.0 / math.sqrt(HD)
    for index in range(count):
        rows = pl.ds(index * block, block)
        tables = (cos_ref[rows, :], low_ref[rows, :], high_ref[rows, :])
        for start, out in ((0, query_ref), (HD, key_ref)):
            out[rows, :LANES] = turn(
                proj_ref[rows, start : start + LANES], *tables, 1.0
            ).astype(jnp.bfloat16)
            out[rows, LANES:] = proj_ref[rows, start + LANES : start + HD].astype(jnp.bfloat16)
        value_ref[rows, :] = proj_ref[rows, 2 * HD :].astype(jnp.bfloat16)

    @pl.loop(0, count)
    def _(q_index):
        rows = pl.ds(pl.multiple_of(q_index * block, block), block)
        top_ref[...] = jnp.full_like(top_ref, NEG)
        sum_ref[...] = jnp.zeros_like(sum_ref)
        acc_ref[...] = jnp.zeros_like(acc_ref)

        @pl.loop(0, count)
        def _(k_index):
            @pl.when(block_meets(bounds_ref, order_ref, q_index, k_index))
            def _():
                keys = pl.ds(pl.multiple_of(k_index * block, block), block)
                scores = contract_last(query_ref[rows, :], key_ref[keys, :]) * score_scale
                allowed = pair_mask(order_ref, seg_col_ref, seg_row_ref, q_index, k_index, block)
                scores = jnp.where(allowed, scores, NEG)
                old_top = top_ref[...]
                new_top = jnp.maximum(old_top, jnp.max(scores, axis=1, keepdims=True))
                shrink = jnp.exp(old_top - new_top)
                weights = jnp.where(allowed, jnp.exp(scores - new_top), 0.0)
                top_ref[...] = new_top
                sum_ref[...] = sum_ref[...] * shrink + jnp.sum(weights, axis=1, keepdims=True)
                acc_ref[...] = acc_ref[...] * shrink + jnp.dot(
                    weights.astype(jnp.bfloat16),
                    value_ref[keys, :],
                    preferred_element_type=jnp.float32,
                )

        attn_ref[rows, :] = (acc_ref[...] / sum_ref[...]).astype(jnp.bfloat16)
        lse_ref[rows, :] = top_ref[...] + jnp.log(sum_ref[...])


def attend_grad_kernel(
    order_ref,
    bounds_ref,
    query_ref,
    key_ref,
    value_ref,
    attn_ref,
    grad_ref,
    lse_ref,
    cos_ref,
    low_ref,
    high_ref,
    seg_col_ref,
    seg_row_ref,
    out_ref,
    sums_ref,
    query_acc,
    key_acc,
    value_acc,
    delta_ref,
    *,
    block,
    count,
):
    score_scale = 1.0 / math.sqrt(HD)
    query_acc[...] = jnp.zeros_like(query_acc)
    delta_ref[...] = jnp.sum(
        grad_ref[...].astype(jnp.float32) * attn_ref[...].astype(jnp.float32),
        axis=1,
        keepdims=True,
    )

    @pl.loop(0, count)
    def _(k_index):
        keys = pl.ds(pl.multiple_of(k_index * block, block), block)
        key_acc[...] = jnp.zeros_like(key_acc)
        value_acc[...] = jnp.zeros_like(value_acc)

        @pl.loop(0, count)
        def _(q_index):
            @pl.when(block_meets(bounds_ref, order_ref, q_index, k_index))
            def _():
                rows = pl.ds(pl.multiple_of(q_index * block, block), block)
                query, key_rows = query_ref[rows, :], key_ref[keys, :]
                grad_rows = grad_ref[rows, :]
                scores = contract_last(query, key_rows) * score_scale
                allowed = pair_mask(order_ref, seg_col_ref, seg_row_ref, q_index, k_index, block)
                probs = jnp.where(allowed, jnp.exp(scores - lse_ref[rows, :]), 0.0)
                prob_grad = contract_last(grad_rows, value_ref[keys, :])
                score_grad = (probs * (prob_grad - delta_ref[rows, :])).astype(jnp.bfloat16)
                value_acc[...] += contract_first(probs.astype(jnp.bfloat16), grad_rows)
                key_acc[...] += contract_first(score_grad, query)
                query_acc[rows, :] += jnp.dot(
                    score_grad, key_rows, preferred_element_type=jnp.float32
                )

        tables = (cos_ref[keys, :], low_ref[keys, :], high_ref[keys, :])
        key_low = turn(key_acc[:, :LANES] * score_scale, *tables, -1.0)
        key_high = key_acc[:, LANES:] * score_scale
        first = k_index == 0
        for start, part in ((HD, key_low), (HD + LANES, key_high), (2 * HD, value_acc[...])):
            columns = slice(start, start + part.shape[1])
            out_ref[keys, columns] = part.astype(jnp.bfloat16)
            sums_ref[:, columns] = jnp.where(first, 0.0, sums_ref[:, columns]) + jnp.sum(
                part, axis=0, keepdims=True
            )

    sums_ref[:, :HD] = jnp.zeros((1, HD), jnp.float32)

    @pl.loop(0, count)
    def _(q_index):
        rows = pl.ds(pl.multiple_of(q_index * block, block), block)
        tables = (cos_ref[rows, :], low_ref[rows, :], high_ref[rows, :])
        query_low = turn(query_acc[rows, :LANES] * score_scale, *tables, -1.0)
        query_high = query_acc[rows, LANES:] * score_scale
        for start, part in ((0, query_low), (LANES, query_high)):
            columns = slice(start, start + part.shape[1])
            out_ref[rows, columns] = part.astype(jnp.bfloat16)
            sums_ref[:, columns] += jnp.sum(part, axis=0, keepdims=True)


MESH = pl.DeviceIdType.MESH


def opening_kernel(*refs, side, second, ranks, square, sizes):
    count = len(sizes)
    gathered_in, refs = refs[:count], refs[count:]
    rows_in, refs = refs[:2], refs[2:]
    later_in, refs = refs[:2], refs[2:]
    gathered_out, refs = refs[:count], refs[count:]
    rows_out, refs = refs[:2], refs[2:]
    later_out, refs = refs[0], refs[1:]
    held, refs = refs[:count], refs[count:]
    held_rows, refs = refs[:2], refs[2:]
    held_later, refs = refs[:2], refs[2:]
    load_sem, store_sem, send_sem, recv_sem, row_send, row_recv = refs

    shard, rank = lax.axis_index("shard"), lax.axis_index("ctx")
    slow, fast = shard // second, shard % second
    flip = rank % 2 if square else 1
    here_first = fast * (1 - flip) + slow * flip
    here_second = slow * (1 - flip) + fast * flip

    def peer(first_step, second_step):
        first = (here_first + first_step + side) % side
        other = (here_second + second_step + second) % second
        return (other * side + first) * (1 - flip) + (first * second + other) * flip

    first_peers = [peer(a, 0) for a in range(1, side)]
    second_peers = [peer(0, b) for b in range(1, second)]
    rank_peers = [(rank + j) % ranks for j in range(1, ranks)]
    barrier = pltpu.get_barrier_semaphore()
    for target in first_peers + second_peers:
        pl.semaphore_signal(barrier, inc=1, device_id={"shard": target}, device_id_type=MESH)
    for target in rank_peers:
        pl.semaphore_signal(barrier, inc=1, device_id={"ctx": target}, device_id_type=MESH)

    loads = []
    for number in range(count):
        source = gathered_in[number]
        if sizes[number] is not None:
            columns = pl.ds(pl.multiple_of(rank * sizes[number], LANES), sizes[number])
            source = source.at[:, columns]
        loads.append(pltpu.make_async_copy(source, held[number], load_sem.at[number]))
    for number in range(2):
        loads.append(
            pltpu.make_async_copy(rows_in[number], held_rows[number], load_sem.at[count + number])
        )
    for number in range(2):
        size = held_later[number].shape[1]
        columns = pl.ds(pl.multiple_of(rank * size, LANES), size)
        loads.append(
            pltpu.make_async_copy(
                later_in[number].at[:, columns], held_later[number], load_sem.at[count + 2 + number]
            )
        )
    for load in loads:
        load.start()
    pl.semaphore_wait(barrier, len(first_peers) + len(second_peers) + len(rank_peers))

    def place(number, first_step, second_step):
        rows = held[number].shape[0]
        start = pl.multiple_of(peer(first_step, second_step) * rows, 16)
        return gathered_out[number].at[pl.ds(start, rows), :]

    copies, slot = {}, 0
    steps = side - 1 + (second - 1) * side

    def send(number, source, a, b, target, key):
        slot = number * steps + key
        copy = pltpu.make_async_remote_copy(
            src_ref=source,
            dst_ref=place(number, a, b),
            send_sem=send_sem.at[slot],
            recv_sem=recv_sem.at[slot],
            device_id={"shard": target},
            device_id_type=MESH,
        )
        copy.start()
        copies[number, key] = copy

    for number in range(count):
        loads[number].wait()
        for a in range(1, side):
            send(number, held[number], 0, 0, first_peers[a - 1], a - 1)
        for b in range(1, second):
            send(number, held[number], 0, 0, second_peers[b - 1], side - 1 + (b - 1) * side)
    row_copies = []
    for number in range(2):
        loads[count + number].wait()
        rows = held_rows[number].shape[0]
        for j in range(1, ranks):
            slot = number * (ranks - 1) + j - 1
            copy = pltpu.make_async_remote_copy(
                src_ref=held_rows[number],
                dst_ref=rows_out[number].at[pl.ds((ranks - j) * rows, rows), :],
                send_sem=row_send.at[slot],
                recv_sem=row_recv.at[slot],
                device_id={"ctx": rank_peers[j - 1]},
                device_id_type=MESH,
            )
            copy.start()
            row_copies.append(copy)
    stores = []
    for number in range(count):
        stores.append(
            pltpu.make_async_copy(held[number], place(number, 0, 0), store_sem.at[number])
        )
    for number in range(2):
        rows = held_rows[number].shape[0]
        stores.append(
            pltpu.make_async_copy(
                held_rows[number],
                rows_out[number].at[pl.ds(0, rows), :],
                store_sem.at[count + number],
            )
        )
    for number in range(2):
        loads[count + 2 + number].wait()
        size = held_later[number].shape[1]
        stores.append(
            pltpu.make_async_copy(
                held_later[number],
                later_out.at[:, pl.ds(number * size, size)],
                store_sem.at[count + 2 + number],
            )
        )
    for store in stores:
        store.start()
    for number in range(count):
        for a in range(1, side):
            copies[number, a - 1].wait_recv()
            for b in range(1, second):
                key = side - 1 + (b - 1) * side + a
                send(number, place(number, -a, 0), -a, 0, second_peers[b - 1], key)
    for store in stores:
        store.wait()
    for (number, key), copy in copies.items():
        copy.wait_send()
        if key >= side - 1:
            copy.wait_recv()
    for copy in row_copies:
        copy.wait_send()
        copy.wait_recv()


def opening(gathered, split, rows, later, ranks):
    shards = lax.axis_size("shard")
    side = math.isqrt(shards)
    square = side * side == shards
    if not square:
        side = 1
    second = shards // side
    sizes = [v.shape[1] // ranks if cut else None for v, cut in zip(gathered, split)]
    held = [(v.shape[0], size or v.shape[1]) for v, size in zip(gathered, sizes)]
    held_later = [(v.shape[0], v.shape[1] // ranks) for v in later]
    count, steps = len(gathered), side - 1 + (second - 1) * side
    bf16 = jnp.bfloat16
    out_shapes = (
        [jax.ShapeDtypeStruct((h[0] * shards, h[1]), bf16) for h in held]
        + [jax.ShapeDtypeStruct((v.shape[0] * ranks, v.shape[1]), bf16) for v in rows]
        + [jax.ShapeDtypeStruct((held_later[0][0], 2 * held_later[0][1]), bf16)]
    )
    hbm = pl.BlockSpec(memory_space=pl.ANY)
    total = count + 4
    row_slots = max(1, 2 * (ranks - 1))
    outs = pl.pallas_call(
        functools.partial(
            opening_kernel, side=side, second=second, ranks=ranks, square=square, sizes=sizes
        ),
        out_shape=tuple(out_shapes),
        in_specs=[hbm] * total,
        out_specs=(hbm,) * (total - 1),
        scratch_shapes=[pltpu.VMEM(h, bf16) for h in held]
        + [pltpu.VMEM(v.shape, bf16) for v in rows]
        + [pltpu.VMEM(h, bf16) for h in held_later]
        + [
            pltpu.SemaphoreType.DMA((total,)),
            pltpu.SemaphoreType.DMA((total,)),
            pltpu.SemaphoreType.DMA((count * steps,)),
            pltpu.SemaphoreType.DMA((count * steps,)),
            pltpu.SemaphoreType.DMA((row_slots,)),
            pltpu.SemaphoreType.DMA((row_slots,)),
        ],
        compiler_params=pltpu.CompilerParams(
            collective_id=0, has_side_effects=True, vmem_limit_bytes=VMEM_LIMIT
        ),
        name="opening",
    )(*gathered, *rows, *later)
    return outs[:count], outs[count : count + 2], outs[count + 2]


def pair_product_kernel(left_ref, right_ref, left_weight, right_weight, *refs):
    out_ref = refs[-1]
    out_ref[...] = (
        contract_last(left_ref[...], left_weight[...])
        + contract_last(right_ref[...], right_weight[...])
    ).astype(out_ref.dtype)


def block_sum_kernel(index_ref, whole_ref, *refs, count):
    del index_ref
    total = whole_ref[...].astype(jnp.float32)
    for ref in refs[:count]:
        total = total + ref[...].astype(jnp.float32)
    refs[-1][...] = total.astype(refs[-1].dtype)


def block_sum(whole, index, received, after, dtype):
    rows, columns = received[0].shape
    step = min(rows, 256)
    tiles = rows // step
    tile = pl.BlockSpec((step, columns), lambda i, index: (i, 0))
    return pl.pallas_call(
        functools.partial(block_sum_kernel, count=len(received)),
        grid_spec=pltpu.PrefetchScalarGridSpec(
            num_scalar_prefetch=1,
            grid=(tiles,),
            in_specs=[pl.BlockSpec((step, columns), lambda i, index: (index[0] * tiles + i, 0))]
            + [tile] * len(received)
            + [pl.BlockSpec(memory_space=pl.ANY)] * len(after),
            out_specs=tile,
        ),
        out_shape=jax.ShapeDtypeStruct((rows, columns), dtype),
        cost_estimate=pl.CostEstimate(
            flops=rows * columns, bytes_accessed=6 * rows * columns, transcendentals=0
        ),
        name="block_sum",
    )(jnp.asarray(index, jnp.int32).reshape(1), whole, *received, *after)


def norm_grad_kernel(
    left_ref,
    right_ref,
    x_ref,
    left_weight,
    right_weight,
    left_gain,
    right_gain,
    after_ref,
    out_ref,
    sums_ref,
):
    del after_ref
    x = x_ref[...].astype(jnp.float32)
    centered = x - jnp.mean(x, axis=-1, keepdims=True)
    inverse = lax.rsqrt(jnp.mean(centered * centered, axis=-1, keepdims=True) + EPSILON)
    hat = centered * inverse
    left = contract_last(left_ref[...], left_weight[...])
    right = contract_last(right_ref[...], right_weight[...])
    scaled = left * left_gain[...] + right * right_gain[...]
    first = pl.program_id(0) == 0
    for row, part in enumerate((left * hat, left, right * hat, right)):
        total = jnp.sum(part, axis=0, keepdims=True)
        sums_ref[row : row + 1, :] = jnp.where(first, 0.0, sums_ref[row : row + 1, :]) + total
    inner = (
        scaled
        - jnp.mean(scaled, axis=-1, keepdims=True)
        - hat * jnp.mean(scaled * hat, axis=-1, keepdims=True)
    )
    out_ref[...] = (inverse * inner).astype(out_ref.dtype)


ROWS_STEP = 256


def row_specs(arrays, start, rows):
    step = min(ROWS_STEP, rows)
    return step, [
        pl.BlockSpec((step, v.shape[1]), lambda i, first=start // step: (first + i, 0))
        for v in arrays
    ]


def whole_spec(array):
    return pl.BlockSpec(array.shape, lambda i: (0, 0))


def half_spec(array, half):
    return pl.BlockSpec((array.shape[0], array.shape[1] // 2), lambda i: (0, half))


def pair_product(left, right, left_weight, right_weight, after, start, rows):
    step, specs = row_specs((left, right), start, rows)
    width = left_weight.shape[0]
    return pl.pallas_call(
        pair_product_kernel,
        grid=(rows // step,),
        out_shape=jax.ShapeDtypeStruct((rows, width), jnp.bfloat16),
        in_specs=specs
        + [whole_spec(left_weight), half_spec(right_weight, 1)]
        + [pl.BlockSpec(memory_space=pl.ANY)] * len(after),
        out_specs=pl.BlockSpec((step, width), lambda i: (i, 0)),
        compiler_params=pltpu.CompilerParams(vmem_limit_bytes=VMEM_LIMIT),
        cost_estimate=pl.CostEstimate(
            flops=2 * rows * width * (left.shape[1] + right.shape[1]),
            bytes_accessed=2 * rows * (width + left.shape[1] + right.shape[1]),
            transcendentals=0,
        ),
        name="pair_product",
    )(left, right, left_weight, right_weight, *after)


def norm_grad(
    left, right, x, left_weight, right_weight, left_gain, right_gain, after, start, rows
):
    step, specs = row_specs((left, right, x), start, rows)
    width = left_weight.shape[0]
    rest = [left_weight, right_weight, left_gain, right_gain]
    return pl.pallas_call(
        norm_grad_kernel,
        grid=(rows // step,),
        out_shape=(
            jax.ShapeDtypeStruct((rows, width), jnp.bfloat16),
            jax.ShapeDtypeStruct((4, width), jnp.float32),
        ),
        in_specs=specs
        + [whole_spec(left_weight), half_spec(right_weight, 0)]
        + [whole_spec(v) for v in rest[2:]]
        + [pl.BlockSpec(memory_space=pl.ANY)],
        out_specs=(
            pl.BlockSpec((step, width), lambda i: (i, 0)),
            pl.BlockSpec((4, width), lambda i: (0, 0)),
        ),
        compiler_params=pltpu.CompilerParams(vmem_limit_bytes=VMEM_LIMIT),
        cost_estimate=pl.CostEstimate(
            flops=2 * rows * width * (left.shape[1] + right.shape[1]),
            bytes_accessed=2 * rows * (2 * width + left.shape[1] + right.shape[1]),
            transcendentals=0,
        ),
        name="norm_grad",
    )(left, right, x, *rest, after)


SCALAR = pl.BlockSpec(memory_space=pltpu.SMEM)
VECTOR = pl.BlockSpec(memory_space=pltpu.VMEM)


def attend(order, bounds, proj, tables, seg_col, seg_row, block, count):
    length = proj.shape[0]
    pairs = length * length
    return pl.pallas_call(
        functools.partial(attend_kernel, block=block, count=count),
        out_shape=(
            jax.ShapeDtypeStruct((length, HD), jnp.bfloat16),
            jax.ShapeDtypeStruct((length, HD), jnp.bfloat16),
            jax.ShapeDtypeStruct((length, HD), jnp.bfloat16),
            jax.ShapeDtypeStruct((length, HD), jnp.bfloat16),
            jax.ShapeDtypeStruct((length, 1), jnp.float32),
        ),
        in_specs=[SCALAR] * 2 + [VECTOR] * 6,
        out_specs=(VECTOR,) * 5,
        scratch_shapes=[
            pltpu.VMEM((block, 1), jnp.float32),
            pltpu.VMEM((block, 1), jnp.float32),
            pltpu.VMEM((block, HD), jnp.float32),
        ],
        compiler_params=pltpu.CompilerParams(vmem_limit_bytes=VMEM_LIMIT),
        cost_estimate=pl.CostEstimate(
            flops=2 * pairs * HD, bytes_accessed=16 * length * HD, transcendentals=pairs // 2
        ),
        name="attend",
    )(order, bounds, proj, *tables, seg_col, seg_row)


def attend_grad(
    order, bounds, query, key, value, attn, grad, lse, tables, seg_col, seg_row, block, count
):
    length = query.shape[0]
    pairs = length * length
    return pl.pallas_call(
        functools.partial(attend_grad_kernel, block=block, count=count),
        out_shape=(
            jax.ShapeDtypeStruct((length, 3 * HD), jnp.bfloat16),
            jax.ShapeDtypeStruct((1, 3 * HD), jnp.float32),
        ),
        in_specs=[SCALAR] * 2 + [VECTOR] * 11,
        out_specs=(VECTOR,) * 2,
        scratch_shapes=[
            pltpu.VMEM((length, HD), jnp.float32),
            pltpu.VMEM((block, HD), jnp.float32),
            pltpu.VMEM((block, HD), jnp.float32),
            pltpu.VMEM((length, 1), jnp.float32),
        ],
        compiler_params=pltpu.CompilerParams(vmem_limit_bytes=VMEM_LIMIT),
        cost_estimate=pl.CostEstimate(
            flops=5 * pairs * HD, bytes_accessed=16 * length * HD, transcendentals=pairs // 2
        ),
        name="attend_grad",
    )(order, bounds, query, key, value, attn, grad, lse, *tables, seg_col, seg_row)


def ring_shift(value, axis, step):
    count = lax.axis_size(axis)
    return lax.ppermute(value, axis, [(i, (i + step) % count) for i in range(count)])


class Plane:
    def __init__(self):
        self.count = lax.axis_size("shard")
        side = math.isqrt(self.count)
        self.square = side * side == self.count
        self.first, self.second = (side, side) if self.square else (1, self.count)
        self.ranks = lax.axis_size("ctx")
        shard = lax.axis_index("shard")
        self.flip = (lax.axis_index("ctx") % 2 == 1) if self.square else False
        slow, fast = shard // self.second, shard % self.second
        if self.square:
            self.here = (jnp.where(self.flip, slow, fast), jnp.where(self.flip, fast, slow))
        else:
            self.here = (slow, fast)

    def index(self, first_step, second_step):
        first = lax.rem(self.here[0] + first_step + self.first, self.first)
        second = lax.rem(self.here[1] + second_step + self.second, self.second)
        if not self.square:
            return first * self.second + second
        side = self.first
        return jnp.where(self.flip, first * side + second, second * side + first)

    def move(self, value, first_step, second_step):
        pairs = []
        for shard in range(self.count):
            for rank in range(self.ranks):
                slow, fast = divmod(shard, self.second)
                if self.square and rank % 2 == 0:
                    slow = (slow + second_step) % self.second
                    fast = (fast + first_step) % self.first
                else:
                    slow = (slow + first_step) % self.first
                    fast = (fast + second_step) % self.second
                target = slow * self.second + fast
                pairs.append((shard * self.ranks + rank, target * self.ranks + rank))
        return lax.ppermute(value, ("shard", "ctx"), pairs)

    def scatter_sum(self, partial, after):
        rows = partial.shape[0] // self.count
        sums, final = {}, []
        for b in list(range(1, self.second)) + [0]:
            received = []
            for a in range(1, self.first):
                block = lax.dynamic_slice_in_dim(partial, self.index(a, b) * rows, rows)
                received.append(self.move(block, a, 0))
            if b == 0:
                final = received
            elif received:
                sums[b] = block_sum(partial, self.index(0, b), received, after, partial.dtype)
            else:
                sums[b] = lax.dynamic_slice_in_dim(partial, self.index(0, b) * rows, rows)
        final = final + [self.move(sums[b], 0, b) for b in range(1, self.second)]
        return block_sum(partial, self.index(0, 0), final, after, jnp.float32)

    def full_sum(self, value):
        total = value
        for a in range(1, self.first):
            total = total + self.move(value, a, 0)
        value = total
        for b in range(1, self.second):
            total = total + self.move(value, 0, b)
        return total


def local(
    hidden_in,
    grad_out,
    segment_ids,
    group_order,
    ln1_gain,
    ln1_bias,
    qkv_weight,
    qkv_bias,
    dense_weight,
    dense_bias,
    ln2_gain,
    ln2_bias,
    up_weight,
    up_bias,
    down_weight,
    down_bias,
):
    _, groups_dev, block_len, width = hidden_in.shape
    tokens = groups_dev * block_len
    seq_len = segment_ids.shape[1]
    groups = seq_len // block_len
    ctx_count, tp_count = lax.axis_size("ctx"), lax.axis_size("tp")
    shard_count = lax.axis_size("shard")
    ctx_rank, tp_rank = lax.axis_index("ctx"), lax.axis_index("tp")
    shard_rank = lax.axis_index("shard")
    slice_width = width // tp_count
    bf16, f32 = jnp.bfloat16, jnp.float32

    def my_columns(matrix):
        columns = matrix.shape[1] // ctx_count
        return lax.dynamic_slice_in_dim(matrix, ctx_rank * columns, columns, 1)

    plane = Plane()

    x_mine = hidden_in.reshape(tokens, width)
    g_mine = grad_out.reshape(tokens, width)
    vectors = [
        ln1_gain, ln1_bias, ln2_gain, ln2_bias, dense_bias, down_bias, qkv_bias[0], up_bias[0],
    ]
    sizes = [v.shape[0] for v in vectors]
    wide = -(-max(sizes) // LANES) * LANES
    packed = jnp.stack([jnp.pad(v, (0, wide - v.shape[0])) for v in vectors])
    packed = jnp.concatenate([packed, jnp.zeros_like(packed)], axis=0)
    (w_vectors, w_qkv, w_dense), (x_row, g_row), wide_mine = opening(
        [packed, qkv_weight, dense_weight],
        [False, True, True],
        [x_mine, g_mine],
        [up_weight, down_weight],
        ctx_count,
    )
    w_wide = lax.all_gather(wide_mine, "shard", axis=0, tiled=True)
    units = w_wide.shape[1] // 2
    w_up, w_down = w_wide[:, :units], w_wide[:, units:]
    w_vectors = w_vectors.reshape(shard_count, packed.shape[0], wide)
    spread = [
        w_vectors[:, number, :size].reshape(-1).astype(f32) for number, size in enumerate(sizes)
    ]
    gain_one, shift_one, gain_two, shift_two, bias_dense, bias_down, bias_qkv, bias_up = spread
    bias_qkv = my_columns(bias_qkv[None])
    bias_up = my_columns(bias_up[None])
    plane = Plane()
    heads_here = w_qkv.shape[1] // (3 * HD)

    own_order = jnp.concatenate(
        [
            lax.dynamic_slice_in_dim(
                group_order, lax.rem(ctx_rank + k, ctx_count) * groups_dev, groups_dev
            )
            for k in range(ctx_count)
        ]
    )
    segments = segment_ids[0]
    positions = segment_positions(segments)

    def stored(values):
        return jnp.concatenate(
            [
                lax.dynamic_slice_in_dim(values, own_order[k] * block_len, block_len)
                for k in range(groups)
            ]
        )

    seg_stored = stored(segments)
    tables = rotary_tables(stored(positions))
    seg_blocks = seg_stored.reshape(groups, block_len)
    bounds = jnp.stack([seg_blocks[:, 0], seg_blocks[:, -1]])
    seg_col, seg_row = seg_stored[:, None], seg_stored[None, :]

    x_float = x_row.astype(f32)
    centered = x_float - jnp.mean(x_float, axis=-1, keepdims=True)
    inverse = lax.rsqrt(jnp.mean(centered * centered, axis=-1, keepdims=True) + EPSILON)
    hat = centered * inverse
    acts_one = (hat * gain_one + shift_one).astype(bf16)
    acts_two = (hat * gain_two + shift_two).astype(bf16)

    projected = jnp.dot(acts_one, w_qkv, preferred_element_type=f32) + bias_qkv
    heads = []
    for h in range(heads_here):
        heads.append(
            attend(
                own_order,
                bounds,
                projected[:, 3 * HD * h : 3 * HD * (h + 1)],
                tables,
                seg_col,
                seg_row,
                block_len,
                groups,
            )
        )
    attn = jnp.concatenate([head[3] for head in heads], axis=1)

    attn_grad = jnp.dot(g_row, w_dense, preferred_element_type=f32).astype(bf16)
    proj_parts, sum_parts = [], []
    for h, (query, key, value, attn_head, lse) in enumerate(heads):
        part, sums = attend_grad(
            own_order,
            bounds,
            query,
            key,
            value,
            attn_head,
            attn_grad[:, HD * h : HD * (h + 1)],
            lse,
            tables,
            seg_col,
            seg_row,
            block_len,
            groups,
        )
        proj_parts.append(part)
        sum_parts.append(sums[0])
    proj_grad_b = jnp.concatenate(proj_parts, axis=1)
    qkv_bias_grad = jnp.concatenate(sum_parts)

    pre_act = jnp.dot(acts_two, w_up, preferred_element_type=f32) + bias_up
    cdf = 0.5 * (1.0 + lax.erf(pre_act * (1.0 / math.sqrt(2.0))))
    hidden = (pre_act * cdf).astype(bf16)
    slope = cdf + pre_act * jnp.exp(-0.5 * pre_act * pre_act) * (1.0 / math.sqrt(2.0 * math.pi))

    def reduce_partial(parts):
        received = [ring_shift(parts[k], "ctx", k) for k in range(1, ctx_count)]
        total = block_sum(parts[0], 0, received, [], bf16)
        return total, lax.psum_scatter(total, "tp", scatter_dimension=1, tiled=True).astype(f32)

    out_parts = {}
    for k in reversed(range(ctx_count)):
        out_parts[k] = pair_product(
            attn,
            hidden,
            w_dense,
            w_wide,
            [proj_grad_b] if k + 1 == ctx_count else [out_parts[k + 1]],
            k * tokens,
            tokens,
        )
    out_total, summed_out = reduce_partial(out_parts)
    out_shift = lax.dynamic_slice_in_dim(bias_dense + bias_down, tp_rank * slice_width, slice_width)
    x_slice = lax.dynamic_slice_in_dim(x_mine, tp_rank * slice_width, slice_width, 1)
    output = x_slice.astype(f32) + summed_out + out_shift

    def reduce_weight(grad, after):
        mine = plane.scatter_sum(grad, after)
        rows, columns = mine.shape
        whole = jnp.zeros((rows, columns * ctx_count), f32)
        for k in range(ctx_count):
            part = mine if k == 0 else ring_shift(mine.astype(bf16), "ctx", ctx_count - k)
            place = lax.rem(ctx_rank + k, ctx_count) * columns
            whole = lax.dynamic_update_slice_in_dim(whole, part.astype(f32), place, 1)
        return whole

    bias_grad = jnp.sum(g_row.astype(f32), axis=0)

    pre_grad = jnp.dot(g_row, w_down, preferred_element_type=f32) * slope
    up_bias_grad = jnp.sum(pre_grad, axis=0)
    pre_grad_b = pre_grad.astype(bf16)

    in_parts, norm_sums = {}, jnp.zeros((4, width), f32)
    for k in reversed(range(ctx_count)):
        in_parts[k], sums = norm_grad(
            proj_grad_b,
            pre_grad_b,
            x_row,
            w_qkv,
            w_wide,
            gain_one[None],
            gain_two[None],
            in_parts[k + 1] if k + 1 in in_parts else out_total,
            k * tokens,
            tokens,
        )
        norm_sums = norm_sums + sums
    _, input_sum = reduce_partial(in_parts)
    g_slice = lax.dynamic_slice_in_dim(g_mine, tp_rank * slice_width, slice_width, 1)
    input_grad = g_slice.astype(f32) + input_sum

    down_local = contract_first(g_row, hidden).astype(bf16)
    dense_local = contract_first(g_row, attn).astype(bf16)
    qkv_local = contract_first(acts_one, proj_grad_b).astype(bf16)
    up_local = contract_first(acts_two, pre_grad_b).astype(bf16)
    late = [dense_local, qkv_local, up_local]
    down_grad = reduce_weight(down_local, [in_parts[0]])
    dense_grad = reduce_weight(dense_local, late)
    qkv_grad = reduce_weight(qkv_local, late)
    up_grad = reduce_weight(up_local, late)

    norm_sums = norm_sums.reshape(-1)
    column_sums = [up_bias_grad, qkv_bias_grad]
    packed = jnp.concatenate([norm_sums] + column_sums)
    wholes = [jnp.zeros((v.shape[0] * ctx_count,), f32) for v in column_sums]
    total = jnp.zeros_like(norm_sums)
    for k in range(ctx_count):
        part = packed if k == 0 else ring_shift(packed, "ctx", ctx_count - k)
        total = total + part[: norm_sums.shape[0]]
        offset = norm_sums.shape[0]
        for number, vector in enumerate(column_sums):
            size = vector.shape[0]
            wholes[number] = lax.dynamic_update_slice_in_dim(
                wholes[number],
                part[offset : offset + size],
                lax.rem(ctx_rank + k, ctx_count) * size,
                0,
            )
            offset += size
    norm_sums = total
    for k in range(1, tp_count):
        norm_sums = norm_sums + ring_shift(total, "tp", k)
    pieces = [bias_grad] + wholes + [
        norm_sums[k * width : (k + 1) * width] for k in range(4)
    ]
    reduced = plane.full_sum(jnp.concatenate(pieces))
    results, offset = [], 0
    for piece in pieces:
        own = piece.shape[0] // shard_count
        results.append(lax.dynamic_slice_in_dim(reduced, offset + shard_rank * own, own))
        offset += piece.shape[0]
    bias_grad, up_bias_grad, qkv_bias_grad = results[:3]
    gain_one_grad, shift_one_grad, gain_two_grad, shift_two_grad = results[3:]
    out_shape = hidden_in.shape[:3] + (slice_width,)
    return (
        output.reshape(out_shape),
        input_grad.reshape(out_shape),
        gain_one_grad,
        shift_one_grad,
        qkv_grad,
        qkv_bias_grad[None],
        dense_grad,
        bias_grad,
        gain_two_grad,
        shift_two_grad,
        up_grad,
        up_bias_grad[None],
        down_grad,
    )


def solution(mesh):
    return jax.shard_map(
        local,
        mesh=mesh,
        in_specs=(
            P("shard", "ctx", None, None),
            P("shard", "ctx", None, None),
            P("shard", None),
            P(),
            P("shard"),
            P("shard"),
            P("shard", "tp"),
            P("tp", "shard"),
            P("shard", "tp"),
            P("shard"),
            P("shard"),
            P("shard"),
            P("shard", "tp"),
            P("tp", "shard"),
            P("shard", "tp"),
            P("shard"),
        ),
        out_specs=(
            P("shard", "ctx", None, "tp"),
            P("shard", "ctx", None, "tp"),
            P("shard"),
            P("shard"),
            P("shard", "tp"),
            P("tp", "shard"),
            P("shard", "tp"),
            P("shard"),
            P("shard"),
            P("shard"),
            P("shard", "tp"),
            P("tp", "shard"),
            P("shard", "tp"),
        ),
        check_vma=False,
    )
```

```python
import functools
import math

import jax
import jax.numpy as jnp
from jax import lax
from jax.experimental import pallas as pl
from jax.experimental.pallas import tpu as pltpu
from jax.sharding import PartitionSpec as P


HD = 256
ROT = 64
LANES = 128

EPSILON = 1e-05
ROTARY_BASE = 10000.0
NEG = -1e30
VMEM_LIMIT = 56 * 1024 * 1024


def segment_positions(segments):
    length_all = segments.shape[0]
    index_row = jnp.arange(length_all, dtype=jnp.int32)
    changed = jnp.concatenate(
        [jnp.ones((1,), dtype=jnp.bool_), segments[1:] != segments[:-1]]
    )
    seg_start = jnp.where(changed, index_row, jnp.zeros_like(segments))
    return index_row - lax.cummax(seg_start, axis=0)


def rotary_tables(positions):
    half_rot = ROT // 2
    frequency = ROTARY_BASE ** (-2.0 * jnp.arange(half_rot, dtype=jnp.float32) / ROT)
    angles = positions.astype(jnp.float32)[:, None] * frequency[None, :]
    cosine, sine = jnp.cos(angles), jnp.sin(angles)
    count = positions.shape[0]
    rest_one = jnp.ones((count, LANES - ROT), jnp.float32)
    rest_zero = jnp.zeros((count, LANES - half_rot), jnp.float32)
    cosine_table = jnp.concatenate([cosine, cosine, rest_one], axis=1)
    low_table = jnp.concatenate([-sine, rest_zero], axis=1)
    high_table = jnp.concatenate(
        [jnp.zeros_like(sine), sine, rest_zero[:, : LANES - ROT]], axis=1
    )
    return cosine_table, low_table, high_table


def turn(values, cosine, low, high, sign):
    half_rot = ROT // 2
    down = pltpu.roll(values, LANES - half_rot, 1)
    up = pltpu.roll(values, half_rot, 1)
    return values * cosine + sign * (down * low + up * high)


def contract_first(left_mat, right_mat):
    return lax.dot_general(
        left_mat, right_mat, (((0,), (0,)), ((), ())), preferred_element_type=jnp.float32
    )


def contract_last(left_mat, right_mat):
    return lax.dot_general(
        left_mat, right_mat, (((1,), (1,)), ((), ())), preferred_element_type=jnp.float32
    )


def block_meets(bounds_ref, order_ref, q_index, k_index):
    return (
        (order_ref[k_index] <= order_ref[q_index])
        & (bounds_ref[0, k_index] <= bounds_ref[1, q_index])
        & (bounds_ref[1, k_index] >= bounds_ref[0, q_index])
    )


def pair_mask(order_ref, seg_col_ref, seg_row_ref, q_index, k_index, block):
    q_place = order_ref[q_index] * block + lax.broadcasted_iota(jnp.int32, (block, block), 0)
    k_place = order_ref[k_index] * block + lax.broadcasted_iota(jnp.int32, (block, block), 1)
    seg_q = seg_col_ref[pl.ds(q_index * block, block), :]
    seg_k = seg_row_ref[:, pl.ds(pl.multiple_of(k_index * block, block), block)]
    return (k_place <= q_place) & (seg_q == seg_k)


def attend_kernel(
    order_ref,
    bounds_ref,
    proj_ref,
    cos_ref,
    low_ref,
    high_ref,
    seg_col_ref,
    seg_row_ref,
    query_ref,
    key_ref,
    value_ref,
    attn_ref,
    lse_ref,
    top_ref,
    sum_ref,
    acc_ref,
    *,
    block,
    count,
):
    score_scale = 1.0 / math.sqrt(HD)
    for index in range(count):
        rows = pl.ds(index * block, block)
        tables = (cos_ref[rows, :], low_ref[rows, :], high_ref[rows, :])
        for start, out in ((0, query_ref), (HD, key_ref)):
            out[rows, :LANES] = turn(
                proj_ref[rows, start : start + LANES], *tables, 1.0
            ).astype(jnp.bfloat16)
            out[rows, LANES:] = proj_ref[rows, start + LANES : start + HD].astype(jnp.bfloat16)
        value_ref[rows, :] = proj_ref[rows, 2 * HD :].astype(jnp.bfloat16)

    @pl.loop(0, count)
    def _(q_index):
        rows = pl.ds(pl.multiple_of(q_index * block, block), block)
        top_ref[...] = jnp.full_like(top_ref, NEG)
        sum_ref[...] = jnp.zeros_like(sum_ref)
        acc_ref[...] = jnp.zeros_like(acc_ref)

        @pl.loop(0, count)
        def _(k_index):
            @pl.when(block_meets(bounds_ref, order_ref, q_index, k_index))
            def _():
                keys = pl.ds(pl.multiple_of(k_index * block, block), block)
                scores = contract_last(query_ref[rows, :], key_ref[keys, :]) * score_scale
                allowed = pair_mask(order_ref, seg_col_ref, seg_row_ref, q_index, k_index, block)
                scores = jnp.where(allowed, scores, NEG)
                old_top = top_ref[...]
                new_top = jnp.maximum(old_top, jnp.max(scores, axis=1, keepdims=True))
                shrink = jnp.exp(old_top - new_top)
                weights = jnp.where(allowed, jnp.exp(scores - new_top), 0.0)
                top_ref[...] = new_top
                sum_ref[...] = sum_ref[...] * shrink + jnp.sum(weights, axis=1, keepdims=True)
                acc_ref[...] = acc_ref[...] * shrink + jnp.dot(
                    weights.astype(jnp.bfloat16),
                    value_ref[keys, :],
                    preferred_element_type=jnp.float32,
                )

        attn_ref[rows, :] = (acc_ref[...] / sum_ref[...]).astype(jnp.bfloat16)
        lse_ref[rows, :] = top_ref[...] + jnp.log(sum_ref[...])


def attend_grad_kernel(
    order_ref,
    bounds_ref,
    query_ref,
    key_ref,
    value_ref,
    attn_ref,
    grad_ref,
    lse_ref,
    cos_ref,
    low_ref,
    high_ref,
    seg_col_ref,
    seg_row_ref,
    out_ref,
    sums_ref,
    query_acc,
    key_acc,
    value_acc,
    delta_ref,
    *,
    block,
    count,
):
    score_scale = 1.0 / math.sqrt(HD)
    query_acc[...] = jnp.zeros_like(query_acc)
    delta_ref[...] = jnp.sum(
        grad_ref[...].astype(jnp.float32) * attn_ref[...].astype(jnp.float32),
        axis=1,
        keepdims=True,
    )

    @pl.loop(0, count)
    def _(k_index):
        keys = pl.ds(pl.multiple_of(k_index * block, block), block)
        key_acc[...] = jnp.zeros_like(key_acc)
        value_acc[...] = jnp.zeros_like(value_acc)

        @pl.loop(0, count)
        def _(q_index):
            @pl.when(block_meets(bounds_ref, order_ref, q_index, k_index))
            def _():
                rows = pl.ds(pl.multiple_of(q_index * block, block), block)
                query, key_rows = query_ref[rows, :], key_ref[keys, :]
                grad_rows = grad_ref[rows, :]
                scores = contract_last(query, key_rows) * score_scale
                allowed = pair_mask(order_ref, seg_col_ref, seg_row_ref, q_index, k_index, block)
                probs = jnp.where(allowed, jnp.exp(scores - lse_ref[rows, :]), 0.0)
                prob_grad = contract_last(grad_rows, value_ref[keys, :])
                score_grad = (probs * (prob_grad - delta_ref[rows, :])).astype(jnp.bfloat16)
                value_acc[...] += contract_first(probs.astype(jnp.bfloat16), grad_rows)
                key_acc[...] += contract_first(score_grad, query)
                query_acc[rows, :] += jnp.dot(
                    score_grad, key_rows, preferred_element_type=jnp.float32
                )

        tables = (cos_ref[keys, :], low_ref[keys, :], high_ref[keys, :])
        key_low = turn(key_acc[:, :LANES] * score_scale, *tables, -1.0)
        key_high = key_acc[:, LANES:] * score_scale
        first = k_index == 0
        for start, part in ((HD, key_low), (HD + LANES, key_high), (2 * HD, value_acc[...])):
            columns = slice(start, start + part.shape[1])
            out_ref[keys, columns] = part.astype(jnp.bfloat16)
            sums_ref[:, columns] = jnp.where(first, 0.0, sums_ref[:, columns]) + jnp.sum(
                part, axis=0, keepdims=True
            )

    sums_ref[:, :HD] = jnp.zeros((1, HD), jnp.float32)

    @pl.loop(0, count)
    def _(q_index):
        rows = pl.ds(pl.multiple_of(q_index * block, block), block)
        tables = (cos_ref[rows, :], low_ref[rows, :], high_ref[rows, :])
        query_low = turn(query_acc[rows, :LANES] * score_scale, *tables, -1.0)
        query_high = query_acc[rows, LANES:] * score_scale
        for start, part in ((0, query_low), (LANES, query_high)):
            columns = slice(start, start + part.shape[1])
            out_ref[rows, columns] = part.astype(jnp.bfloat16)
            sums_ref[:, columns] += jnp.sum(part, axis=0, keepdims=True)


MESH = pl.DeviceIdType.MESH


def opening_kernel(*refs, side, second, ranks, square, sizes):
    count = len(sizes)
    gathered_in, refs = refs[:count], refs[count:]
    rows_in, refs = refs[:2], refs[2:]
    later_in, refs = refs[:2], refs[2:]
    gathered_out, refs = refs[:count], refs[count:]
    rows_out, refs = refs[:2], refs[2:]
    later_out, refs = refs[0], refs[1:]
    held, refs = refs[:count], refs[count:]
    held_rows, refs = refs[:2], refs[2:]
    held_later, refs = refs[:2], refs[2:]
    load_sem, store_sem, send_sem, recv_sem, row_send, row_recv = refs

    shard, rank = lax.axis_index("shard"), lax.axis_index("ctx")
    slow, fast = shard // second, shard % second
    flip = rank % 2 if square else 1
    here_first = fast * (1 - flip) + slow * flip
    here_second = slow * (1 - flip) + fast * flip

    def peer(first_step, second_step):
        first = (here_first + first_step + side) % side
        other = (here_second + second_step + second) % second
        return (other * side + first) * (1 - flip) + (first * second + other) * flip

    first_peers = [peer(a, 0) for a in range(1, side)]
    second_peers = [peer(0, b) for b in range(1, second)]
    rank_peers = [(rank + j) % ranks for j in range(1, ranks)]
    barrier = pltpu.get_barrier_semaphore()
    for target in first_peers + second_peers:
        pl.semaphore_signal(barrier, inc=1, device_id={"shard": target}, device_id_type=MESH)
    for target in rank_peers:
        pl.semaphore_signal(barrier, inc=1, device_id={"ctx": target}, device_id_type=MESH)

    loads = []
    for number in range(count):
        source = gathered_in[number]
        if sizes[number] is not None:
            columns = pl.ds(pl.multiple_of(rank * sizes[number], LANES), sizes[number])
            source = source.at[:, columns]
        loads.append(pltpu.make_async_copy(source, held[number], load_sem.at[number]))
    for number in range(2):
        loads.append(
            pltpu.make_async_copy(rows_in[number], held_rows[number], load_sem.at[count + number])
        )
    for number in range(2):
        size = held_later[number].shape[1]
        columns = pl.ds(pl.multiple_of(rank * size, LANES), size)
        loads.append(
            pltpu.make_async_copy(
                later_in[number].at[:, columns], held_later[number], load_sem.at[count + 2 + number]
            )
        )
    for load in loads:
        load.start()
    pl.semaphore_wait(barrier, len(first_peers) + len(second_peers) + len(rank_peers))

    def place(number, first_step, second_step):
        rows = held[number].shape[0]
        start = pl.multiple_of(peer(first_step, second_step) * rows, 16)
        return gathered_out[number].at[pl.ds(start, rows), :]

    copies, slot = {}, 0
    steps = side - 1 + (second - 1) * side

    def send(number, source, a, b, target, key):
        slot = number * steps + key
        copy = pltpu.make_async_remote_copy(
            src_ref=source,
            dst_ref=place(number, a, b),
            send_sem=send_sem.at[slot],
            recv_sem=recv_sem.at[slot],
            device_id={"shard": target},
            device_id_type=MESH,
        )
        copy.start()
        copies[number, key] = copy

    for number in range(count):
        loads[number].wait()
        for a in range(1, side):
            send(number, held[number], 0, 0, first_peers[a - 1], a - 1)
        for b in range(1, second):
            send(number, held[number], 0, 0, second_peers[b - 1], side - 1 + (b - 1) * side)
    row_copies = []
    for number in range(2):
        loads[count + number].wait()
        rows = held_rows[number].shape[0]
        for j in range(1, ranks):
            slot = number * (ranks - 1) + j - 1
            copy = pltpu.make_async_remote_copy(
                src_ref=held_rows[number],
                dst_ref=rows_out[number].at[pl.ds((ranks - j) * rows, rows), :],
                send_sem=row_send.at[slot],
                recv_sem=row_recv.at[slot],
                device_id={"ctx": rank_peers[j - 1]},
                device_id_type=MESH,
            )
            copy.start()
            row_copies.append(copy)
    stores = []
    for number in range(count):
        stores.append(
            pltpu.make_async_copy(held[number], place(number, 0, 0), store_sem.at[number])
        )
    for number in range(2):
        rows = held_rows[number].shape[0]
        stores.append(
            pltpu.make_async_copy(
                held_rows[number],
                rows_out[number].at[pl.ds(0, rows), :],
                store_sem.at[count + number],
            )
        )
    for number in range(2):
        loads[count + 2 + number].wait()
        size = held_later[number].shape[1]
        stores.append(
            pltpu.make_async_copy(
                held_later[number],
                later_out.at[:, pl.ds(number * size, size)],
                store_sem.at[count + 2 + number],
            )
        )
    for store in stores:
        store.start()
    for number in range(count):
        for a in range(1, side):
            copies[number, a - 1].wait_recv()
            for b in range(1, second):
                key = side - 1 + (b - 1) * side + a
                send(number, place(number, -a, 0), -a, 0, second_peers[b - 1], key)
    for store in stores:
        store.wait()
    for (number, key), copy in copies.items():
        copy.wait_send()
        if key >= side - 1:
            copy.wait_recv()
    for copy in row_copies:
        copy.wait_send()
        copy.wait_recv()


def opening(gathered, split, rows, later, ranks):
    shards = lax.axis_size("shard")
    side = math.isqrt(shards)
    square = side * side == shards
    if not square:
        side = 1
    second = shards // side
    sizes = [v.shape[1] // ranks if cut else None for v, cut in zip(gathered, split)]
    held = [(v.shape[0], size or v.shape[1]) for v, size in zip(gathered, sizes)]
    held_later = [(v.shape[0], v.shape[1] // ranks) for v in later]
    count, steps = len(gathered), side - 1 + (second - 1) * side
    bf16 = jnp.bfloat16
    out_shapes = (
        [jax.ShapeDtypeStruct((h[0] * shards, h[1]), bf16) for h in held]
        + [jax.ShapeDtypeStruct((v.shape[0] * ranks, v.shape[1]), bf16) for v in rows]
        + [jax.ShapeDtypeStruct((held_later[0][0], 2 * held_later[0][1]), bf16)]
    )
    hbm = pl.BlockSpec(memory_space=pl.ANY)
    total = count + 4
    row_slots = max(1, 2 * (ranks - 1))
    outs = pl.pallas_call(
        functools.partial(
            opening_kernel, side=side, second=second, ranks=ranks, square=square, sizes=sizes
        ),
        out_shape=tuple(out_shapes),
        in_specs=[hbm] * total,
        out_specs=(hbm,) * (total - 1),
        scratch_shapes=[pltpu.VMEM(h, bf16) for h in held]
        + [pltpu.VMEM(v.shape, bf16) for v in rows]
        + [pltpu.VMEM(h, bf16) for h in held_later]
        + [
            pltpu.SemaphoreType.DMA((total,)),
            pltpu.SemaphoreType.DMA((total,)),
            pltpu.SemaphoreType.DMA((count * steps,)),
            pltpu.SemaphoreType.DMA((count * steps,)),
            pltpu.SemaphoreType.DMA((row_slots,)),
            pltpu.SemaphoreType.DMA((row_slots,)),
        ],
        compiler_params=pltpu.CompilerParams(
            collective_id=0, has_side_effects=True, vmem_limit_bytes=VMEM_LIMIT
        ),
        name="opening",
    )(*gathered, *rows, *later)
    return outs[:count], outs[count : count + 2], outs[count + 2]


def pair_product_kernel(left_ref, right_ref, left_weight, right_weight, *refs):
    out_ref = refs[-1]
    out_ref[...] = (
        contract_last(left_ref[...], left_weight[...])
        + contract_last(right_ref[...], right_weight[...])
    ).astype(out_ref.dtype)


def block_sum_kernel(index_ref, whole_ref, *refs, count):
    del index_ref
    total = whole_ref[...].astype(jnp.float32)
    for ref in refs[:count]:
        total = total + ref[...].astype(jnp.float32)
    refs[-1][...] = total.astype(refs[-1].dtype)


def block_sum(whole, index, received, after, dtype):
    rows, columns = received[0].shape
    step = min(rows, 256)
    tiles = rows // step
    tile = pl.BlockSpec((step, columns), lambda i, index: (i, 0))
    return pl.pallas_call(
        functools.partial(block_sum_kernel, count=len(received)),
        grid_spec=pltpu.PrefetchScalarGridSpec(
            num_scalar_prefetch=1,
            grid=(tiles,),
            in_specs=[pl.BlockSpec((step, columns), lambda i, index: (index[0] * tiles + i, 0))]
            + [tile] * len(received)
            + [pl.BlockSpec(memory_space=pl.ANY)] * len(after),
            out_specs=tile,
        ),
        out_shape=jax.ShapeDtypeStruct((rows, columns), dtype),
        cost_estimate=pl.CostEstimate(
            flops=rows * columns, bytes_accessed=6 * rows * columns, transcendentals=0
        ),
        name="block_sum",
    )(jnp.asarray(index, jnp.int32).reshape(1), whole, *received, *after)


def place_columns_kernel(rank_ref, *refs):
    del rank_ref
    for number, ref in enumerate(refs[:-1]):

        @pl.when(pl.program_id(1) == number)
        def _():
            refs[-1][...] = ref[...].astype(refs[-1].dtype)


def place_columns(parts, rank):
    count = len(parts)
    rows, columns = parts[0].shape
    step = min(rows, 256)
    tile = pl.BlockSpec((step, columns), lambda i, k, rank: (i, 0))
    return pl.pallas_call(
        place_columns_kernel,
        grid_spec=pltpu.PrefetchScalarGridSpec(
            num_scalar_prefetch=1,
            grid=(rows // step, count),
            in_specs=[tile] * count,
            out_specs=pl.BlockSpec(
                (step, columns), lambda i, k, rank: (i, lax.rem(rank[0] + k, count))
            ),
        ),
        out_shape=jax.ShapeDtypeStruct((rows, columns * count), jnp.float32),
        cost_estimate=pl.CostEstimate(
            flops=0, bytes_accessed=6 * rows * columns * count, transcendentals=0
        ),
        name="place_columns",
    )(jnp.asarray(rank, jnp.int32).reshape(1), *parts)


def norm_grad_kernel(
    left_ref,
    right_ref,
    x_ref,
    left_weight,
    right_weight,
    left_gain,
    right_gain,
    after_ref,
    out_ref,
    sums_ref,
):
    del after_ref
    x = x_ref[...].astype(jnp.float32)
    centered = x - jnp.mean(x, axis=-1, keepdims=True)
    inverse = lax.rsqrt(jnp.mean(centered * centered, axis=-1, keepdims=True) + EPSILON)
    hat = centered * inverse
    left = contract_last(left_ref[...], left_weight[...])
    right = contract_last(right_ref[...], right_weight[...])
    scaled = left * left_gain[...] + right * right_gain[...]
    first = pl.program_id(0) == 0
    for row, part in enumerate((left * hat, left, right * hat, right)):
        total = jnp.sum(part, axis=0, keepdims=True)
        sums_ref[row : row + 1, :] = jnp.where(first, 0.0, sums_ref[row : row + 1, :]) + total
    inner = (
        scaled
        - jnp.mean(scaled, axis=-1, keepdims=True)
        - hat * jnp.mean(scaled * hat, axis=-1, keepdims=True)
    )
    out_ref[...] = (inverse * inner).astype(out_ref.dtype)


ROWS_STEP = 256


def row_specs(arrays, start, rows):
    step = min(ROWS_STEP, rows)
    return step, [
        pl.BlockSpec((step, v.shape[1]), lambda i, first=start // step: (first + i, 0))
        for v in arrays
    ]


def whole_spec(array):
    return pl.BlockSpec(array.shape, lambda i: (0, 0))


def half_spec(array, half):
    return pl.BlockSpec((array.shape[0], array.shape[1] // 2), lambda i: (0, half))


def pair_product(left, right, left_weight, right_weight, after, start, rows):
    step, specs = row_specs((left, right), start, rows)
    width = left_weight.shape[0]
    return pl.pallas_call(
        pair_product_kernel,
        grid=(rows // step,),
        out_shape=jax.ShapeDtypeStruct((rows, width), jnp.bfloat16),
        in_specs=specs
        + [whole_spec(left_weight), half_spec(right_weight, 1)]
        + [pl.BlockSpec(memory_space=pl.ANY)] * len(after),
        out_specs=pl.BlockSpec((step, width), lambda i: (i, 0)),
        compiler_params=pltpu.CompilerParams(vmem_limit_bytes=VMEM_LIMIT),
        cost_estimate=pl.CostEstimate(
            flops=2 * rows * width * (left.shape[1] + right.shape[1]),
            bytes_accessed=2 * rows * (width + left.shape[1] + right.shape[1]),
            transcendentals=0,
        ),
        name="pair_product",
    )(left, right, left_weight, right_weight, *after)


def norm_grad(
    left, right, x, left_weight, right_weight, left_gain, right_gain, after, start, rows
):
    step, specs = row_specs((left, right, x), start, rows)
    width = left_weight.shape[0]
    rest = [left_weight, right_weight, left_gain, right_gain]
    return pl.pallas_call(
        norm_grad_kernel,
        grid=(rows // step,),
        out_shape=(
            jax.ShapeDtypeStruct((rows, width), jnp.bfloat16),
            jax.ShapeDtypeStruct((4, width), jnp.float32),
        ),
        in_specs=specs
        + [whole_spec(left_weight), half_spec(right_weight, 0)]
        + [whole_spec(v) for v in rest[2:]]
        + [pl.BlockSpec(memory_space=pl.ANY)],
        out_specs=(
            pl.BlockSpec((step, width), lambda i: (i, 0)),
            pl.BlockSpec((4, width), lambda i: (0, 0)),
        ),
        compiler_params=pltpu.CompilerParams(vmem_limit_bytes=VMEM_LIMIT),
        cost_estimate=pl.CostEstimate(
            flops=2 * rows * width * (left.shape[1] + right.shape[1]),
            bytes_accessed=2 * rows * (2 * width + left.shape[1] + right.shape[1]),
            transcendentals=0,
        ),
        name="norm_grad",
    )(left, right, x, *rest, after)


SCALAR = pl.BlockSpec(memory_space=pltpu.SMEM)
VECTOR = pl.BlockSpec(memory_space=pltpu.VMEM)


def attend(order, bounds, proj, tables, seg_col, seg_row, block, count):
    length = proj.shape[0]
    pairs = length * length
    return pl.pallas_call(
        functools.partial(attend_kernel, block=block, count=count),
        out_shape=(
            jax.ShapeDtypeStruct((length, HD), jnp.bfloat16),
            jax.ShapeDtypeStruct((length, HD), jnp.bfloat16),
            jax.ShapeDtypeStruct((length, HD), jnp.bfloat16),
            jax.ShapeDtypeStruct((length, HD), jnp.bfloat16),
            jax.ShapeDtypeStruct((length, 1), jnp.float32),
        ),
        in_specs=[SCALAR] * 2 + [VECTOR] * 6,
        out_specs=(VECTOR,) * 5,
        scratch_shapes=[
            pltpu.VMEM((block, 1), jnp.float32),
            pltpu.VMEM((block, 1), jnp.float32),
            pltpu.VMEM((block, HD), jnp.float32),
        ],
        compiler_params=pltpu.CompilerParams(vmem_limit_bytes=VMEM_LIMIT),
        cost_estimate=pl.CostEstimate(
            flops=2 * pairs * HD, bytes_accessed=16 * length * HD, transcendentals=pairs // 2
        ),
        name="attend",
    )(order, bounds, proj, *tables, seg_col, seg_row)


def attend_grad(
    order, bounds, query, key, value, attn, grad, lse, tables, seg_col, seg_row, block, count
):
    length = query.shape[0]
    pairs = length * length
    return pl.pallas_call(
        functools.partial(attend_grad_kernel, block=block, count=count),
        out_shape=(
            jax.ShapeDtypeStruct((length, 3 * HD), jnp.bfloat16),
            jax.ShapeDtypeStruct((1, 3 * HD), jnp.float32),
        ),
        in_specs=[SCALAR] * 2 + [VECTOR] * 11,
        out_specs=(VECTOR,) * 2,
        scratch_shapes=[
            pltpu.VMEM((length, HD), jnp.float32),
            pltpu.VMEM((block, HD), jnp.float32),
            pltpu.VMEM((block, HD), jnp.float32),
            pltpu.VMEM((length, 1), jnp.float32),
        ],
        compiler_params=pltpu.CompilerParams(vmem_limit_bytes=VMEM_LIMIT),
        cost_estimate=pl.CostEstimate(
            flops=5 * pairs * HD, bytes_accessed=16 * length * HD, transcendentals=pairs // 2
        ),
        name="attend_grad",
    )(order, bounds, query, key, value, attn, grad, lse, *tables, seg_col, seg_row)


def ring_shift(value, axis, step):
    count = lax.axis_size(axis)
    return lax.ppermute(value, axis, [(i, (i + step) % count) for i in range(count)])


class Plane:
    def __init__(self):
        self.count = lax.axis_size("shard")
        side = math.isqrt(self.count)
        self.square = side * side == self.count
        self.first, self.second = (side, side) if self.square else (1, self.count)
        self.ranks = lax.axis_size("ctx")
        shard = lax.axis_index("shard")
        self.flip = (lax.axis_index("ctx") % 2 == 1) if self.square else False
        slow, fast = shard // self.second, shard % self.second
        if self.square:
            self.here = (jnp.where(self.flip, slow, fast), jnp.where(self.flip, fast, slow))
        else:
            self.here = (slow, fast)

    def index(self, first_step, second_step):
        first = lax.rem(self.here[0] + first_step + self.first, self.first)
        second = lax.rem(self.here[1] + second_step + self.second, self.second)
        if not self.square:
            return first * self.second + second
        side = self.first
        return jnp.where(self.flip, first * side + second, second * side + first)

    def move(self, value, first_step, second_step):
        pairs = []
        for shard in range(self.count):
            for rank in range(self.ranks):
                slow, fast = divmod(shard, self.second)
                if self.square and rank % 2 == 0:
                    slow = (slow + second_step) % self.second
                    fast = (fast + first_step) % self.first
                else:
                    slow = (slow + first_step) % self.first
                    fast = (fast + second_step) % self.second
                target = slow * self.second + fast
                pairs.append((shard * self.ranks + rank, target * self.ranks + rank))
        return lax.ppermute(value, ("shard", "ctx"), pairs)

    def scatter_sum(self, partial, after, last=()):
        rows = partial.shape[0] // self.count
        sums, final = {}, []
        for b in list(range(1, self.second)) + [0]:
            received = []
            for a in range(1, self.first):
                block = lax.dynamic_slice_in_dim(partial, self.index(a, b) * rows, rows)
                received.append(self.move(block, a, 0))
            if b == 0:
                final = received
            elif received:
                sums[b] = block_sum(partial, self.index(0, b), received, after, partial.dtype)
            else:
                sums[b] = lax.dynamic_slice_in_dim(partial, self.index(0, b) * rows, rows)
        final = final + [self.move(sums[b], 0, b) for b in range(1, self.second)]
        return block_sum(partial, self.index(0, 0), final, [*after, *last], partial.dtype)

    def full_sum(self, value):
        total = value
        for a in range(1, self.first):
            total = total + self.move(value, a, 0)
        value = total
        for b in range(1, self.second):
            total = total + self.move(value, 0, b)
        return total


def local(
    hidden_in,
    grad_out,
    segment_ids,
    group_order,
    ln1_gain,
    ln1_bias,
    qkv_weight,
    qkv_bias,
    dense_weight,
    dense_bias,
    ln2_gain,
    ln2_bias,
    up_weight,
    up_bias,
    down_weight,
    down_bias,
):
    _, groups_dev, block_len, width = hidden_in.shape
    tokens = groups_dev * block_len
    seq_len = segment_ids.shape[1]
    groups = seq_len // block_len
    ctx_count, tp_count = lax.axis_size("ctx"), lax.axis_size("tp")
    shard_count = lax.axis_size("shard")
    ctx_rank, tp_rank = lax.axis_index("ctx"), lax.axis_index("tp")
    shard_rank = lax.axis_index("shard")
    slice_width = width // tp_count
    bf16, f32 = jnp.bfloat16, jnp.float32

    def my_columns(matrix):
        columns = matrix.shape[1] // ctx_count
        return lax.dynamic_slice_in_dim(matrix, ctx_rank * columns, columns, 1)

    plane = Plane()

    x_mine = hidden_in.reshape(tokens, width)
    g_mine = grad_out.reshape(tokens, width)
    vectors = [
        ln1_gain, ln1_bias, ln2_gain, ln2_bias, dense_bias, down_bias, qkv_bias[0], up_bias[0],
    ]
    sizes = [v.shape[0] for v in vectors]
    wide = -(-max(sizes) // LANES) * LANES
    packed = jnp.stack([jnp.pad(v, (0, wide - v.shape[0])) for v in vectors])
    packed = jnp.concatenate([packed, jnp.zeros_like(packed)], axis=0)
    (w_vectors, w_qkv, w_dense), (x_row, g_row), wide_mine = opening(
        [packed, qkv_weight, dense_weight],
        [False, True, True],
        [x_mine, g_mine],
        [up_weight, down_weight],
        ctx_count,
    )
    w_wide = lax.all_gather(wide_mine, "shard", axis=0, tiled=True)
    units = w_wide.shape[1] // 2
    w_up, w_down = w_wide[:, :units], w_wide[:, units:]
    w_vectors = w_vectors.reshape(shard_count, packed.shape[0], wide)
    spread = [
        w_vectors[:, number, :size].reshape(-1).astype(f32) for number, size in enumerate(sizes)
    ]
    gain_one, shift_one, gain_two, shift_two, bias_dense, bias_down, bias_qkv, bias_up = spread
    bias_qkv = my_columns(bias_qkv[None])
    bias_up = my_columns(bias_up[None])
    plane = Plane()
    heads_here = w_qkv.shape[1] // (3 * HD)

    own_order = jnp.concatenate(
        [
            lax.dynamic_slice_in_dim(
                group_order, lax.rem(ctx_rank + k, ctx_count) * groups_dev, groups_dev
            )
            for k in range(ctx_count)
        ]
    )
    segments = segment_ids[0]
    positions = segment_positions(segments)

    def stored(values):
        return jnp.concatenate(
            [
                lax.dynamic_slice_in_dim(values, own_order[k] * block_len, block_len)
                for k in range(groups)
            ]
        )

    seg_stored = stored(segments)
    tables = rotary_tables(stored(positions))
    seg_blocks = seg_stored.reshape(groups, block_len)
    bounds = jnp.stack([seg_blocks[:, 0], seg_blocks[:, -1]])
    seg_col, seg_row = seg_stored[:, None], seg_stored[None, :]

    x_float = x_row.astype(f32)
    centered = x_float - jnp.mean(x_float, axis=-1, keepdims=True)
    inverse = lax.rsqrt(jnp.mean(centered * centered, axis=-1, keepdims=True) + EPSILON)
    hat = centered * inverse
    acts_one = (hat * gain_one + shift_one).astype(bf16)
    acts_two = (hat * gain_two + shift_two).astype(bf16)

    projected = jnp.dot(acts_one, w_qkv, preferred_element_type=f32) + bias_qkv
    heads = []
    for h in range(heads_here):
        heads.append(
            attend(
                own_order,
                bounds,
                projected[:, 3 * HD * h : 3 * HD * (h + 1)],
                tables,
                seg_col,
                seg_row,
                block_len,
                groups,
            )
        )
    attn = jnp.concatenate([head[3] for head in heads], axis=1)

    attn_grad = jnp.dot(g_row, w_dense, preferred_element_type=f32).astype(bf16)
    proj_parts, sum_parts = [], []
    for h, (query, key, value, attn_head, lse) in enumerate(heads):
        part, sums = attend_grad(
            own_order,
            bounds,
            query,
            key,
            value,
            attn_head,
            attn_grad[:, HD * h : HD * (h + 1)],
            lse,
            tables,
            seg_col,
            seg_row,
            block_len,
            groups,
        )
        proj_parts.append(part)
        sum_parts.append(sums[0])
    proj_grad_b = jnp.concatenate(proj_parts, axis=1)
    qkv_bias_grad = jnp.concatenate(sum_parts)

    pre_act = jnp.dot(acts_two, w_up, preferred_element_type=f32) + bias_up
    cdf = 0.5 * (1.0 + lax.erf(pre_act * (1.0 / math.sqrt(2.0))))
    hidden = (pre_act * cdf).astype(bf16)
    slope = cdf + pre_act * jnp.exp(-0.5 * pre_act * pre_act) * (1.0 / math.sqrt(2.0 * math.pi))

    def reduce_partial(parts):
        received = [ring_shift(parts[k], "ctx", k) for k in range(1, ctx_count)]
        total = block_sum(parts[0], 0, received, [], bf16)
        return total, lax.psum_scatter(total, "tp", scatter_dimension=1, tiled=True).astype(f32)

    dense_local = contract_first(g_row, attn).astype(bf16)
    out_parts = {}
    for k in reversed(range(ctx_count)):
        out_parts[k] = pair_product(
            attn,
            hidden,
            w_dense,
            w_wide,
            [proj_grad_b, dense_local] if k + 1 == ctx_count else [out_parts[k + 1]],
            k * tokens,
            tokens,
        )
    out_total, summed_out = reduce_partial(out_parts)
    out_shift = lax.dynamic_slice_in_dim(bias_dense + bias_down, tp_rank * slice_width, slice_width)
    x_slice = lax.dynamic_slice_in_dim(x_mine, tp_rank * slice_width, slice_width, 1)
    output = x_slice.astype(f32) + summed_out + out_shift

    def reduce_weight(grad, after, last=()):
        mine = plane.scatter_sum(grad, after, last)
        parts = [mine] + [ring_shift(mine, "ctx", ctx_count - k) for k in range(1, ctx_count)]
        return place_columns(parts, ctx_rank)

    bias_grad = jnp.sum(g_row.astype(f32), axis=0)

    pre_grad = jnp.dot(g_row, w_down, preferred_element_type=f32) * slope
    up_bias_grad = jnp.sum(pre_grad, axis=0)
    pre_grad_b = pre_grad.astype(bf16)

    in_parts, norm_sums = {}, jnp.zeros((4, width), f32)
    for k in reversed(range(ctx_count)):
        in_parts[k], sums = norm_grad(
            proj_grad_b,
            pre_grad_b,
            x_row,
            w_qkv,
            w_wide,
            gain_one[None],
            gain_two[None],
            in_parts[k + 1] if k + 1 in in_parts else out_total,
            k * tokens,
            tokens,
        )
        norm_sums = norm_sums + sums
    in_total, input_sum = reduce_partial(in_parts)
    g_slice = lax.dynamic_slice_in_dim(g_mine, tp_rank * slice_width, slice_width, 1)
    input_grad = g_slice.astype(f32) + input_sum

    down_local = contract_first(g_row, hidden).astype(bf16)
    qkv_local = contract_first(acts_one, proj_grad_b).astype(bf16)
    up_local = contract_first(acts_two, pre_grad_b).astype(bf16)
    late = [qkv_local, up_local]
    down_grad = reduce_weight(down_local, [in_total])
    dense_grad = reduce_weight(dense_local, [out_total])

    norm_sums = norm_sums.reshape(-1)
    column_sums = [up_bias_grad, qkv_bias_grad]
    packed = jnp.concatenate([norm_sums] + column_sums)
    wholes = [jnp.zeros((v.shape[0] * ctx_count,), f32) for v in column_sums]
    total = jnp.zeros_like(norm_sums)
    for k in range(ctx_count):
        part = packed if k == 0 else ring_shift(packed, "ctx", ctx_count - k)
        total = total + part[: norm_sums.shape[0]]
        offset = norm_sums.shape[0]
        for number, vector in enumerate(column_sums):
            size = vector.shape[0]
            wholes[number] = lax.dynamic_update_slice_in_dim(
                wholes[number],
                part[offset : offset + size],
                lax.rem(ctx_rank + k, ctx_count) * size,
                0,
            )
            offset += size
    norm_sums = total
    for k in range(1, tp_count):
        norm_sums = norm_sums + ring_shift(total, "tp", k)
    pieces = [bias_grad] + wholes + [
        norm_sums[k * width : (k + 1) * width] for k in range(4)
    ]
    reduced = plane.full_sum(jnp.concatenate(pieces))
    qkv_grad = reduce_weight(qkv_local, late, [reduced])
    up_grad = reduce_weight(up_local, late, [reduced])
    results, offset = [], 0
    for piece in pieces:
        own = piece.shape[0] // shard_count
        results.append(lax.dynamic_slice_in_dim(reduced, offset + shard_rank * own, own))
        offset += piece.shape[0]
    bias_grad, up_bias_grad, qkv_bias_grad = results[:3]
    gain_one_grad, shift_one_grad, gain_two_grad, shift_two_grad = results[3:]
    out_shape = hidden_in.shape[:3] + (slice_width,)
    return (
        output.reshape(out_shape),
        input_grad.reshape(out_shape),
        gain_one_grad,
        shift_one_grad,
        qkv_grad,
        qkv_bias_grad[None],
        dense_grad,
        bias_grad,
        gain_two_grad,
        shift_two_grad,
        up_grad,
        up_bias_grad[None],
        down_grad,
    )


def solution(mesh):
    return jax.shard_map(
        local,
        mesh=mesh,
        in_specs=(
            P("shard", "ctx", None, None),
            P("shard", "ctx", None, None),
            P("shard", None),
            P(),
            P("shard"),
            P("shard"),
            P("shard", "tp"),
            P("tp", "shard"),
            P("shard", "tp"),
            P("shard"),
            P("shard"),
            P("shard"),
            P("shard", "tp"),
            P("tp", "shard"),
            P("shard", "tp"),
            P("shard"),
        ),
        out_specs=(
            P("shard", "ctx", None, "tp"),
            P("shard", "ctx", None, "tp"),
            P("shard"),
            P("shard"),
            P("shard", "tp"),
            P("tp", "shard"),
            P("shard", "tp"),
            P("shard"),
            P("shard"),
            P("shard"),
            P("shard", "tp"),
            P("tp", "shard"),
            P("shard", "tp"),
        ),
        check_vma=False,
    )
```

```python
import functools
import math

import jax
import jax.numpy as jnp
from jax import lax
from jax.experimental import pallas as pl
from jax.experimental.pallas import tpu as pltpu
from jax.sharding import PartitionSpec as P


HD = 256
ROT = 64
LANES = 128

EPSILON = 1e-05
ROTARY_BASE = 10000.0
NEG = -1e30
VMEM_LIMIT = 56 * 1024 * 1024


def segment_positions(segments):
    length_all = segments.shape[0]
    index_row = jnp.arange(length_all, dtype=jnp.int32)
    changed = jnp.concatenate(
        [jnp.ones((1,), dtype=jnp.bool_), segments[1:] != segments[:-1]]
    )
    seg_start = jnp.where(changed, index_row, jnp.zeros_like(segments))
    return index_row - lax.cummax(seg_start, axis=0)


def rotary_tables(positions):
    half_rot = ROT // 2
    frequency = ROTARY_BASE ** (-2.0 * jnp.arange(half_rot, dtype=jnp.float32) / ROT)
    angles = positions.astype(jnp.float32)[:, None] * frequency[None, :]
    cosine, sine = jnp.cos(angles), jnp.sin(angles)
    count = positions.shape[0]
    rest_one = jnp.ones((count, LANES - ROT), jnp.float32)
    rest_zero = jnp.zeros((count, LANES - half_rot), jnp.float32)
    cosine_table = jnp.concatenate([cosine, cosine, rest_one], axis=1)
    low_table = jnp.concatenate([-sine, rest_zero], axis=1)
    high_table = jnp.concatenate(
        [jnp.zeros_like(sine), sine, rest_zero[:, : LANES - ROT]], axis=1
    )
    return cosine_table, low_table, high_table


def turn(values, cosine, low, high, sign):
    half_rot = ROT // 2
    down = pltpu.roll(values, LANES - half_rot, 1)
    up = pltpu.roll(values, half_rot, 1)
    return values * cosine + sign * (down * low + up * high)


def contract_first(left_mat, right_mat):
    return lax.dot_general(
        left_mat, right_mat, (((0,), (0,)), ((), ())), preferred_element_type=jnp.float32
    )


def contract_last(left_mat, right_mat):
    return lax.dot_general(
        left_mat, right_mat, (((1,), (1,)), ((), ())), preferred_element_type=jnp.float32
    )


def block_meets(bounds_ref, order_ref, q_index, k_index):
    return (
        (order_ref[k_index] <= order_ref[q_index])
        & (bounds_ref[0, k_index] <= bounds_ref[1, q_index])
        & (bounds_ref[1, k_index] >= bounds_ref[0, q_index])
    )


def pair_mask(order_ref, seg_col_ref, seg_row_ref, q_index, k_index, block):
    q_place = order_ref[q_index] * block + lax.broadcasted_iota(jnp.int32, (block, block), 0)
    k_place = order_ref[k_index] * block + lax.broadcasted_iota(jnp.int32, (block, block), 1)
    seg_q = seg_col_ref[pl.ds(q_index * block, block), :]
    seg_k = seg_row_ref[:, pl.ds(pl.multiple_of(k_index * block, block), block)]
    return (k_place <= q_place) & (seg_q == seg_k)


def attend_kernel(
    order_ref,
    bounds_ref,
    proj_ref,
    cos_ref,
    low_ref,
    high_ref,
    seg_col_ref,
    seg_row_ref,
    query_ref,
    key_ref,
    value_ref,
    attn_ref,
    lse_ref,
    top_ref,
    sum_ref,
    acc_ref,
    *,
    block,
    count,
):
    score_scale = 1.0 / math.sqrt(HD)
    for index in range(count):
        rows = pl.ds(index * block, block)
        tables = (cos_ref[rows, :], low_ref[rows, :], high_ref[rows, :])
        for start, out in ((0, query_ref), (HD, key_ref)):
            out[rows, :LANES] = turn(
                proj_ref[rows, start : start + LANES], *tables, 1.0
            ).astype(jnp.bfloat16)
            out[rows, LANES:] = proj_ref[rows, start + LANES : start + HD].astype(jnp.bfloat16)
        value_ref[rows, :] = proj_ref[rows, 2 * HD :].astype(jnp.bfloat16)

    @pl.loop(0, count)
    def _(q_index):
        rows = pl.ds(pl.multiple_of(q_index * block, block), block)
        top_ref[...] = jnp.full_like(top_ref, NEG)
        sum_ref[...] = jnp.zeros_like(sum_ref)
        acc_ref[...] = jnp.zeros_like(acc_ref)

        @pl.loop(0, count)
        def _(k_index):
            @pl.when(block_meets(bounds_ref, order_ref, q_index, k_index))
            def _():
                keys = pl.ds(pl.multiple_of(k_index * block, block), block)
                scores = contract_last(query_ref[rows, :], key_ref[keys, :]) * score_scale
                allowed = pair_mask(order_ref, seg_col_ref, seg_row_ref, q_index, k_index, block)
                scores = jnp.where(allowed, scores, NEG)
                old_top = top_ref[...]
                new_top = jnp.maximum(old_top, jnp.max(scores, axis=1, keepdims=True))
                shrink = jnp.exp(old_top - new_top)
                weights = jnp.where(allowed, jnp.exp(scores - new_top), 0.0)
                top_ref[...] = new_top
                sum_ref[...] = sum_ref[...] * shrink + jnp.sum(weights, axis=1, keepdims=True)
                acc_ref[...] = acc_ref[...] * shrink + jnp.dot(
                    weights.astype(jnp.bfloat16),
                    value_ref[keys, :],
                    preferred_element_type=jnp.float32,
                )

        attn_ref[rows, :] = (acc_ref[...] / sum_ref[...]).astype(jnp.bfloat16)
        lse_ref[rows, :] = top_ref[...] + jnp.log(sum_ref[...])


def attend_grad_kernel(
    order_ref,
    bounds_ref,
    query_ref,
    key_ref,
    value_ref,
    attn_ref,
    grad_ref,
    lse_ref,
    cos_ref,
    low_ref,
    high_ref,
    seg_col_ref,
    seg_row_ref,
    out_ref,
    sums_ref,
    query_acc,
    key_acc,
    value_acc,
    delta_ref,
    *,
    block,
    count,
):
    score_scale = 1.0 / math.sqrt(HD)
    query_acc[...] = jnp.zeros_like(query_acc)
    delta_ref[...] = jnp.sum(
        grad_ref[...].astype(jnp.float32) * attn_ref[...].astype(jnp.float32),
        axis=1,
        keepdims=True,
    )

    @pl.loop(0, count)
    def _(k_index):
        keys = pl.ds(pl.multiple_of(k_index * block, block), block)
        key_acc[...] = jnp.zeros_like(key_acc)
        value_acc[...] = jnp.zeros_like(value_acc)

        @pl.loop(0, count)
        def _(q_index):
            @pl.when(block_meets(bounds_ref, order_ref, q_index, k_index))
            def _():
                rows = pl.ds(pl.multiple_of(q_index * block, block), block)
                query, key_rows = query_ref[rows, :], key_ref[keys, :]
                grad_rows = grad_ref[rows, :]
                scores = contract_last(query, key_rows) * score_scale
                allowed = pair_mask(order_ref, seg_col_ref, seg_row_ref, q_index, k_index, block)
                probs = jnp.where(allowed, jnp.exp(scores - lse_ref[rows, :]), 0.0)
                prob_grad = contract_last(grad_rows, value_ref[keys, :])
                score_grad = (probs * (prob_grad - delta_ref[rows, :])).astype(jnp.bfloat16)
                value_acc[...] += contract_first(probs.astype(jnp.bfloat16), grad_rows)
                key_acc[...] += contract_first(score_grad, query)
                query_acc[rows, :] += jnp.dot(
                    score_grad, key_rows, preferred_element_type=jnp.float32
                )

        tables = (cos_ref[keys, :], low_ref[keys, :], high_ref[keys, :])
        key_low = turn(key_acc[:, :LANES] * score_scale, *tables, -1.0)
        key_high = key_acc[:, LANES:] * score_scale
        first = k_index == 0
        for start, part in ((HD, key_low), (HD + LANES, key_high), (2 * HD, value_acc[...])):
            columns = slice(start, start + part.shape[1])
            out_ref[keys, columns] = part.astype(jnp.bfloat16)
            sums_ref[:, columns] = jnp.where(first, 0.0, sums_ref[:, columns]) + jnp.sum(
                part, axis=0, keepdims=True
            )

    sums_ref[:, :HD] = jnp.zeros((1, HD), jnp.float32)

    @pl.loop(0, count)
    def _(q_index):
        rows = pl.ds(pl.multiple_of(q_index * block, block), block)
        tables = (cos_ref[rows, :], low_ref[rows, :], high_ref[rows, :])
        query_low = turn(query_acc[rows, :LANES] * score_scale, *tables, -1.0)
        query_high = query_acc[rows, LANES:] * score_scale
        for start, part in ((0, query_low), (LANES, query_high)):
            columns = slice(start, start + part.shape[1])
            out_ref[rows, columns] = part.astype(jnp.bfloat16)
            sums_ref[:, columns] += jnp.sum(part, axis=0, keepdims=True)


MESH = pl.DeviceIdType.MESH


def opening_kernel(*refs, side, second, ranks, square, sizes):
    count = len(sizes)
    gathered_in, refs = refs[:count], refs[count:]
    rows_in, refs = refs[:2], refs[2:]
    later_in, refs = refs[:2], refs[2:]
    gathered_out, refs = refs[:count], refs[count:]
    rows_out, refs = refs[:2], refs[2:]
    later_out, refs = refs[0], refs[1:]
    held, refs = refs[:count], refs[count:]
    held_rows, refs = refs[:2], refs[2:]
    held_later, refs = refs[:2], refs[2:]
    load_sem, store_sem, send_sem, recv_sem, row_send, row_recv = refs

    shard, rank = lax.axis_index("shard"), lax.axis_index("ctx")
    slow, fast = shard // second, shard % second
    flip = rank % 2 if square else 1
    here_first = fast * (1 - flip) + slow * flip
    here_second = slow * (1 - flip) + fast * flip

    def peer(first_step, second_step):
        first = (here_first + first_step + side) % side
        other = (here_second + second_step + second) % second
        return (other * side + first) * (1 - flip) + (first * second + other) * flip

    first_peers = [peer(a, 0) for a in range(1, side)]
    second_peers = [peer(0, b) for b in range(1, second)]
    rank_peers = [(rank + j) % ranks for j in range(1, ranks)]
    barrier = pltpu.get_barrier_semaphore()
    for target in first_peers + second_peers:
        pl.semaphore_signal(barrier, inc=1, device_id={"shard": target}, device_id_type=MESH)
    for target in rank_peers:
        pl.semaphore_signal(barrier, inc=1, device_id={"ctx": target}, device_id_type=MESH)

    loads = []
    for number in range(count):
        source = gathered_in[number]
        if sizes[number] is not None:
            columns = pl.ds(pl.multiple_of(rank * sizes[number], LANES), sizes[number])
            source = source.at[:, columns]
        loads.append(pltpu.make_async_copy(source, held[number], load_sem.at[number]))
    for number in range(2):
        loads.append(
            pltpu.make_async_copy(rows_in[number], held_rows[number], load_sem.at[count + number])
        )
    for number in range(2):
        size = held_later[number].shape[1]
        columns = pl.ds(pl.multiple_of(rank * size, LANES), size)
        loads.append(
            pltpu.make_async_copy(
                later_in[number].at[:, columns], held_later[number], load_sem.at[count + 2 + number]
            )
        )
    for load in loads:
        load.start()
    pl.semaphore_wait(barrier, len(first_peers) + len(second_peers) + len(rank_peers))

    def place(number, first_step, second_step):
        rows = held[number].shape[0]
        start = pl.multiple_of(peer(first_step, second_step) * rows, 16)
        return gathered_out[number].at[pl.ds(start, rows), :]

    copies, slot = {}, 0
    steps = side - 1 + (second - 1) * side

    def send(number, source, a, b, target, key):
        slot = number * steps + key
        copy = pltpu.make_async_remote_copy(
            src_ref=source,
            dst_ref=place(number, a, b),
            send_sem=send_sem.at[slot],
            recv_sem=recv_sem.at[slot],
            device_id={"shard": target},
            device_id_type=MESH,
        )
        copy.start()
        copies[number, key] = copy

    for number in range(count):
        loads[number].wait()
        for a in range(1, side):
            send(number, held[number], 0, 0, first_peers[a - 1], a - 1)
        for b in range(1, second):
            send(number, held[number], 0, 0, second_peers[b - 1], side - 1 + (b - 1) * side)
    row_copies = []
    for number in range(2):
        loads[count + number].wait()
        rows = held_rows[number].shape[0]
        for j in range(1, ranks):
            slot = number * (ranks - 1) + j - 1
            copy = pltpu.make_async_remote_copy(
                src_ref=held_rows[number],
                dst_ref=rows_out[number].at[pl.ds((ranks - j) * rows, rows), :],
                send_sem=row_send.at[slot],
                recv_sem=row_recv.at[slot],
                device_id={"ctx": rank_peers[j - 1]},
                device_id_type=MESH,
            )
            copy.start()
            row_copies.append(copy)
    stores = []
    for number in range(count):
        stores.append(
            pltpu.make_async_copy(held[number], place(number, 0, 0), store_sem.at[number])
        )
    for number in range(2):
        rows = held_rows[number].shape[0]
        stores.append(
            pltpu.make_async_copy(
                held_rows[number],
                rows_out[number].at[pl.ds(0, rows), :],
                store_sem.at[count + number],
            )
        )
    for number in range(2):
        loads[count + 2 + number].wait()
        size = held_later[number].shape[1]
        stores.append(
            pltpu.make_async_copy(
                held_later[number],
                later_out.at[:, pl.ds(number * size, size)],
                store_sem.at[count + 2 + number],
            )
        )
    for store in stores:
        store.start()
    for number in range(count):
        for a in range(1, side):
            copies[number, a - 1].wait_recv()
            for b in range(1, second):
                key = side - 1 + (b - 1) * side + a
                send(number, place(number, -a, 0), -a, 0, second_peers[b - 1], key)
    for store in stores:
        store.wait()
    for (number, key), copy in copies.items():
        copy.wait_send()
        if key >= side - 1:
            copy.wait_recv()
    for copy in row_copies:
        copy.wait_send()
        copy.wait_recv()


def opening(gathered, split, rows, later, ranks):
    shards = lax.axis_size("shard")
    side = math.isqrt(shards)
    square = side * side == shards
    if not square:
        side = 1
    second = shards // side
    sizes = [v.shape[1] // ranks if cut else None for v, cut in zip(gathered, split)]
    held = [(v.shape[0], size or v.shape[1]) for v, size in zip(gathered, sizes)]
    held_later = [(v.shape[0], v.shape[1] // ranks) for v in later]
    count, steps = len(gathered), side - 1 + (second - 1) * side
    bf16 = jnp.bfloat16
    out_shapes = (
        [jax.ShapeDtypeStruct((h[0] * shards, h[1]), bf16) for h in held]
        + [jax.ShapeDtypeStruct((v.shape[0] * ranks, v.shape[1]), bf16) for v in rows]
        + [jax.ShapeDtypeStruct((held_later[0][0], 2 * held_later[0][1]), bf16)]
    )
    hbm = pl.BlockSpec(memory_space=pl.ANY)
    total = count + 4
    row_slots = max(1, 2 * (ranks - 1))
    outs = pl.pallas_call(
        functools.partial(
            opening_kernel, side=side, second=second, ranks=ranks, square=square, sizes=sizes
        ),
        out_shape=tuple(out_shapes),
        in_specs=[hbm] * total,
        out_specs=(hbm,) * (total - 1),
        scratch_shapes=[pltpu.VMEM(h, bf16) for h in held]
        + [pltpu.VMEM(v.shape, bf16) for v in rows]
        + [pltpu.VMEM(h, bf16) for h in held_later]
        + [
            pltpu.SemaphoreType.DMA((total,)),
            pltpu.SemaphoreType.DMA((total,)),
            pltpu.SemaphoreType.DMA((count * steps,)),
            pltpu.SemaphoreType.DMA((count * steps,)),
            pltpu.SemaphoreType.DMA((row_slots,)),
            pltpu.SemaphoreType.DMA((row_slots,)),
        ],
        compiler_params=pltpu.CompilerParams(
            collective_id=0, has_side_effects=True, vmem_limit_bytes=VMEM_LIMIT
        ),
        name="opening",
    )(*gathered, *rows, *later)
    return outs[:count], outs[count : count + 2], outs[count + 2]


def pair_product_kernel(left_ref, right_ref, left_weight, right_weight, *refs):
    out_ref = refs[-1]
    out_ref[...] = (
        contract_last(left_ref[...], left_weight[...])
        + contract_last(right_ref[...], right_weight[...])
    ).astype(out_ref.dtype)


def block_sum_kernel(index_ref, whole_ref, *refs, count):
    del index_ref
    total = whole_ref[...].astype(jnp.float32)
    for ref in refs[:count]:
        total = total + ref[...].astype(jnp.float32)
    refs[-1][...] = total.astype(refs[-1].dtype)


def block_sum(whole, index, received, after, dtype):
    rows, columns = received[0].shape
    step = min(rows, 256)
    tiles = rows // step
    tile = pl.BlockSpec((step, columns), lambda i, index: (i, 0))
    return pl.pallas_call(
        functools.partial(block_sum_kernel, count=len(received)),
        grid_spec=pltpu.PrefetchScalarGridSpec(
            num_scalar_prefetch=1,
            grid=(tiles,),
            in_specs=[pl.BlockSpec((step, columns), lambda i, index: (index[0] * tiles + i, 0))]
            + [tile] * len(received)
            + [pl.BlockSpec(memory_space=pl.ANY)] * len(after),
            out_specs=tile,
        ),
        out_shape=jax.ShapeDtypeStruct((rows, columns), dtype),
        cost_estimate=pl.CostEstimate(
            flops=rows * columns, bytes_accessed=6 * rows * columns, transcendentals=0
        ),
        name="block_sum",
    )(jnp.asarray(index, jnp.int32).reshape(1), whole, *received, *after)


def place_columns_kernel(rank_ref, *refs):
    del rank_ref
    for number, ref in enumerate(refs[:-1]):

        @pl.when(pl.program_id(1) == number)
        def _():
            refs[-1][...] = ref[...].astype(refs[-1].dtype)


def place_columns(parts, rank):
    count = len(parts)
    rows, columns = parts[0].shape
    step = min(rows, 256)
    tile = pl.BlockSpec((step, columns), lambda i, k, rank: (i, 0))
    return pl.pallas_call(
        place_columns_kernel,
        grid_spec=pltpu.PrefetchScalarGridSpec(
            num_scalar_prefetch=1,
            grid=(rows // step, count),
            in_specs=[tile] * count,
            out_specs=pl.BlockSpec(
                (step, columns), lambda i, k, rank: (i, lax.rem(rank[0] + k, count))
            ),
        ),
        out_shape=jax.ShapeDtypeStruct((rows, columns * count), jnp.float32),
        cost_estimate=pl.CostEstimate(
            flops=0, bytes_accessed=6 * rows * columns * count, transcendentals=0
        ),
        name="place_columns",
    )(jnp.asarray(rank, jnp.int32).reshape(1), *parts)


def norm_grad_kernel(
    left_ref,
    right_ref,
    x_ref,
    left_weight,
    right_weight,
    left_gain,
    right_gain,
    after_ref,
    out_ref,
    sums_ref,
):
    del after_ref
    x = x_ref[...].astype(jnp.float32)
    centered = x - jnp.mean(x, axis=-1, keepdims=True)
    inverse = lax.rsqrt(jnp.mean(centered * centered, axis=-1, keepdims=True) + EPSILON)
    hat = centered * inverse
    left = contract_last(left_ref[...], left_weight[...])
    right = contract_last(right_ref[...], right_weight[...])
    scaled = left * left_gain[...] + right * right_gain[...]
    first = pl.program_id(0) == 0
    for row, part in enumerate((left * hat, left, right * hat, right)):
        total = jnp.sum(part, axis=0, keepdims=True)
        sums_ref[row : row + 1, :] = jnp.where(first, 0.0, sums_ref[row : row + 1, :]) + total
    inner = (
        scaled
        - jnp.mean(scaled, axis=-1, keepdims=True)
        - hat * jnp.mean(scaled * hat, axis=-1, keepdims=True)
    )
    out_ref[...] = (inverse * inner).astype(out_ref.dtype)


ROWS_STEP = 256


def row_specs(arrays, start, rows):
    step = min(ROWS_STEP, rows)
    return step, [
        pl.BlockSpec((step, v.shape[1]), lambda i, first=start // step: (first + i, 0))
        for v in arrays
    ]


def whole_spec(array):
    return pl.BlockSpec(array.shape, lambda i: (0, 0))


def half_spec(array, half):
    return pl.BlockSpec((array.shape[0], array.shape[1] // 2), lambda i: (0, half))


def pair_product(left, right, left_weight, right_weight, after, start, rows):
    step, specs = row_specs((left, right), start, rows)
    width = left_weight.shape[0]
    return pl.pallas_call(
        pair_product_kernel,
        grid=(rows // step,),
        out_shape=jax.ShapeDtypeStruct((rows, width), jnp.bfloat16),
        in_specs=specs
        + [whole_spec(left_weight), half_spec(right_weight, 1)]
        + [pl.BlockSpec(memory_space=pl.ANY)] * len(after),
        out_specs=pl.BlockSpec((step, width), lambda i: (i, 0)),
        compiler_params=pltpu.CompilerParams(vmem_limit_bytes=VMEM_LIMIT),
        cost_estimate=pl.CostEstimate(
            flops=2 * rows * width * (left.shape[1] + right.shape[1]),
            bytes_accessed=2 * rows * (width + left.shape[1] + right.shape[1]),
            transcendentals=0,
        ),
        name="pair_product",
    )(left, right, left_weight, right_weight, *after)


def norm_grad(
    left, right, x, left_weight, right_weight, left_gain, right_gain, after, start, rows
):
    step, specs = row_specs((left, right, x), start, rows)
    width = left_weight.shape[0]
    rest = [left_weight, right_weight, left_gain, right_gain]
    return pl.pallas_call(
        norm_grad_kernel,
        grid=(rows // step,),
        out_shape=(
            jax.ShapeDtypeStruct((rows, width), jnp.bfloat16),
            jax.ShapeDtypeStruct((4, width), jnp.float32),
        ),
        in_specs=specs
        + [whole_spec(left_weight), half_spec(right_weight, 0)]
        + [whole_spec(v) for v in rest[2:]]
        + [pl.BlockSpec(memory_space=pl.ANY)],
        out_specs=(
            pl.BlockSpec((step, width), lambda i: (i, 0)),
            pl.BlockSpec((4, width), lambda i: (0, 0)),
        ),
        compiler_params=pltpu.CompilerParams(vmem_limit_bytes=VMEM_LIMIT),
        cost_estimate=pl.CostEstimate(
            flops=2 * rows * width * (left.shape[1] + right.shape[1]),
            bytes_accessed=2 * rows * (2 * width + left.shape[1] + right.shape[1]),
            transcendentals=0,
        ),
        name="norm_grad",
    )(left, right, x, *rest, after)


SCALAR = pl.BlockSpec(memory_space=pltpu.SMEM)
VECTOR = pl.BlockSpec(memory_space=pltpu.VMEM)


def attend(order, bounds, proj, tables, seg_col, seg_row, block, count):
    length = proj.shape[0]
    pairs = length * length
    return pl.pallas_call(
        functools.partial(attend_kernel, block=block, count=count),
        out_shape=(
            jax.ShapeDtypeStruct((length, HD), jnp.bfloat16),
            jax.ShapeDtypeStruct((length, HD), jnp.bfloat16),
            jax.ShapeDtypeStruct((length, HD), jnp.bfloat16),
            jax.ShapeDtypeStruct((length, HD), jnp.bfloat16),
            jax.ShapeDtypeStruct((length, 1), jnp.float32),
        ),
        in_specs=[SCALAR] * 2 + [VECTOR] * 6,
        out_specs=(VECTOR,) * 5,
        scratch_shapes=[
            pltpu.VMEM((block, 1), jnp.float32),
            pltpu.VMEM((block, 1), jnp.float32),
            pltpu.VMEM((block, HD), jnp.float32),
        ],
        compiler_params=pltpu.CompilerParams(vmem_limit_bytes=VMEM_LIMIT),
        cost_estimate=pl.CostEstimate(
            flops=2 * pairs * HD, bytes_accessed=16 * length * HD, transcendentals=pairs // 2
        ),
        name="attend",
    )(order, bounds, proj, *tables, seg_col, seg_row)


def attend_grad(
    order, bounds, query, key, value, attn, grad, lse, tables, seg_col, seg_row, block, count
):
    length = query.shape[0]
    pairs = length * length
    return pl.pallas_call(
        functools.partial(attend_grad_kernel, block=block, count=count),
        out_shape=(
            jax.ShapeDtypeStruct((length, 3 * HD), jnp.bfloat16),
            jax.ShapeDtypeStruct((1, 3 * HD), jnp.float32),
        ),
        in_specs=[SCALAR] * 2 + [VECTOR] * 11,
        out_specs=(VECTOR,) * 2,
        scratch_shapes=[
            pltpu.VMEM((length, HD), jnp.float32),
            pltpu.VMEM((block, HD), jnp.float32),
            pltpu.VMEM((block, HD), jnp.float32),
            pltpu.VMEM((length, 1), jnp.float32),
        ],
        compiler_params=pltpu.CompilerParams(vmem_limit_bytes=VMEM_LIMIT),
        cost_estimate=pl.CostEstimate(
            flops=5 * pairs * HD, bytes_accessed=16 * length * HD, transcendentals=pairs // 2
        ),
        name="attend_grad",
    )(order, bounds, query, key, value, attn, grad, lse, *tables, seg_col, seg_row)


def ring_shift(value, axis, step):
    count = lax.axis_size(axis)
    return lax.ppermute(value, axis, [(i, (i + step) % count) for i in range(count)])


class Plane:
    def __init__(self):
        self.count = lax.axis_size("shard")
        side = math.isqrt(self.count)
        self.square = side * side == self.count
        self.first, self.second = (side, side) if self.square else (1, self.count)
        self.ranks = lax.axis_size("ctx")
        shard = lax.axis_index("shard")
        self.flip = (lax.axis_index("ctx") % 2 == 1) if self.square else False
        slow, fast = shard // self.second, shard % self.second
        if self.square:
            self.here = (jnp.where(self.flip, slow, fast), jnp.where(self.flip, fast, slow))
        else:
            self.here = (slow, fast)

    def index(self, first_step, second_step):
        first = lax.rem(self.here[0] + first_step + self.first, self.first)
        second = lax.rem(self.here[1] + second_step + self.second, self.second)
        if not self.square:
            return first * self.second + second
        side = self.first
        return jnp.where(self.flip, first * side + second, second * side + first)

    def move(self, value, first_step, second_step):
        pairs = []
        for shard in range(self.count):
            for rank in range(self.ranks):
                slow, fast = divmod(shard, self.second)
                if self.square and rank % 2 == 0:
                    slow = (slow + second_step) % self.second
                    fast = (fast + first_step) % self.first
                else:
                    slow = (slow + first_step) % self.first
                    fast = (fast + second_step) % self.second
                target = slow * self.second + fast
                pairs.append((shard * self.ranks + rank, target * self.ranks + rank))
        return lax.ppermute(value, ("shard", "ctx"), pairs)

    def scatter_sum(self, partial, after, last=()):
        rows = partial.shape[0] // self.count
        sums, final = {}, []
        for b in list(range(1, self.second)) + [0]:
            received = []
            for a in range(1, self.first):
                block = lax.dynamic_slice_in_dim(partial, self.index(a, b) * rows, rows)
                received.append(self.move(block, a, 0))
            if b == 0:
                final = received
            elif received:
                sums[b] = block_sum(partial, self.index(0, b), received, after, partial.dtype)
            else:
                sums[b] = lax.dynamic_slice_in_dim(partial, self.index(0, b) * rows, rows)
        final = final + [self.move(sums[b], 0, b) for b in range(1, self.second)]
        return block_sum(partial, self.index(0, 0), final, [*after, *last], partial.dtype)

    def full_sum(self, value):
        total = value
        for a in range(1, self.first):
            total = total + self.move(value, a, 0)
        value = total
        for b in range(1, self.second):
            total = total + self.move(value, 0, b)
        return total


def local(
    hidden_in,
    grad_out,
    segment_ids,
    group_order,
    ln1_gain,
    ln1_bias,
    qkv_weight,
    qkv_bias,
    dense_weight,
    dense_bias,
    ln2_gain,
    ln2_bias,
    up_weight,
    up_bias,
    down_weight,
    down_bias,
):
    _, groups_dev, block_len, width = hidden_in.shape
    tokens = groups_dev * block_len
    seq_len = segment_ids.shape[1]
    groups = seq_len // block_len
    ctx_count, tp_count = lax.axis_size("ctx"), lax.axis_size("tp")
    shard_count = lax.axis_size("shard")
    ctx_rank, tp_rank = lax.axis_index("ctx"), lax.axis_index("tp")
    shard_rank = lax.axis_index("shard")
    slice_width = width // tp_count
    bf16, f32 = jnp.bfloat16, jnp.float32

    def my_columns(matrix):
        columns = matrix.shape[1] // ctx_count
        return lax.dynamic_slice_in_dim(matrix, ctx_rank * columns, columns, 1)

    plane = Plane()

    x_mine = hidden_in.reshape(tokens, width)
    g_mine = grad_out.reshape(tokens, width)
    vectors = [
        ln1_gain, ln1_bias, ln2_gain, ln2_bias, dense_bias, down_bias, qkv_bias[0], up_bias[0],
    ]
    sizes = [v.shape[0] for v in vectors]
    wide = -(-max(sizes) // LANES) * LANES
    packed = jnp.stack([jnp.pad(v, (0, wide - v.shape[0])) for v in vectors])
    packed = jnp.concatenate([packed, jnp.zeros_like(packed)], axis=0)
    (w_vectors, w_qkv, w_dense), (x_row, g_row), wide_mine = opening(
        [packed, qkv_weight, dense_weight],
        [False, True, True],
        [x_mine, g_mine],
        [up_weight, down_weight],
        ctx_count,
    )
    w_wide = lax.all_gather(wide_mine, "shard", axis=0, tiled=True)
    units = w_wide.shape[1] // 2
    w_up, w_down = w_wide[:, :units], w_wide[:, units:]
    w_vectors = w_vectors.reshape(shard_count, packed.shape[0], wide)
    spread = [
        w_vectors[:, number, :size].reshape(-1).astype(f32) for number, size in enumerate(sizes)
    ]
    gain_one, shift_one, gain_two, shift_two, bias_dense, bias_down, bias_qkv, bias_up = spread
    bias_qkv = my_columns(bias_qkv[None])
    bias_up = my_columns(bias_up[None])
    plane = Plane()
    heads_here = w_qkv.shape[1] // (3 * HD)

    own_order = jnp.concatenate(
        [
            lax.dynamic_slice_in_dim(
                group_order, lax.rem(ctx_rank + k, ctx_count) * groups_dev, groups_dev
            )
            for k in range(ctx_count)
        ]
    )
    segments = segment_ids[0]
    positions = segment_positions(segments)

    def stored(values):
        return jnp.concatenate(
            [
                lax.dynamic_slice_in_dim(values, own_order[k] * block_len, block_len)
                for k in range(groups)
            ]
        )

    seg_stored = stored(segments)
    tables = rotary_tables(stored(positions))
    seg_blocks = seg_stored.reshape(groups, block_len)
    bounds = jnp.stack([seg_blocks[:, 0], seg_blocks[:, -1]])
    seg_col, seg_row = seg_stored[:, None], seg_stored[None, :]

    x_float = x_row.astype(f32)
    centered = x_float - jnp.mean(x_float, axis=-1, keepdims=True)
    inverse = lax.rsqrt(jnp.mean(centered * centered, axis=-1, keepdims=True) + EPSILON)
    hat = centered * inverse
    acts_one = (hat * gain_one + shift_one).astype(bf16)
    acts_two = (hat * gain_two + shift_two).astype(bf16)

    projected = jnp.dot(acts_one, w_qkv, preferred_element_type=f32) + bias_qkv
    heads = []
    for h in range(heads_here):
        heads.append(
            attend(
                own_order,
                bounds,
                projected[:, 3 * HD * h : 3 * HD * (h + 1)],
                tables,
                seg_col,
                seg_row,
                block_len,
                groups,
            )
        )
    attn = jnp.concatenate([head[3] for head in heads], axis=1)

    attn_grad = jnp.dot(g_row, w_dense, preferred_element_type=f32).astype(bf16)
    proj_parts, sum_parts = [], []
    for h, (query, key, value, attn_head, lse) in enumerate(heads):
        part, sums = attend_grad(
            own_order,
            bounds,
            query,
            key,
            value,
            attn_head,
            attn_grad[:, HD * h : HD * (h + 1)],
            lse,
            tables,
            seg_col,
            seg_row,
            block_len,
            groups,
        )
        proj_parts.append(part)
        sum_parts.append(sums[0])
    proj_grad_b = jnp.concatenate(proj_parts, axis=1)
    qkv_bias_grad = jnp.concatenate(sum_parts)

    pre_act = jnp.dot(acts_two, w_up, preferred_element_type=f32) + bias_up
    cdf = 0.5 * (1.0 + lax.erf(pre_act * (1.0 / math.sqrt(2.0))))
    hidden = (pre_act * cdf).astype(bf16)
    slope = cdf + pre_act * jnp.exp(-0.5 * pre_act * pre_act) * (1.0 / math.sqrt(2.0 * math.pi))

    def reduce_partial(parts):
        received = [ring_shift(parts[k], "ctx", k) for k in range(1, ctx_count)]
        total = block_sum(parts[0], 0, received, [], bf16)
        return total, lax.psum_scatter(total, "tp", scatter_dimension=1, tiled=True).astype(f32)

    dense_local = contract_first(g_row, attn).astype(bf16)
    out_parts = {}
    for k in reversed(range(ctx_count)):
        out_parts[k] = pair_product(
            attn,
            hidden,
            w_dense,
            w_wide,
            [proj_grad_b, dense_local] if k + 1 == ctx_count else [out_parts[k + 1]],
            k * tokens,
            tokens,
        )
    out_total, summed_out = reduce_partial(out_parts)
    out_shift = lax.dynamic_slice_in_dim(bias_dense + bias_down, tp_rank * slice_width, slice_width)
    x_slice = lax.dynamic_slice_in_dim(x_mine, tp_rank * slice_width, slice_width, 1)
    output = x_slice.astype(f32) + summed_out + out_shift

    def reduce_weight(grad, after, last=()):
        mine = plane.scatter_sum(grad, after, last)
        parts = [mine] + [ring_shift(mine, "ctx", ctx_count - k) for k in range(1, ctx_count)]
        return place_columns(parts, ctx_rank)

    bias_grad = jnp.sum(g_row.astype(f32), axis=0)

    pre_grad = jnp.dot(g_row, w_down, preferred_element_type=f32) * slope
    up_bias_grad = jnp.sum(pre_grad, axis=0)
    pre_grad_b = pre_grad.astype(bf16)

    in_parts, norm_sums = {}, jnp.zeros((4, width), f32)
    for k in reversed(range(ctx_count)):
        in_parts[k], sums = norm_grad(
            proj_grad_b,
            pre_grad_b,
            x_row,
            w_qkv,
            w_wide,
            gain_one[None],
            gain_two[None],
            in_parts[k + 1] if k + 1 in in_parts else out_total,
            k * tokens,
            tokens,
        )
        norm_sums = norm_sums + sums
    in_total, input_sum = reduce_partial(in_parts)
    g_slice = lax.dynamic_slice_in_dim(g_mine, tp_rank * slice_width, slice_width, 1)
    input_grad = g_slice.astype(f32) + input_sum

    down_local = contract_first(g_row, hidden).astype(bf16)
    qkv_local = contract_first(acts_one, proj_grad_b).astype(bf16)
    up_local = contract_first(acts_two, pre_grad_b).astype(bf16)
    late = [qkv_local, up_local]
    down_grad = reduce_weight(down_local, [in_total])
    dense_grad = reduce_weight(dense_local, [in_total])

    norm_sums = norm_sums.reshape(-1)
    column_sums = [up_bias_grad, qkv_bias_grad]
    packed = jnp.concatenate([norm_sums] + column_sums)
    wholes = [jnp.zeros((v.shape[0] * ctx_count,), f32) for v in column_sums]
    total = jnp.zeros_like(norm_sums)
    for k in range(ctx_count):
        part = packed if k == 0 else ring_shift(packed, "ctx", ctx_count - k)
        total = total + part[: norm_sums.shape[0]]
        offset = norm_sums.shape[0]
        for number, vector in enumerate(column_sums):
            size = vector.shape[0]
            wholes[number] = lax.dynamic_update_slice_in_dim(
                wholes[number],
                part[offset : offset + size],
                lax.rem(ctx_rank + k, ctx_count) * size,
                0,
            )
            offset += size
    norm_sums = total
    for k in range(1, tp_count):
        norm_sums = norm_sums + ring_shift(total, "tp", k)
    pieces = [bias_grad] + wholes + [
        norm_sums[k * width : (k + 1) * width] for k in range(4)
    ]
    reduced = plane.full_sum(jnp.concatenate(pieces))
    ready = [norm_sums, dense_grad, down_grad]
    qkv_grad = reduce_weight(qkv_local, late, ready)
    up_grad = reduce_weight(up_local, late, ready)
    results, offset = [], 0
    for piece in pieces:
        own = piece.shape[0] // shard_count
        results.append(lax.dynamic_slice_in_dim(reduced, offset + shard_rank * own, own))
        offset += piece.shape[0]
    bias_grad, up_bias_grad, qkv_bias_grad = results[:3]
    gain_one_grad, shift_one_grad, gain_two_grad, shift_two_grad = results[3:]
    out_shape = hidden_in.shape[:3] + (slice_width,)
    return (
        output.reshape(out_shape),
        input_grad.reshape(out_shape),
        gain_one_grad,
        shift_one_grad,
        qkv_grad,
        qkv_bias_grad[None],
        dense_grad,
        bias_grad,
        gain_two_grad,
        shift_two_grad,
        up_grad,
        up_bias_grad[None],
        down_grad,
    )


def solution(mesh):
    return jax.shard_map(
        local,
        mesh=mesh,
        in_specs=(
            P("shard", "ctx", None, None),
            P("shard", "ctx", None, None),
            P("shard", None),
            P(),
            P("shard"),
            P("shard"),
            P("shard", "tp"),
            P("tp", "shard"),
            P("shard", "tp"),
            P("shard"),
            P("shard"),
            P("shard"),
            P("shard", "tp"),
            P("tp", "shard"),
            P("shard", "tp"),
            P("shard"),
        ),
        out_specs=(
            P("shard", "ctx", None, "tp"),
            P("shard", "ctx", None, "tp"),
            P("shard"),
            P("shard"),
            P("shard", "tp"),
            P("tp", "shard"),
            P("shard", "tp"),
            P("shard"),
            P("shard"),
            P("shard"),
            P("shard", "tp"),
            P("tp", "shard"),
            P("shard", "tp"),
        ),
        check_vma=False,
    )
```
